64 devices in a mesh: prob: 4 (over x, y), feat: 16 (over z, core).
Axes of the slice: x: 2, y: 2, z: 8, core: 2. Of those that a mesh axis runs over, the one named last changes fastest.
The devices are a block of a 4x4x8 slice.
Arguments:
- x_data: bfloat16 [4096, 3072], P('prob'), parts along dimension 0
- targets: float32 [4096], P('prob'), parts along dimension 0
- w_in: float32 [8192, 3072], P(('prob', 'feat')), parts along dimension 0
- w_out: float32 [8192], P(('prob', 'feat')), parts along dimension 0
- reg_weight: float32 [4], P('prob'), parts along dimension 0
- step_size: float32 [4], P('prob'), parts along dimension 0
Outputs:
- output 1: float32 [8192, 3072], P(('prob', 'feat')), parts along dimension 0
- output 2: float32 [8192], P(('prob', 'feat')), parts along dimension 0
- output 3: float32 [24], P('prob'), parts along dimension 0
There are 4 independent parts. The reference program is written for one: setup_inputs(seed, part) draws one part's arguments, and reference() takes and returns one part's arrays. A program takes and returns all parts, laid end to end along the dimension named above; each array names one.
All inputs are finite; a program needn't handle non-finite values.
Results may differ from the reference program's by a relative error of at most 0.001.
Values are sent between devices in bfloat16 or wider.
A program may use at most 768 MiB of HBM per device.

```python
import math
import jax
import jax.numpy as jnp
from jax import lax

NUM_ROWS = 1024
IN_DIM = 3072
HIDDEN = 2048
NUM_ITERS = 6
HIST_LEN = 3

IN_SCALE = 1.0 / math.sqrt(IN_DIM)
OUT_SCALE = 1.0 / math.sqrt(HIDDEN)


def setup_inputs(seed: int = 0, part: int = 0) -> dict:
    base_key = jax.random.fold_in(jax.random.key(seed), part)
    sub_keys = jax.random.split(base_key, 7)
    labels = jax.random.randint(sub_keys[0], (NUM_ROWS,), 0, 2)
    label_sign = (2 * labels - 1).astype(jnp.float32)
    mean_dir = 0.5 * jax.random.normal(sub_keys[1], (IN_DIM,), jnp.float32)
    noise_mat = jax.random.normal(sub_keys[2], (NUM_ROWS, IN_DIM), jnp.float32)
    x_data = (noise_mat + label_sign[:, None] * mean_dir[None, :]).astype(jnp.bfloat16)
    unit_pos = jnp.arange(HIDDEN, dtype=jnp.float32) / HIDDEN
    row_scale = jnp.exp2(2.0 * unit_pos - 1.0)
    w_in = jax.random.normal(sub_keys[3], (HIDDEN, IN_DIM), jnp.float32) * row_scale[:, None]
    w_out = jax.random.normal(sub_keys[4], (HIDDEN,), jnp.float32)
    reg_weight = jax.random.uniform(sub_keys[5], (1,), jnp.float32, 0.01, 0.02)
    step_size = jax.random.uniform(sub_keys[6], (1,), jnp.float32, 0.08, 0.2)
    return {"x_data": x_data, "targets": labels.astype(jnp.float32), "w_in": w_in, "w_out": w_out, "reg_weight": reg_weight, "step_size": step_size}


def fit_loss(w_in, w_out, x_f32, targets):
    pre_act = lax.dot_general(x_f32, w_in, (((1,), (1,)), ((), ()))) * IN_SCALE
    logits = jnp.dot(jnp.tanh(pre_act), w_out) * OUT_SCALE
    return jnp.mean(jax.nn.softplus(logits) - targets * logits)


def pair_dot(first, second):
    return jnp.sum(first[0] * second[0]) + jnp.sum(first[1] * second[1])


def pair_axpy(base, coef, other):
    return (base[0] + coef * other[0], base[1] + coef * other[1])


def two_loop(full_grad, hist_s, hist_y, rho_vals, gamma_scale, dot_fn):
    query_vec = full_grad
    a_coefs = {}
    for pos_idx in reversed(range(len(hist_s))):
        a_coefs[pos_idx] = rho_vals[pos_idx] * dot_fn(hist_s[pos_idx], query_vec)
        query_vec = pair_axpy(query_vec, -a_coefs[pos_idx], hist_y[pos_idx])
    result = (gamma_scale * query_vec[0], gamma_scale * query_vec[1])
    for pos_idx in range(len(hist_s)):
        b_coef = rho_vals[pos_idx] * dot_fn(hist_y[pos_idx], result)
        result = pair_axpy(result, a_coefs[pos_idx] - b_coef, hist_s[pos_idx])
    return result


def reference(x_data, targets, w_in, w_out, reg_weight, step_size):
    x_f32 = x_data.astype(jnp.float32)
    reg_coef = reg_weight[0]
    step_coef = step_size[0]
    loss_grad = jax.value_and_grad(fit_loss, argnums=(0, 1))
    params = (w_in, w_out)
    prev_params = params
    prev_grad = params
    hist_s = []
    hist_y = []
    rho_vals = []
    losses = []
    for iter_idx in range(NUM_ITERS):
        loss_val, fit_grad = loss_grad(params[0], params[1], x_f32, targets)
        losses.append(loss_val)
        full_grad = pair_axpy(fit_grad, reg_coef, params)
        if iter_idx == 0:
            direction = full_grad
        else:
            s_vec = pair_axpy(params, -1.0, prev_params)
            y_vec = pair_axpy(full_grad, -1.0, prev_grad)
            curv_ys = pair_dot(y_vec, s_vec)
            hist_s = (hist_s + [s_vec])[-HIST_LEN:]
            hist_y = (hist_y + [y_vec])[-HIST_LEN:]
            rho_vals = (rho_vals + [1.0 / curv_ys])[-HIST_LEN:]
            gamma_scale = curv_ys / pair_dot(y_vec, y_vec)
            direction = two_loop(full_grad, hist_s, hist_y, rho_vals, gamma_scale, pair_dot)
        prev_params = params
        prev_grad = full_grad
        params = pair_axpy(params, -step_coef, direction)
    return params[0], params[1], jnp.stack(losses)
```

```python
import functools
import math

import jax
import jax.numpy as jnp
from jax import lax
from jax.experimental import pallas as pl
from jax.experimental.pallas import tpu as pltpu
from jax.sharding import PartitionSpec as P

NUM_ITERS = 6
HIST = 3
LANES = 128
SUBL = 8
ROW_CHUNK = 512
COL_CHUNK = 512
NUM_DOTS = 8
MESH = pl.DeviceIdType.MESH
F32 = jnp.float32
BF16 = jnp.bfloat16


def split3(val):
    high = val.astype(BF16)
    rest = val - high.astype(F32)
    mid = rest.astype(BF16)
    low = (rest - mid.astype(F32)).astype(BF16)
    return high, mid, low


def fold(val):
    rows, cols = val.shape
    part = jnp.sum(val.reshape(rows // SUBL, SUBL, cols), axis=0)
    total = part[:, :LANES]
    for start in range(LANES, cols, LANES):
        total = total + part[:, start : start + LANES]
    return total


def merge3(prod, rows):
    return (prod[2 * rows :] + prod[rows : 2 * rows]) + prod[:rows]


def kernel(
    axis, n, in_scale, out_scale,
    x_hbm, t_ref, win_hbm, wout_ref, reg_ref, step_ref,
    out_w, out_w2, out_loss,
    x_v, theta, grad, hist_s, hist_y, pre, hid, fac, q_s, q_y, q_g,
    split_d, split_g, resid, logits_v, coef,
    z_src, z_buf, d_src, d_buf,
    load_sem, out_sem, send_sem, recv_sem,
):
    num_rows, dim = x_v.shape
    hid_rows = grad.shape[0]
    row_tiles = num_rows // LANES
    me = lax.axis_index(axis)
    offsets = sorted(range(1, n), key=lambda off: -min(off, n - off))
    peers = [lax.rem(me + off, n) for off in offsets]

    barrier = pltpu.get_barrier_semaphore()
    for peer in peers:
        pl.semaphore_signal(barrier, inc=1, device_id={axis: peer}, device_id_type=MESH)

    w_load = pltpu.make_async_copy(win_hbm, theta.at[:, pl.ds(0, dim)], load_sem.at[0])
    w_load.start()
    x_loads = []
    for idx in range(num_rows // ROW_CHUNK):
        part = pl.ds(idx * ROW_CHUNK, ROW_CHUNK)
        load = pltpu.make_async_copy(x_hbm.at[part], x_v.at[part], load_sem.at[1 + idx])
        load.start()
        x_loads.append(load)

    reg = reg_ref[0]
    step = step_ref[0]
    lane = lax.broadcasted_iota(jnp.int32, (hid_rows, LANES), 1)
    eye = lane == lax.broadcasted_iota(jnp.int32, (hid_rows, LANES), 0)
    col_parts = [pl.ds(start, COL_CHUNK) for start in range(0, dim, COL_CHUNK)]
    tail = pl.ds(dim, LANES)

    def send_all(src, dst, sem):
        for peer in peers:
            pltpu.make_async_remote_copy(
                src_ref=src, dst_ref=dst.at[me], send_sem=send_sem.at[sem], recv_sem=recv_sem.at[sem],
                device_id={axis: peer}, device_id_type=MESH,
            ).start()

    def wait_all(dst, sem):
        others = dst.at[pl.ds(0, n - 1)]
        pltpu.make_async_copy(others, others, recv_sem.at[sem]).wait()
        pltpu.make_async_copy(others, others, send_sem.at[sem]).wait()

    def times_x(out_fn):
        for idx in range(num_rows // ROW_CHUNK):
            part = pl.ds(idx * ROW_CHUNK, ROW_CHUNK)
            prod = lax.dot_general(split_g[...], x_v[part, :], (((1,), (1,)), ((), ())), preferred_element_type=F32)
            out_fn(part, merge3(prod, hid_rows) * in_scale)

    def store_split(ref, part, val):
        for idx, term in enumerate(split3(val)):
            ref[idx * hid_rows : (idx + 1) * hid_rows, part] = term

    def send_logits(buf, sem):
        w2 = jnp.broadcast_to(theta[:, dim : dim + 1], (hid_rows, LANES))
        rows = []
        for idx in range(row_tiles):
            part = pl.ds(idx * LANES, LANES)
            act = jnp.tanh(pre[:, part])
            hid[:, part] = act
            rows.append(jnp.sum(fold(act * w2), axis=0, keepdims=True))
        z_mine = jnp.concatenate(rows, axis=0)
        z_src[...] = z_mine
        buf[me] = z_mine
        send_all(z_src, buf, sem)
        w2s = w2 * (out_scale * in_scale)
        for idx in range(row_tiles):
            part = pl.ds(idx * LANES, LANES)
            act = hid[:, part]
            fac[:, part] = w2s * (1.0 - act * act)

    def residual(buf, sem):
        wait_all(buf, sem)
        logits = jnp.sum(buf[...], axis=0) * out_scale
        logits_v[...] = logits
        resid[...] = (jax.nn.sigmoid(logits) - t_ref[...]) * (1.0 / num_rows)
        for idx in range(row_tiles):
            part = pl.ds(idx * LANES, LANES)
            store_split(split_d, part, fac[:, part] * resid[idx : idx + 1, :])

    def grad_tail():
        total = hid[:, :LANES] * resid[0:1, :]
        for idx in range(1, row_tiles):
            total = total + hid[:, idx * LANES : (idx + 1) * LANES] * resid[idx : idx + 1, :]
        g_out = jnp.sum(total, axis=1, keepdims=True) * out_scale
        return jnp.where(lane == 0, g_out, 0.0) + reg * theta[:, tail]

    def grad_part(part):
        prod = jnp.dot(split_d[...], x_v[:, part], preferred_element_type=F32)
        return merge3(prod, hid_rows) + reg * theta[:, part]

    def store_loss(idx):
        logits = logits_v[...]
        soft = jnp.maximum(logits, 0.0) + jnp.log1p(jnp.exp(-jnp.abs(logits)))
        out_loss[idx] = jnp.sum(soft - t_ref[...] * logits) * (1.0 / num_rows)

    def combine(cfs, slots, vec_g, vec_s, vec_y, part):
        rows, cols = vec_g.shape[0], part.size

        def scaled(cf, val):
            parts = [
                (val[:, start : start + LANES].reshape(rows // SUBL, SUBL, LANES) * cf[None]).reshape(rows, LANES)
                for start in range(0, cols, LANES)
            ]
            return parts[0] if len(parts) == 1 else jnp.concatenate(parts, axis=1)

        total = scaled(cfs[0], vec_g[:, part])
        for idx, slot in enumerate(slots):
            total = total + scaled(cfs[1 + idx], vec_s[slot, :, part])
            total = total + scaled(cfs[1 + HIST + idx], vec_y[slot, :, part])
        return total

    def move(k, cfs, slots):
        slot_new = slots[-1]
        s_part = combine(cfs, slots, grad, hist_s, hist_y, tail)
        hist_s[slot_new, :, tail] = s_part
        theta[:, tail] = theta[:, tail] + s_part
        for idx in range(row_tiles):
            part = pl.ds(idx * LANES, LANES)
            q_part = combine(cfs, slots, q_g, q_s, q_y, part)
            q_s[slot_new, :, part] = q_part
            pre[:, part] = pre[:, part] + q_part

    def move_rest(cfs, slots):
        slot_new = slots[-1]
        acc = fold(grad[:, tail] * hist_s[slot_new, :, tail])
        for part in col_parts:
            s_part = combine(cfs, slots, grad, hist_s, hist_y, part)
            hist_s[slot_new, :, part] = s_part
            theta[:, part] = theta[:, part] + s_part
            acc = acc + fold(grad[:, part] * s_part)
        return acc

    def new_grad(slots, acc_gs):
        new, old1, old2 = slots
        accs = [None] * 7

        def add(part, g_new):
            g_old = grad[:, part]
            y_new = g_new - g_old
            grad[:, part] = g_new
            others = [
                hist_s[new, :, part], hist_s[old1, :, part], hist_s[old2, :, part],
                y_new, hist_y[old1, :, part], hist_y[old2, :, part], g_old,
            ]
            hist_y[new, :, part] = y_new
            for idx, other in enumerate(others):
                term = fold(y_new * other)
                accs[idx] = term if accs[idx] is None else accs[idx] + term

        add(tail, grad_tail())
        for part in col_parts:
            add(part, grad_part(part))
        sums = [jnp.sum(acc, axis=0, keepdims=True) for acc in accs + [acc_gs]]
        totals = jnp.sum(jnp.concatenate(sums, axis=0), axis=1, keepdims=True)
        packed = jnp.sum(jnp.where(eye[:NUM_DOTS], totals, 0.0), axis=0, keepdims=True)
        d_src[...] = packed
        d_buf[me] = packed
        send_all(d_src, d_buf, 2)

    def new_q(slot):
        for part in col_parts:
            store_split(split_g, part, grad[:, part])

        def keep(part, val):
            q_y[slot, :, part] = val - q_g[:, part]
            q_g[:, part] = val

        times_x(keep)

    def two_loop(carry):
        rho1, rho2, psg0, psg1, pyg0, pyg1, pys1, yy11, yy12, yy22 = carry
        wait_all(d_buf, 2)
        total = jnp.sum(d_buf[...], axis=0)
        ys0, ys1, ys2, yy0, yy1, yy2, ygp, gs0 = (
            jnp.broadcast_to(total[:, idx : idx + 1], (SUBL, LANES)) for idx in range(NUM_DOTS)
        )
        sg0, sg1, sg2 = gs0 + ys0, psg0 + ys1, psg1 + ys2
        yg0, yg1, yg2 = ygp + yy0, pyg0 + yy1, pyg1 + yy2
        rho0 = 1.0 / ys0
        gamma = ys0 / yy0
        a0 = rho0 * sg0
        a1 = rho1 * (sg1 - a0 * ys1)
        a2 = rho2 * (sg2 - a0 * ys2 - a1 * pys1)
        yq2 = yg2 - a0 * yy2 - a1 * yy12 - a2 * yy22
        yq1 = yg1 - a0 * yy1 - a1 * yy11 - a2 * yy12
        yq0 = yg0 - a0 * yy0 - a1 * yy1 - a2 * yy2
        c2 = a2 - rho2 * (gamma * yq2)
        c1 = a1 - rho1 * (gamma * yq1 + c2 * pys1)
        c0 = a0 - rho0 * (gamma * yq0 + c2 * ys2 + c1 * ys1)
        sgam = step * gamma
        for idx, val in enumerate((-sgam, -step * c0, -step * c1, -step * c2, sgam * a0, sgam * a1, sgam * a2)):
            coef[idx] = val
        return rho0, rho1, sg0, sg1, yg0, yg1, ys1, yy0, yy1, yy11

    def load_coef():
        return [coef[idx] for idx in range(1 + 2 * HIST)]

    w2_row = jnp.broadcast_to(wout_ref[...], (hid_rows, LANES))
    w2_col = jnp.sum(jnp.where(eye, w2_row, 0.0), axis=1, keepdims=True)
    theta[:, tail] = jnp.where(lane == 0, w2_col, 0.0)
    w_load.wait()
    for part in col_parts:
        store_split(split_g, part, theta[:, part])
    for idx in range(num_rows // ROW_CHUNK):
        part = pl.ds(idx * ROW_CHUNK, ROW_CHUNK)
        x_loads[idx].wait()
        prod = lax.dot_general(split_g[...], x_v[part, :], (((1,), (1,)), ((), ())), preferred_element_type=F32)
        pre[:, part] = merge3(prod, hid_rows) * in_scale
    pl.semaphore_wait(barrier, n - 1)
    send_logits(z_buf.at[0], 0)
    hist_s[...] = jnp.zeros_like(hist_s)
    hist_y[...] = jnp.zeros_like(hist_y)
    q_s[...] = jnp.zeros_like(q_s)
    q_y[...] = jnp.zeros_like(q_y)
    residual(z_buf.at[0], 0)
    grad[:, tail] = grad_tail()
    for part in col_parts:
        g_part = grad_part(part)
        grad[:, part] = g_part
        store_split(split_g, part, g_part)

    def keep_first(part, val):
        q_g[:, part] = val

    times_x(keep_first)
    store_loss(0)
    coef[...] = jnp.zeros_like(coef)
    coef[0] = jnp.full((SUBL, LANES), -step, F32)

    def slots_at(k):
        return lax.rem(k, HIST), lax.rem(k + 2, HIST), lax.rem(k + 1, HIST)

    def head(k):
        new, old1, old2 = slots_at(k)
        prev = (old1, old2, new)
        cfs = load_coef()
        move(k, cfs, prev)
        send_logits(z_buf.at[1], 1)
        acc_gs = move_rest(cfs, prev)
        residual(z_buf.at[1], 1)
        new_grad((new, old1, old2), acc_gs)
        return new

    def body(k, carry):
        new = head(k)
        new_q(new)
        store_loss(k)
        return two_loop(carry)

    zero = jnp.zeros((SUBL, LANES), F32)
    carry = lax.fori_loop(1, NUM_ITERS - 1, body, (zero,) * 10)

    last = NUM_ITERS - 1
    head(last)
    store_loss(last)
    two_loop(carry)
    new, old1, old2 = (last % HIST, (last + 2) % HIST, (last + 1) % HIST)
    cfs = load_coef()
    slots = (new, old1, old2)
    w2_new = theta[:, tail] + combine(cfs, slots, grad, hist_s, hist_y, tail)
    w2_new = jnp.broadcast_to(w2_new[:, 0:1], (hid_rows, LANES))
    out_w2[...] = jnp.sum(jnp.where(eye, w2_new, 0.0), axis=0, keepdims=True)
    stores = []
    for idx, part in enumerate(col_parts):
        theta[:, part] = theta[:, part] + combine(cfs, slots, grad, hist_s, hist_y, part)
        store = pltpu.make_async_copy(theta.at[:, part], out_w.at[:, part], out_sem.at[idx])
        store.start()
        stores.append(store)
    for store in stores:
        store.wait()


def solution(mesh):
    n = mesh.shape["feat"]

    def local_solve(x_loc, t_loc, win_loc, wout_loc, reg_loc, step_loc):
        num_rows, dim = x_loc.shape
        hid_rows = win_loc.shape[0]
        wide = dim + LANES
        in_scale = 1.0 / math.sqrt(dim)
        out_scale = 1.0 / math.sqrt(hid_rows * n)
        row_tiles = num_rows // LANES
        vmem = pl.BlockSpec(memory_space=pltpu.VMEM)
        smem = pl.BlockSpec(memory_space=pltpu.SMEM)
        anym = pl.BlockSpec(memory_space=pl.ANY)
        new_w, new_w2, losses = pl.pallas_call(
            functools.partial(kernel, "feat", n, in_scale, out_scale),
            out_shape=(
                jax.ShapeDtypeStruct((hid_rows, dim), F32),
                jax.ShapeDtypeStruct((1, hid_rows), F32),
                jax.ShapeDtypeStruct((NUM_ITERS,), F32),
            ),
            in_specs=[anym, vmem, anym, vmem, smem, smem],
            out_specs=(anym, vmem, smem),
            scratch_shapes=[
                pltpu.VMEM((num_rows, dim), BF16),
                pltpu.VMEM((hid_rows, wide), F32),
                pltpu.VMEM((hid_rows, wide), F32),
                pltpu.VMEM((HIST, hid_rows, wide), F32),
                pltpu.VMEM((HIST, hid_rows, wide), F32),
                pltpu.VMEM((hid_rows, num_rows), F32),
                pltpu.VMEM((hid_rows, num_rows), F32),
                pltpu.VMEM((hid_rows, num_rows), F32),
                pltpu.VMEM((HIST, hid_rows, num_rows), F32),
                pltpu.VMEM((HIST, hid_rows, num_rows), F32),
                pltpu.VMEM((hid_rows, num_rows), F32),
                pltpu.VMEM((3 * hid_rows, num_rows), BF16),
                pltpu.VMEM((3 * hid_rows, dim), BF16),
                pltpu.VMEM((row_tiles, LANES), F32),
                pltpu.VMEM((row_tiles, LANES), F32),
                pltpu.VMEM((1 + 2 * HIST, SUBL, LANES), F32),
                pltpu.VMEM((row_tiles, LANES), F32),
                pltpu.VMEM((2, n, row_tiles, LANES), F32),
                pltpu.VMEM((1, LANES), F32),
                pltpu.VMEM((n, 1, LANES), F32),
                pltpu.SemaphoreType.DMA((1 + num_rows // ROW_CHUNK,)),
                pltpu.SemaphoreType.DMA((dim // COL_CHUNK,)),
                pltpu.SemaphoreType.DMA((3,)),
                pltpu.SemaphoreType.DMA((3,)),
            ],
            compiler_params=pltpu.CompilerParams(
                collective_id=0, has_side_effects=True, vmem_limit_bytes=60 * 1024 * 1024
            ),
        )(x_loc, t_loc.reshape(row_tiles, LANES), win_loc, wout_loc.reshape(1, hid_rows), reg_loc, step_loc)
        return new_w, new_w2.reshape(hid_rows), losses

    specs_in = (P("prob", None), P("prob"), P(("prob", "feat"), None), P(("prob", "feat")), P("prob"), P("prob"))
    specs_out = (P(("prob", "feat"), None), P(("prob", "feat")), P("prob"))
    return jax.shard_map(local_solve, mesh=mesh, in_specs=specs_in, out_specs=specs_out, check_vma=False)
```

```python
import functools
import math

import jax
import jax.numpy as jnp
from jax import lax
from jax.experimental import pallas as pl
from jax.experimental.pallas import tpu as pltpu
from jax.sharding import PartitionSpec as P

NUM_ITERS = 6
HIST = 3
LANES = 128
SUBL = 8
ROW_CHUNK = 512
COL_CHUNK = 512
NUM_DOTS = 8
MESH = pl.DeviceIdType.MESH
F32 = jnp.float32
BF16 = jnp.bfloat16


def split3(val):
    high = val.astype(BF16)
    rest = val - high.astype(F32)
    mid = rest.astype(BF16)
    low = (rest - mid.astype(F32)).astype(BF16)
    return high, mid, low


def fold(val):
    rows, cols = val.shape
    part = jnp.sum(val.reshape(rows // SUBL, SUBL, cols), axis=0)
    total = part[:, :LANES]
    for start in range(LANES, cols, LANES):
        total = total + part[:, start : start + LANES]
    return total


def merge3(prod, rows):
    return (prod[2 * rows :] + prod[rows : 2 * rows]) + prod[:rows]


def kernel(
    axis, n, in_scale, out_scale,
    x_hbm, t_hbm, win_hbm, wout_hbm, reg_hbm, step_hbm,
    out_w, out_w2, out_loss,
    t_ref, wout_ref, reg_ref, step_ref,
    x_v, theta, grad, hist_s, hist_y, pre, hid, fac, q_s, q_y, q_g,
    split_d, split_g, resid, logits_v, coef,
    z_src, z_buf, d_src, d_buf,
    load_sem, small_sem, send_sem, recv_sem,
):
    num_rows, dim = x_v.shape
    hid_rows = grad.shape[0]
    row_tiles = num_rows // LANES
    me = lax.axis_index(axis)
    offsets = sorted(range(1, n), key=lambda off: -min(off, n - off))
    peers = [lax.rem(me + off, n) for off in offsets]

    w_load = pltpu.make_async_copy(win_hbm, theta.at[:, pl.ds(0, dim)], load_sem.at[0])
    w_load.start()
    x_loads = []
    for idx in range(num_rows // ROW_CHUNK):
        part = pl.ds(idx * ROW_CHUNK, ROW_CHUNK)
        load = pltpu.make_async_copy(x_hbm.at[part], x_v.at[part], load_sem.at[1 + idx])
        load.start()
        x_loads.append(load)

    smalls = []
    for idx, (src, dst) in enumerate(((t_hbm, t_ref), (wout_hbm, wout_ref), (reg_hbm, reg_ref), (step_hbm, step_ref))):
        load = pltpu.make_async_copy(src, dst, small_sem.at[idx])
        load.start()
        smalls.append(load)

    barrier = pltpu.get_barrier_semaphore()
    for peer in peers:
        pl.semaphore_signal(barrier, inc=1, device_id={axis: peer}, device_id_type=MESH)

    for load in smalls:
        load.wait()
    reg = reg_ref[0]
    step = step_ref[0]
    lane = lax.broadcasted_iota(jnp.int32, (hid_rows, LANES), 1)
    eye = lane == lax.broadcasted_iota(jnp.int32, (hid_rows, LANES), 0)
    col_parts = [pl.ds(start, COL_CHUNK) for start in range(0, dim, COL_CHUNK)]
    tail = pl.ds(dim, LANES)

    def send_all(src, dst, sem):
        for peer in peers:
            pltpu.make_async_remote_copy(
                src_ref=src, dst_ref=dst.at[me], send_sem=send_sem.at[sem], recv_sem=recv_sem.at[sem],
                device_id={axis: peer}, device_id_type=MESH,
            ).start()

    def wait_all(dst, sem):
        others = dst.at[pl.ds(0, n - 1)]
        pltpu.make_async_copy(others, others, recv_sem.at[sem]).wait()
        pltpu.make_async_copy(others, others, send_sem.at[sem]).wait()

    def times_x(out_fn):
        for idx in range(num_rows // ROW_CHUNK):
            part = pl.ds(idx * ROW_CHUNK, ROW_CHUNK)
            prod = lax.dot_general(split_g[...], x_v[part, :], (((1,), (1,)), ((), ())), preferred_element_type=F32)
            out_fn(part, merge3(prod, hid_rows) * in_scale)

    def store_split(ref, part, val):
        for idx, term in enumerate(split3(val)):
            ref[idx * hid_rows : (idx + 1) * hid_rows, part] = term

    def send_logits(buf, sem):
        w2 = jnp.broadcast_to(theta[:, dim : dim + 1], (hid_rows, LANES))
        rows = []
        for idx in range(row_tiles):
            part = pl.ds(idx * LANES, LANES)
            act = jnp.tanh(pre[:, part])
            hid[:, part] = act
            rows.append(jnp.sum(fold(act * w2), axis=0, keepdims=True))
        z_mine = jnp.concatenate(rows, axis=0)
        z_src[...] = z_mine
        buf[me] = z_mine
        send_all(z_src, buf, sem)
        w2s = w2 * (out_scale * in_scale)
        for idx in range(row_tiles):
            part = pl.ds(idx * LANES, LANES)
            act = hid[:, part]
            fac[:, part] = w2s * (1.0 - act * act)

    def residual(buf, sem):
        wait_all(buf, sem)
        logits = jnp.sum(buf[...], axis=0) * out_scale
        logits_v[...] = logits
        resid[...] = (jax.nn.sigmoid(logits) - t_ref[...]) * (1.0 / num_rows)
        for idx in range(row_tiles):
            part = pl.ds(idx * LANES, LANES)
            store_split(split_d, part, fac[:, part] * resid[idx : idx + 1, :])

    def grad_tail():
        total = hid[:, :LANES] * resid[0:1, :]
        for idx in range(1, row_tiles):
            total = total + hid[:, idx * LANES : (idx + 1) * LANES] * resid[idx : idx + 1, :]
        g_out = jnp.sum(total, axis=1, keepdims=True) * out_scale
        return jnp.where(lane == 0, g_out, 0.0) + reg * theta[:, tail]

    def grad_part(part):
        prod = jnp.dot(split_d[...], x_v[:, part], preferred_element_type=F32)
        return merge3(prod, hid_rows) + reg * theta[:, part]

    def store_loss(idx):
        logits = logits_v[...]
        soft = jnp.maximum(logits, 0.0) + jnp.log1p(jnp.exp(-jnp.abs(logits)))
        out_loss[idx] = jnp.sum(soft - t_ref[...] * logits) * (1.0 / num_rows)

    def combine(cfs, slots, vec_g, vec_s, vec_y, part):
        rows, cols = vec_g.shape[0], part.size

        def scaled(cf, val):
            parts = [
                (val[:, start : start + LANES].reshape(rows // SUBL, SUBL, LANES) * cf[None]).reshape(rows, LANES)
                for start in range(0, cols, LANES)
            ]
            return parts[0] if len(parts) == 1 else jnp.concatenate(parts, axis=1)

        total = scaled(cfs[0], vec_g[:, part])
        for idx, slot in enumerate(slots):
            total = total + scaled(cfs[1 + idx], vec_s[slot, :, part])
            total = total + scaled(cfs[1 + HIST + idx], vec_y[slot, :, part])
        return total

    def move(k, cfs, slots):
        slot_new = slots[-1]
        s_part = combine(cfs, slots, grad, hist_s, hist_y, tail)
        hist_s[slot_new, :, tail] = s_part
        theta[:, tail] = theta[:, tail] + s_part
        for idx in range(row_tiles):
            part = pl.ds(idx * LANES, LANES)
            q_part = combine(cfs, slots, q_g, q_s, q_y, part)
            q_s[slot_new, :, part] = q_part
            pre[:, part] = pre[:, part] + q_part

    def move_rest(cfs, slots):
        slot_new = slots[-1]
        acc = fold(grad[:, tail] * hist_s[slot_new, :, tail])
        for part in col_parts:
            s_part = combine(cfs, slots, grad, hist_s, hist_y, part)
            hist_s[slot_new, :, part] = s_part
            theta[:, part] = theta[:, part] + s_part
            acc = acc + fold(grad[:, part] * s_part)
        return acc

    def new_grad(slots, acc_gs):
        new, old1, old2 = slots
        accs = [None] * 7

        def add(part, g_new):
            g_old = grad[:, part]
            y_new = g_new - g_old
            grad[:, part] = g_new
            others = [
                hist_s[new, :, part], hist_s[old1, :, part], hist_s[old2, :, part],
                y_new, hist_y[old1, :, part], hist_y[old2, :, part], g_old,
            ]
            hist_y[new, :, part] = y_new
            for idx, other in enumerate(others):
                term = fold(y_new * other)
                accs[idx] = term if accs[idx] is None else accs[idx] + term

        add(tail, grad_tail())
        for part in col_parts:
            add(part, grad_part(part))
        sums = [jnp.sum(acc, axis=0, keepdims=True) for acc in accs + [acc_gs]]
        totals = jnp.sum(jnp.concatenate(sums, axis=0), axis=1, keepdims=True)
        packed = jnp.sum(jnp.where(eye[:NUM_DOTS], totals, 0.0), axis=0, keepdims=True)
        d_src[...] = packed
        d_buf[me] = packed
        send_all(d_src, d_buf, 2)

    def new_q(slot):
        for part in col_parts:
            store_split(split_g, part, grad[:, part])

        def keep(part, val):
            q_y[slot, :, part] = val - q_g[:, part]
            q_g[:, part] = val

        times_x(keep)

    def two_loop(carry):
        rho1, rho2, psg0, psg1, pyg0, pyg1, pys1, yy11, yy12, yy22 = carry
        wait_all(d_buf, 2)
        total = jnp.sum(d_buf[...], axis=0)
        ys0, ys1, ys2, yy0, yy1, yy2, ygp, gs0 = (
            jnp.broadcast_to(total[:, idx : idx + 1], (SUBL, LANES)) for idx in range(NUM_DOTS)
        )
        sg0, sg1, sg2 = gs0 + ys0, psg0 + ys1, psg1 + ys2
        yg0, yg1, yg2 = ygp + yy0, pyg0 + yy1, pyg1 + yy2
        rho0 = 1.0 / ys0
        gamma = ys0 / yy0
        a0 = rho0 * sg0
        a1 = rho1 * (sg1 - a0 * ys1)
        a2 = rho2 * (sg2 - a0 * ys2 - a1 * pys1)
        yq2 = yg2 - a0 * yy2 - a1 * yy12 - a2 * yy22
        yq1 = yg1 - a0 * yy1 - a1 * yy11 - a2 * yy12
        yq0 = yg0 - a0 * yy0 - a1 * yy1 - a2 * yy2
        c2 = a2 - rho2 * (gamma * yq2)
        c1 = a1 - rho1 * (gamma * yq1 + c2 * pys1)
        c0 = a0 - rho0 * (gamma * yq0 + c2 * ys2 + c1 * ys1)
        sgam = step * gamma
        for idx, val in enumerate((-sgam, -step * c0, -step * c1, -step * c2, sgam * a0, sgam * a1, sgam * a2)):
            coef[idx] = val
        return rho0, rho1, sg0, sg1, yg0, yg1, ys1, yy0, yy1, yy11

    def load_coef():
        return [coef[idx] for idx in range(1 + 2 * HIST)]

    w2_row = jnp.broadcast_to(wout_ref[...], (hid_rows, LANES))
    w2_col = jnp.sum(jnp.where(eye, w2_row, 0.0), axis=1, keepdims=True)
    theta[:, tail] = jnp.where(lane == 0, w2_col, 0.0)
    w_load.wait()
    for part in col_parts:
        store_split(split_g, part, theta[:, part])
    for idx in range(num_rows // ROW_CHUNK):
        part = pl.ds(idx * ROW_CHUNK, ROW_CHUNK)
        x_loads[idx].wait()
        prod = lax.dot_general(split_g[...], x_v[part, :], (((1,), (1,)), ((), ())), preferred_element_type=F32)
        pre[:, part] = merge3(prod, hid_rows) * in_scale
    pl.semaphore_wait(barrier, n - 1)
    send_logits(z_buf.at[0], 0)
    hist_s[...] = jnp.zeros_like(hist_s)
    hist_y[...] = jnp.zeros_like(hist_y)
    q_s[...] = jnp.zeros_like(q_s)
    q_y[...] = jnp.zeros_like(q_y)
    residual(z_buf.at[0], 0)
    grad[:, tail] = grad_tail()
    for part in col_parts:
        g_part = grad_part(part)
        grad[:, part] = g_part
        store_split(split_g, part, g_part)

    def keep_first(part, val):
        q_g[:, part] = val

    times_x(keep_first)
    store_loss(0)
    coef[...] = jnp.zeros_like(coef)
    coef[0] = jnp.full((SUBL, LANES), -step, F32)

    def slots_at(k):
        return lax.rem(k, HIST), lax.rem(k + 2, HIST), lax.rem(k + 1, HIST)

    def head(k):
        new, old1, old2 = slots_at(k)
        prev = (old1, old2, new)
        cfs = load_coef()
        move(k, cfs, prev)
        send_logits(z_buf.at[1], 1)
        acc_gs = move_rest(cfs, prev)
        residual(z_buf.at[1], 1)
        new_grad((new, old1, old2), acc_gs)
        return new

    def body(k, carry):
        new = head(k)
        new_q(new)
        store_loss(k)
        return two_loop(carry)

    zero = jnp.zeros((SUBL, LANES), F32)
    carry = lax.fori_loop(1, NUM_ITERS - 1, body, (zero,) * 10)

    last = NUM_ITERS - 1
    head(last)
    store_loss(last)
    two_loop(carry)
    new, old1, old2 = (last % HIST, (last + 2) % HIST, (last + 1) % HIST)
    cfs = load_coef()
    slots = (new, old1, old2)
    w2_new = theta[:, tail] + combine(cfs, slots, grad, hist_s, hist_y, tail)
    w2_new = jnp.broadcast_to(w2_new[:, 0:1], (hid_rows, LANES))
    out_w2[...] = jnp.sum(jnp.where(eye, w2_new, 0.0), axis=0, keepdims=True)
    for part in col_parts:
        out_w[:, part] = theta[:, part] + combine(cfs, slots, grad, hist_s, hist_y, part)


def write_out(w_ref, w2_ref, loss_ref, out_w, out_w2, out_loss, sems):
    copies = [
        pltpu.make_async_copy(src, dst, sems.at[idx])
        for idx, (src, dst) in enumerate(((w_ref, out_w), (w2_ref, out_w2), (loss_ref, out_loss)))
    ]
    for copy in copies:
        copy.start()
    for copy in copies:
        copy.wait()


def solution(mesh):
    n = mesh.shape["feat"]

    def local_solve(x_loc, t_loc, win_loc, wout_loc, reg_loc, step_loc):
        num_rows, dim = x_loc.shape
        hid_rows = win_loc.shape[0]
        wide = dim + LANES
        in_scale = 1.0 / math.sqrt(dim)
        out_scale = 1.0 / math.sqrt(hid_rows * n)
        row_tiles = num_rows // LANES
        vmem = pl.BlockSpec(memory_space=pltpu.VMEM)
        smem = pl.BlockSpec(memory_space=pltpu.SMEM)
        anym = pl.BlockSpec(memory_space=pl.ANY)
        shapes = ((hid_rows, dim), (1, hid_rows), (NUM_ITERS,))
        solved = pl.pallas_call(
            functools.partial(kernel, "feat", n, in_scale, out_scale),
            out_shape=(pltpu.VMEM(shapes[0], F32), pltpu.VMEM(shapes[1], F32), pltpu.SMEM(shapes[2], F32)),
            in_specs=[anym] * 6,
            out_specs=(vmem, vmem, smem),
            scratch_shapes=[
                pltpu.VMEM((row_tiles, LANES), F32),
                pltpu.VMEM((1, hid_rows), F32),
                pltpu.SMEM((1,), F32),
                pltpu.SMEM((1,), F32),
                pltpu.VMEM((num_rows, dim), BF16),
                pltpu.VMEM((hid_rows, wide), F32),
                pltpu.VMEM((hid_rows, wide), F32),
                pltpu.VMEM((HIST, hid_rows, wide), F32),
                pltpu.VMEM((HIST, hid_rows, wide), F32),
                pltpu.VMEM((hid_rows, num_rows), F32),
                pltpu.VMEM((hid_rows, num_rows), F32),
                pltpu.VMEM((hid_rows, num_rows), F32),
                pltpu.VMEM((HIST, hid_rows, num_rows), F32),
                pltpu.VMEM((HIST, hid_rows, num_rows), F32),
                pltpu.VMEM((hid_rows, num_rows), F32),
                pltpu.VMEM((3 * hid_rows, num_rows), BF16),
                pltpu.VMEM((3 * hid_rows, dim), BF16),
                pltpu.VMEM((row_tiles, LANES), F32),
                pltpu.VMEM((row_tiles, LANES), F32),
                pltpu.VMEM((1 + 2 * HIST, SUBL, LANES), F32),
                pltpu.VMEM((row_tiles, LANES), F32),
                pltpu.VMEM((2, n, row_tiles, LANES), F32),
                pltpu.VMEM((1, LANES), F32),
                pltpu.VMEM((n, 1, LANES), F32),
                pltpu.SemaphoreType.DMA((1 + num_rows // ROW_CHUNK,)),
                pltpu.SemaphoreType.DMA((4,)),
                pltpu.SemaphoreType.DMA((3,)),
                pltpu.SemaphoreType.DMA((3,)),
            ],
            compiler_params=pltpu.CompilerParams(
                collective_id=0, has_side_effects=True, vmem_limit_bytes=61 * 1024 * 1024
            ),
        )(
            *(
                pltpu.with_memory_space_constraint(arg, pltpu.HBM)
                for arg in (x_loc, t_loc.reshape(row_tiles, LANES), win_loc, wout_loc.reshape(1, hid_rows))
            ),
            reg_loc, step_loc,
        )
        new_w, new_w2, losses = pl.pallas_call(
            write_out,
            out_shape=tuple(jax.ShapeDtypeStruct(shape, F32) for shape in shapes),
            in_specs=[vmem, vmem, smem],
            out_specs=(anym, anym, anym),
            scratch_shapes=[pltpu.SemaphoreType.DMA((3,))],
            compiler_params=pltpu.CompilerParams(vmem_limit_bytes=1024 * 1024),
        )(*solved)
        return new_w, new_w2.reshape(hid_rows), losses

    specs_in = (P("prob", None), P("prob"), P(("prob", "feat"), None), P(("prob", "feat")), P("prob"), P("prob"))
    specs_out = (P(("prob", "feat"), None), P(("prob", "feat")), P("prob"))
    return jax.shard_map(local_solve, mesh=mesh, in_specs=specs_in, out_specs=specs_out, check_vma=False)
```

```python
import functools
import math

import jax
import jax.numpy as jnp
from jax import lax
from jax.experimental import pallas as pl
from jax.experimental.pallas import tpu as pltpu
from jax.sharding import PartitionSpec as P

NUM_ITERS = 6
HIST = 3
LANES = 128
SUBL = 8
ROW_CHUNK = 512
COL_CHUNK = 512
NUM_DOTS = 8
MESH = pl.DeviceIdType.MESH
F32 = jnp.float32
BF16 = jnp.bfloat16


def split3(val):
    high = val.astype(BF16)
    rest = val - high.astype(F32)
    mid = rest.astype(BF16)
    low = (rest - mid.astype(F32)).astype(BF16)
    return high, mid, low


def fold(val):
    rows, cols = val.shape
    part = jnp.sum(val.reshape(rows // SUBL, SUBL, cols), axis=0)
    total = part[:, :LANES]
    for start in range(LANES, cols, LANES):
        total = total + part[:, start : start + LANES]
    return total


def merge3(prod, rows):
    return (prod[2 * rows :] + prod[rows : 2 * rows]) + prod[:rows]


def power_of_two(peak):
    scale = jnp.float32(1.0)
    inverse = jnp.float32(1.0)
    for up in (True, False):
        for bits in (64, 32, 16, 8, 4, 2):
            big, small = 2.0**bits, 2.0**-bits
            grow, shrink = (small, big) if up else (big, small)
            hit = (peak >= big) if up else (peak <= small)
            peak = jnp.where(hit, peak * grow, peak)
            inverse = jnp.where(hit, inverse * grow, inverse)
            scale = jnp.where(hit, scale * shrink, scale)
    return scale, inverse


def kernel(
    axis, n, in_scale, out_scale,
    x_hbm, t_hbm, win_hbm, wout_hbm, reg_hbm, step_hbm,
    out_w, out_w2, out_loss,
    t_ref, wout_ref, reg_ref, step_ref,
    x_v, xs, w0, gram, g_parts, pre, pre0, hid, fac, d_old,
    q_s, q_y, q_g, d_s, d_y, d_g, m_s, m_y, m_g, w2, cv,
    split_d, split_w, resid, logits_v, coef,
    z_src, z_buf, dot_src, dot_buf,
    load_sem, small_sem, send_sem, recv_sem,
):
    num_rows, dim = x_v.shape
    hid_rows = w0.shape[0]
    row_tiles = num_rows // LANES
    me = lax.axis_index(axis)
    offsets = sorted(range(1, n), key=lambda off: -min(off, n - off))
    peers = [lax.rem(me + off, n) for off in offsets]

    w_load = pltpu.make_async_copy(win_hbm, w0, load_sem.at[0])
    w_load.start()
    x_loads = []
    row_parts = [pl.ds(start, ROW_CHUNK) for start in range(0, num_rows, ROW_CHUNK)]
    for idx, part in enumerate(row_parts):
        load = pltpu.make_async_copy(x_hbm.at[part], x_v.at[part], load_sem.at[1 + idx])
        load.start()
        x_loads.append(load)
    smalls = []
    for idx, (src, dst) in enumerate(((t_hbm, t_ref), (wout_hbm, wout_ref), (reg_hbm, reg_ref), (step_hbm, step_ref))):
        load = pltpu.make_async_copy(src, dst, small_sem.at[idx])
        load.start()
        smalls.append(load)

    barrier = pltpu.get_barrier_semaphore()
    for peer in peers:
        pl.semaphore_signal(barrier, inc=1, device_id={axis: peer}, device_id_type=MESH)

    for load in smalls:
        load.wait()
    reg = reg_ref[0]
    step = step_ref[0]
    eye = lax.broadcasted_iota(jnp.int32, (hid_rows, LANES), 1) == lax.broadcasted_iota(jnp.int32, (hid_rows, LANES), 0)
    unit = lax.broadcasted_iota(jnp.int32, (SUBL, LANES), 0)
    col_parts = [pl.ds(start, COL_CHUNK) for start in range(0, dim, COL_CHUNK)]
    tiles = [pl.ds(start, LANES) for start in range(0, num_rows, LANES)]
    sums, cfrow, w2rows = pl.ds(0, SUBL), pl.ds(SUBL, SUBL), pl.ds(2 * SUBL, hid_rows)
    top = pl.ds(SUBL, 1)

    def send_all(src, dst, sem):
        for peer in peers:
            pltpu.make_async_remote_copy(
                src_ref=src, dst_ref=dst.at[me], send_sem=send_sem.at[sem], recv_sem=recv_sem.at[sem],
                device_id={axis: peer}, device_id_type=MESH,
            ).start()

    def wait_all(dst, sem):
        others = dst.at[pl.ds(0, n - 1)]
        pltpu.make_async_copy(others, others, recv_sem.at[sem]).wait()
        pltpu.make_async_copy(others, others, send_sem.at[sem]).wait()

    def splat(row):
        return jnp.broadcast_to(row, (SUBL, LANES))

    def store_split(ref, part, val):
        for idx, term in enumerate(split3(val)):
            ref[idx * hid_rows : (idx + 1) * hid_rows, part] = term

    def send_logits(buf, sem):
        rows = []
        for part in tiles:
            act = jnp.tanh(pre[:, part])
            hid[:, part] = act
            rows.append(jnp.sum(fold(act * w2[...]), axis=0, keepdims=True))
        z_mine = jnp.concatenate(rows, axis=0)
        z_src[...] = z_mine
        buf[me] = z_mine
        send_all(z_src, buf, sem)
        w2s = w2[...] * out_scale
        for part in tiles:
            act = hid[:, part]
            fac[:, part] = w2s * (1.0 - act * act)

    def residual(buf, sem):
        wait_all(buf, sem)
        logits = jnp.sum(buf[...], axis=0) * out_scale
        logits_v[...] = logits
        resid[...] = (jax.nn.sigmoid(logits) - t_ref[...]) * (1.0 / num_rows)

    def w2_grad():
        total = hid[:, tiles[0]] * resid[0:1, :]
        for idx in range(1, row_tiles):
            total = total + hid[:, tiles[idx]] * resid[idx : idx + 1, :]
        g_out = jnp.sum(total, axis=1, keepdims=True) * out_scale
        return jnp.broadcast_to(g_out, (hid_rows, LANES)) + reg * w2[...]

    def gram_times(part):
        high = jnp.dot(split_d[...], gram[0, :, part], preferred_element_type=F32)
        mid = jnp.dot(split_d[: 2 * hid_rows], gram[1, :, part], preferred_element_type=F32)
        low = jnp.dot(split_d[:hid_rows], gram[2, :, part], preferred_element_type=F32)
        small = (high[2 * hid_rows :] + mid[hid_rows:]) + low
        return (((high[hid_rows : 2 * hid_rows] + mid[:hid_rows]) + small + high[:hid_rows]) * x_scale) * x_scale

    def keep_g_part(idx):
        for part in col_parts:
            prod = jnp.dot(split_d[...], xs[:, part], preferred_element_type=F32)
            g_parts[idx, :, part] = merge3(prod, hid_rows) * in_scale * x_scale

    def store_loss(idx):
        logits = logits_v[...]
        soft = jnp.maximum(logits, 0.0) + jnp.log1p(jnp.exp(-jnp.abs(logits)))
        out_loss[idx] = jnp.sum(soft - t_ref[...] * logits) * (1.0 / num_rows)

    def combine(cfs, slots, vec_g, vec_s, vec_y, rows, part):
        def scaled(cf, val):
            count = val.shape[0]
            return (val.reshape(count // SUBL, SUBL, LANES) * cf[None]).reshape(count, LANES)

        total = scaled(cfs[0], vec_g[rows, part])
        for idx, slot in enumerate(slots):
            total = total + scaled(cfs[1 + idx], vec_s[slot, rows, part])
            total = total + scaled(cfs[1 + HIST + idx], vec_y[slot, rows, part])
        return total

    every, lanes = pl.ds(0, hid_rows), pl.ds(0, LANES)

    def move(cfs, slots):
        new = slots[-1]
        s_part = combine(cfs, slots, m_g, m_s, m_y, w2rows, lanes)
        m_s[new, w2rows, :] = s_part
        w2[...] = w2[...] + s_part
        for part in tiles:
            q_part = combine(cfs, slots, q_g, q_s, q_y, every, part)
            q_s[new, :, part] = q_part
            pre[:, part] = pre[:, part] + q_part

    def move_rest(cfs, slots):
        new = slots[-1]
        s_part = combine(cfs, slots, m_g, m_s, m_y, pl.ds(0, 2 * SUBL), lanes)
        m_s[new, pl.ds(0, 2 * SUBL), :] = s_part
        cv[...] = cv[...] + s_part[SUBL:]
        acc = splat(m_g[top, :]) * s_part[:SUBL] + fold(m_g[w2rows, :] * m_s[new, w2rows, :]) * (1.0 / LANES)
        for part in tiles:
            d_part = combine(cfs, slots, d_g, d_s, d_y, every, part)
            d_s[new, :, part] = d_part
            acc = acc + fold(d_g[:, part] * q_s[new, :, part])
        return acc

    def new_grad(k, slots, acc_gs):
        new, old1, old2 = slots
        w2_part = w2_grad() - m_g[w2rows, :]
        acc_w0 = jnp.zeros((SUBL, LANES), F32)
        for idx, part in enumerate(tiles):
            d_new = fac[:, part] * resid[idx : idx + 1, :]
            diff = d_new - d_old[:, part]
            d_old[:, part] = d_new
            store_split(split_d, part, diff)
            d_y[new, :, part] = reg * d_s[new, :, part] + diff
            acc_w0 = acc_w0 + fold(diff * pre0[:, part])
        w0_y = reg * m_s[new, sums, :] + acc_w0
        cf_y = reg * m_s[new, cfrow, :] + jnp.where(unit == k + 1, 1.0, 0.0)
        c_y = splat(cf_y[0:1, :])
        m_y[new, sums, :] = w0_y
        m_y[new, cfrow, :] = cf_y
        m_y[new, w2rows, :] = w2_part
        others = [(q_s, m_s, new), (q_s, m_s, old1), (q_s, m_s, old2), (q_y, m_y, old1), (q_y, m_y, old2)]
        accs = [
            c_y * m[slot, sums, :] + fold(w2_part * m[slot, w2rows, :]) * (1.0 / LANES) for _, m, slot in others
        ]
        acc_gp = c_y * m_g[sums, :] + fold(w2_part * m_g[w2rows, :]) * (1.0 / LANES)
        acc_yy = c_y * w0_y + fold(w2_part * w2_part) * (1.0 / LANES)
        for part in row_parts:
            d_part = d_y[new, :, part]
            for idx, (q, _, slot) in enumerate(others):
                accs[idx] = accs[idx] + fold(d_part * q[slot, :, part])
            q_old = q_g[:, part]
            acc_gp = acc_gp + fold(d_part * q_old)
            q_new = reg * q_s[new, :, part] + gram_times(part)
            q_y[new, :, part] = q_new
            q_g[:, part] = q_old + q_new
            acc_yy = acc_yy + fold(d_part * q_new)
        order = accs[:3] + [acc_yy] + accs[3:] + [acc_gp, acc_gs]
        rows = [jnp.sum(acc, axis=0, keepdims=True) for acc in order]
        totals = jnp.sum(jnp.concatenate(rows, axis=0), axis=1, keepdims=True)
        packed = jnp.sum(jnp.where(eye[:NUM_DOTS], totals, 0.0), axis=0, keepdims=True)
        dot_src[...] = packed
        dot_buf[me] = packed
        send_all(dot_src, dot_buf, 2)
        m_g[...] = m_g[...] + m_y[new]
        for part in tiles:
            d_g[:, part] = d_g[:, part] + d_y[new, :, part]

    def two_loop(carry):
        rho1, rho2, psg0, psg1, pyg0, pyg1, pys1, yy11, yy12, yy22 = carry
        wait_all(dot_buf, 2)
        total = jnp.sum(dot_buf[...], axis=0)
        ys0, ys1, ys2, yy0, yy1, yy2, ygp, gs0 = (
            jnp.broadcast_to(total[:, idx : idx + 1], (SUBL, LANES)) for idx in range(NUM_DOTS)
        )
        sg0, sg1, sg2 = gs0 + ys0, psg0 + ys1, psg1 + ys2
        yg0, yg1, yg2 = ygp + yy0, pyg0 + yy1, pyg1 + yy2
        rho0 = 1.0 / ys0
        gamma = ys0 / yy0
        a0 = rho0 * sg0
        a1 = rho1 * (sg1 - a0 * ys1)
        a2 = rho2 * (sg2 - a0 * ys2 - a1 * pys1)
        yq2 = yg2 - a0 * yy2 - a1 * yy12 - a2 * yy22
        yq1 = yg1 - a0 * yy1 - a1 * yy11 - a2 * yy12
        yq0 = yg0 - a0 * yy0 - a1 * yy1 - a2 * yy2
        c2 = a2 - rho2 * (gamma * yq2)
        c1 = a1 - rho1 * (gamma * yq1 + c2 * pys1)
        c0 = a0 - rho0 * (gamma * yq0 + c2 * ys2 + c1 * ys1)
        sgam = step * gamma
        for idx, val in enumerate((-sgam, -step * c0, -step * c1, -step * c2, sgam * a0, sgam * a1, sgam * a2)):
            coef[idx] = val
        return rho0, rho1, sg0, sg1, yg0, yg1, ys1, yy0, yy1, yy11

    def load_coef():
        return [coef[idx] for idx in range(1 + 2 * HIST)]

    w2_row = jnp.broadcast_to(wout_ref[...], (hid_rows, LANES))
    w2_col = jnp.sum(jnp.where(eye, w2_row, 0.0), axis=1, keepdims=True)
    w2[...] = jnp.broadcast_to(w2_col, (hid_rows, LANES))
    w_load.wait()
    w0_w0 = jnp.zeros((SUBL, LANES), F32)
    for part in col_parts:
        w_part = w0[:, part]
        w0_w0 = w0_w0 + fold(w_part * w_part)
        store_split(split_w, part, w_part)
    peaks = []
    for idx, part in enumerate(row_parts):
        x_loads[idx].wait()
        x_part = x_v[part, :]
        prod = lax.dot_general(split_w[...], x_part, (((1,), (1,)), ((), ())), preferred_element_type=F32)
        pre_part = merge3(prod, hid_rows) * in_scale
        pre[:, part] = pre_part
        pre0[:, part] = pre_part
        peaks.append(jnp.max(jnp.abs(x_part).reshape(ROW_CHUNK // 16, 16, dim), axis=0))
    pl.semaphore_wait(barrier, n - 1)
    send_logits(z_buf.at[0], 0)
    x_scale, x_inverse = power_of_two(jnp.max(functools.reduce(jnp.maximum, peaks).astype(F32)))
    for part in row_parts:
        xs[part, :] = x_v[part, :] * jnp.full((ROW_CHUNK, dim), x_inverse, F32).astype(BF16)
    for row, row_part in enumerate(row_parts):
        for col, col_part in enumerate(row_parts[: row + 1]):
            block = lax.dot_general(
                xs[row_part, :], xs[col_part, :], (((1,), (1,)), ((), ())), preferred_element_type=F32
            ) * (in_scale * in_scale)
            for idx, term in enumerate(split3(block)):
                gram[idx, row_part, col_part] = term
            if col < row:
                for idx, term in enumerate(split3(block.T)):
                    gram[idx, col_part, row_part] = term
    for ref in (q_s, q_y, d_s, d_y, m_s, m_y, coef):
        ref[...] = jnp.zeros_like(ref)
    cv[...] = jnp.where(unit == 0, 1.0, 0.0)
    coef[0] = jnp.full((SUBL, LANES), -step, F32)
    residual(z_buf.at[0], 0)
    acc_w0 = reg * w0_w0
    for idx, part in enumerate(tiles):
        d_new = fac[:, part] * resid[idx : idx + 1, :]
        d_old[:, part] = d_new
        d_g[:, part] = d_new
        store_split(split_d, part, d_new)
        acc_w0 = acc_w0 + fold(d_new * pre0[:, part])
    m_g[sums, :] = acc_w0
    m_g[cfrow, :] = reg * cv[...] + jnp.where(unit == 1, 1.0, 0.0)
    m_g[w2rows, :] = w2_grad()
    for part in row_parts:
        q_g[:, part] = reg * pre0[:, part] + gram_times(part)
    store_loss(0)

    def head(k):
        new, old1, old2 = lax.rem(k, HIST), lax.rem(k + 2, HIST), lax.rem(k + 1, HIST)
        prev = (old1, old2, new)
        cfs = load_coef()
        move(cfs, prev)
        send_logits(z_buf.at[1], 1)
        acc_gs = move_rest(cfs, prev)
        keep_g_part(k - 1)
        residual(z_buf.at[1], 1)
        new_grad(k, (new, old1, old2), acc_gs)

    def body(k, carry):
        head(k)
        store_loss(k)
        return two_loop(carry)

    zero = jnp.zeros((SUBL, LANES), F32)
    carry = lax.fori_loop(1, NUM_ITERS - 1, body, (zero,) * 10)

    last = NUM_ITERS - 1
    head(last)
    store_loss(last)
    keep_g_part(last)
    two_loop(carry)
    slots = (last % HIST, (last + 2) % HIST, (last + 1) % HIST)
    cfs = load_coef()
    w2_new = w2[...] + combine(cfs, slots, m_g, m_s, m_y, w2rows, lanes)
    out_w2[...] = jnp.sum(jnp.where(eye, w2_new, 0.0), axis=0, keepdims=True)
    cv_new = cv[...] + combine(cfs, slots, m_g, m_s, m_y, cfrow, lanes)
    weights = [splat(cv_new[idx : idx + 1, :]) for idx in range(1 + NUM_ITERS)]
    for start in range(0, dim, LANES):
        part = pl.ds(start, LANES)

        def weighted(cf, val):
            return (val.reshape(hid_rows // SUBL, SUBL, LANES) * cf[None]).reshape(hid_rows, LANES)

        total = weighted(weights[0], w0[:, part])
        for idx in range(NUM_ITERS):
            total = total + weighted(weights[1 + idx], g_parts[idx, :, part])
        out_w[:, part] = total


def write_out(w_ref, w2_ref, loss_ref, out_w, out_w2, out_loss, sems):
    copies = [
        pltpu.make_async_copy(src, dst, sems.at[idx])
        for idx, (src, dst) in enumerate(((w_ref, out_w), (w2_ref, out_w2), (loss_ref, out_loss)))
    ]
    for copy in copies:
        copy.start()
    for copy in copies:
        copy.wait()


def solution(mesh):
    n = mesh.shape["feat"]

    def local_solve(x_loc, t_loc, win_loc, wout_loc, reg_loc, step_loc):
        num_rows, dim = x_loc.shape
        hid_rows = win_loc.shape[0]
        flat = pltpu.VMEM((hid_rows, num_rows), F32)
        past = pltpu.VMEM((HIST, hid_rows, num_rows), F32)
        meta = 2 * SUBL + hid_rows
        in_scale = 1.0 / math.sqrt(dim)
        out_scale = 1.0 / math.sqrt(hid_rows * n)
        row_tiles = num_rows // LANES
        vmem = pl.BlockSpec(memory_space=pltpu.VMEM)
        smem = pl.BlockSpec(memory_space=pltpu.SMEM)
        anym = pl.BlockSpec(memory_space=pl.ANY)
        shapes = ((hid_rows, dim), (1, hid_rows), (NUM_ITERS,))
        solved = pl.pallas_call(
            functools.partial(kernel, "feat", n, in_scale, out_scale),
            out_shape=(pltpu.VMEM(shapes[0], F32), pltpu.VMEM(shapes[1], F32), pltpu.SMEM(shapes[2], F32)),
            in_specs=[anym] * 6,
            out_specs=(vmem, vmem, smem),
            scratch_shapes=[
                pltpu.VMEM((row_tiles, LANES), F32),
                pltpu.VMEM((1, hid_rows), F32),
                pltpu.SMEM((1,), F32),
                pltpu.SMEM((1,), F32),
                pltpu.VMEM((num_rows, dim), BF16),
                pltpu.VMEM((num_rows, dim), BF16),
                pltpu.VMEM((hid_rows, dim), F32),
                pltpu.VMEM((3, num_rows, num_rows), BF16),
                pltpu.VMEM((NUM_ITERS, hid_rows, dim), F32),
                *([flat] * 5),
                past, past, flat, past, past, flat,
                pltpu.VMEM((HIST, meta, LANES), F32),
                pltpu.VMEM((HIST, meta, LANES), F32),
                pltpu.VMEM((meta, LANES), F32),
                pltpu.VMEM((hid_rows, LANES), F32),
                pltpu.VMEM((SUBL, LANES), F32),
                pltpu.VMEM((3 * hid_rows, num_rows), BF16),
                pltpu.VMEM((3 * hid_rows, dim), BF16),
                pltpu.VMEM((row_tiles, LANES), F32),
                pltpu.VMEM((row_tiles, LANES), F32),
                pltpu.VMEM((1 + 2 * HIST, SUBL, LANES), F32),
                pltpu.VMEM((row_tiles, LANES), F32),
                pltpu.VMEM((2, n, row_tiles, LANES), F32),
                pltpu.VMEM((1, LANES), F32),
                pltpu.VMEM((n, 1, LANES), F32),
                pltpu.SemaphoreType.DMA((1 + num_rows // ROW_CHUNK,)),
                pltpu.SemaphoreType.DMA((4,)),
                pltpu.SemaphoreType.DMA((3,)),
                pltpu.SemaphoreType.DMA((3,)),
            ],
            compiler_params=pltpu.CompilerParams(
                collective_id=0, has_side_effects=True, vmem_limit_bytes=61 * 1024 * 1024
            ),
        )(
            *(
                pltpu.with_memory_space_constraint(arg, pltpu.HBM)
                for arg in (x_loc, t_loc.reshape(row_tiles, LANES), win_loc, wout_loc.reshape(1, hid_rows))
            ),
            reg_loc, step_loc,
        )
        new_w, new_w2, losses = pl.pallas_call(
            write_out,
            out_shape=tuple(jax.ShapeDtypeStruct(shape, F32) for shape in shapes),
            in_specs=[vmem, vmem, smem],
            out_specs=(anym, anym, anym),
            scratch_shapes=[pltpu.SemaphoreType.DMA((3,))],
            compiler_params=pltpu.CompilerParams(vmem_limit_bytes=1024 * 1024),
        )(*solved)
        return new_w, new_w2.reshape(hid_rows), losses

    specs_in = (P("prob", None), P("prob"), P(("prob", "feat"), None), P(("prob", "feat")), P("prob"), P("prob"))
    specs_out = (P(("prob", "feat"), None), P(("prob", "feat")), P("prob"))
    return jax.shard_map(local_solve, mesh=mesh, in_specs=specs_in, out_specs=specs_out, check_vma=False)
```

```python
import functools
import math

import jax
import jax.numpy as jnp
from jax import lax
from jax.experimental import pallas as pl
from jax.experimental.pallas import tpu as pltpu
from jax.sharding import PartitionSpec as P

NUM_ITERS = 6
HIST = 3
LANES = 128
SUBL = 8
ROW_CHUNK = 512
COL_CHUNK = 512
NUM_DOTS = 8
MESH = pl.DeviceIdType.MESH
F32 = jnp.float32
BF16 = jnp.bfloat16


def split3(val):
    high = val.astype(BF16)
    rest = val - high.astype(F32)
    mid = rest.astype(BF16)
    low = (rest - mid.astype(F32)).astype(BF16)
    return high, mid, low


def fold(val):
    rows, cols = val.shape
    part = jnp.sum(val.reshape(rows // SUBL, SUBL, cols), axis=0)
    total = part[:, :LANES]
    for start in range(LANES, cols, LANES):
        total = total + part[:, start : start + LANES]
    return total


def merge3(prod, rows):
    return (prod[2 * rows :] + prod[rows : 2 * rows]) + prod[:rows]


def power_of_two(peak):
    scale = jnp.float32(1.0)
    inverse = jnp.float32(1.0)
    for up in (True, False):
        for bits in (64, 32, 16, 8, 4, 2):
            big, small = 2.0**bits, 2.0**-bits
            grow, shrink = (small, big) if up else (big, small)
            hit = (peak >= big) if up else (peak <= small)
            peak = jnp.where(hit, peak * grow, peak)
            inverse = jnp.where(hit, inverse * grow, inverse)
            scale = jnp.where(hit, scale * shrink, scale)
    return scale, inverse


def kernel(
    axis, n, in_scale, out_scale,
    x_hbm, t_hbm, win_hbm, wout_hbm, reg_hbm, step_hbm,
    w0, g_parts, weights, out_w2, out_loss,
    t_ref, wout_ref, reg_ref, step_ref,
    x_v, xs, gram, pre, pre0, hid, fac, d_old,
    q_s, q_y, q_g, d_s, d_y, d_g, m_s, m_y, m_g, w2, cv,
    split_d, split_w, resid, logits_v, coef,
    z_src, z_buf, dot_src, dot_buf,
    load_sem, small_sem, send_sem, recv_sem,
):
    num_rows, dim = x_v.shape
    hid_rows = w0.shape[0]
    row_tiles = num_rows // LANES
    me = lax.axis_index(axis)
    offsets = sorted(range(1, n), key=lambda off: -min(off, n - off))
    peers = [lax.rem(me + off, n) for off in offsets]

    w_load = pltpu.make_async_copy(win_hbm, w0.at[:, pl.ds(0, dim)], load_sem.at[0])
    w_load.start()
    x_loads = []
    row_parts = [pl.ds(start, ROW_CHUNK) for start in range(0, num_rows, ROW_CHUNK)]
    for idx, part in enumerate(row_parts):
        load = pltpu.make_async_copy(x_hbm.at[part], x_v.at[part], load_sem.at[1 + idx])
        load.start()
        x_loads.append(load)
    smalls = []
    for idx, (src, dst) in enumerate(((t_hbm, t_ref), (wout_hbm, wout_ref), (reg_hbm, reg_ref), (step_hbm, step_ref))):
        load = pltpu.make_async_copy(src, dst, small_sem.at[idx])
        load.start()
        smalls.append(load)

    barrier = pltpu.get_barrier_semaphore()
    for peer in peers:
        pl.semaphore_signal(barrier, inc=1, device_id={axis: peer}, device_id_type=MESH)

    for load in smalls:
        load.wait()
    reg = reg_ref[0]
    step = step_ref[0]
    eye = lax.broadcasted_iota(jnp.int32, (hid_rows, LANES), 1) == lax.broadcasted_iota(jnp.int32, (hid_rows, LANES), 0)
    unit = lax.broadcasted_iota(jnp.int32, (SUBL, LANES), 0)
    col_parts = [pl.ds(start, COL_CHUNK) for start in range(0, dim, COL_CHUNK)]
    tiles = [pl.ds(start, LANES) for start in range(0, num_rows, LANES)]
    sums, cfrow, w2rows = pl.ds(0, SUBL), pl.ds(SUBL, SUBL), pl.ds(2 * SUBL, hid_rows)
    top = pl.ds(SUBL, 1)

    def send_all(src, dst, sem):
        for peer in peers:
            pltpu.make_async_remote_copy(
                src_ref=src, dst_ref=dst.at[me], send_sem=send_sem.at[sem], recv_sem=recv_sem.at[sem],
                device_id={axis: peer}, device_id_type=MESH,
            ).start()

    def wait_all(dst, sem):
        others = dst.at[pl.ds(0, n - 1)]
        pltpu.make_async_copy(others, others, recv_sem.at[sem]).wait()
        pltpu.make_async_copy(others, others, send_sem.at[sem]).wait()

    def splat(row):
        return jnp.broadcast_to(row, (SUBL, LANES))

    def store_split(ref, part, val):
        for idx, term in enumerate(split3(val)):
            ref[idx * hid_rows : (idx + 1) * hid_rows, part] = term

    def send_logits(buf, sem):
        rows = []
        for part in tiles:
            act = jnp.tanh(pre[:, part])
            hid[:, part] = act
            rows.append(jnp.sum(fold(act * w2[...]), axis=0, keepdims=True))
        z_mine = jnp.concatenate(rows, axis=0)
        z_src[...] = z_mine
        buf[me] = z_mine
        send_all(z_src, buf, sem)
        w2s = w2[...] * out_scale
        for part in tiles:
            act = hid[:, part]
            fac[:, part] = w2s * (1.0 - act * act)

    def residual(buf, sem):
        wait_all(buf, sem)
        logits = jnp.sum(buf[...], axis=0) * out_scale
        logits_v[...] = logits
        resid[...] = (jax.nn.sigmoid(logits) - t_ref[...]) * (1.0 / num_rows)

    def w2_grad():
        total = hid[:, tiles[0]] * resid[0:1, :]
        for idx in range(1, row_tiles):
            total = total + hid[:, tiles[idx]] * resid[idx : idx + 1, :]
        g_out = jnp.sum(total, axis=1, keepdims=True) * out_scale
        return jnp.broadcast_to(g_out, (hid_rows, LANES)) + reg * w2[...]

    def gram_times(part):
        high = jnp.dot(split_d[...], gram[0, :, part], preferred_element_type=F32)
        mid = jnp.dot(split_d[: 2 * hid_rows], gram[1, :, part], preferred_element_type=F32)
        low = jnp.dot(split_d[:hid_rows], gram[2, :, part], preferred_element_type=F32)
        small = (high[2 * hid_rows :] + mid[hid_rows:]) + low
        return (((high[hid_rows : 2 * hid_rows] + mid[:hid_rows]) + small + high[:hid_rows]) * x_scale) * x_scale

    def keep_g_part(idx):
        for part in col_parts:
            prod = jnp.dot(split_d[...], xs[:, part], preferred_element_type=F32)
            g_parts[idx, :, part] = merge3(prod, hid_rows) * in_scale * x_scale

    def store_loss(idx):
        logits = logits_v[...]
        soft = jnp.maximum(logits, 0.0) + jnp.log1p(jnp.exp(-jnp.abs(logits)))
        out_loss[idx] = jnp.sum(soft - t_ref[...] * logits) * (1.0 / num_rows)

    def combine(cfs, slots, vec_g, vec_s, vec_y, rows, part):
        def scaled(cf, val):
            count = val.shape[0]
            return (val.reshape(count // SUBL, SUBL, LANES) * cf[None]).reshape(count, LANES)

        total = scaled(cfs[0], vec_g[rows, part])
        for idx, slot in enumerate(slots):
            total = total + scaled(cfs[1 + idx], vec_s[slot, rows, part])
            total = total + scaled(cfs[1 + HIST + idx], vec_y[slot, rows, part])
        return total

    every, lanes = pl.ds(0, hid_rows), pl.ds(0, LANES)

    def move(cfs, slots):
        new = slots[-1]
        s_part = combine(cfs, slots, m_g, m_s, m_y, w2rows, lanes)
        m_s[new, w2rows, :] = s_part
        w2[...] = w2[...] + s_part
        for part in tiles:
            q_part = combine(cfs, slots, q_g, q_s, q_y, every, part)
            q_s[new, :, part] = q_part
            pre[:, part] = pre[:, part] + q_part

    def move_rest(cfs, slots):
        new = slots[-1]
        s_part = combine(cfs, slots, m_g, m_s, m_y, pl.ds(0, 2 * SUBL), lanes)
        m_s[new, pl.ds(0, 2 * SUBL), :] = s_part
        cv[...] = cv[...] + s_part[SUBL:]
        acc = splat(m_g[top, :]) * s_part[:SUBL] + fold(m_g[w2rows, :] * m_s[new, w2rows, :]) * (1.0 / LANES)
        for part in tiles:
            d_part = combine(cfs, slots, d_g, d_s, d_y, every, part)
            d_s[new, :, part] = d_part
            acc = acc + fold(d_g[:, part] * q_s[new, :, part])
        return acc

    def new_grad(k, slots, acc_gs):
        new, old1, old2 = slots
        w2_part = w2_grad() - m_g[w2rows, :]
        acc_w0 = jnp.zeros((SUBL, LANES), F32)
        for idx, part in enumerate(tiles):
            d_new = fac[:, part] * resid[idx : idx + 1, :]
            diff = d_new - d_old[:, part]
            d_old[:, part] = d_new
            store_split(split_d, part, diff)
            d_y[new, :, part] = reg * d_s[new, :, part] + diff
            acc_w0 = acc_w0 + fold(diff * pre0[:, part])
        w0_y = reg * m_s[new, sums, :] + acc_w0
        cf_y = reg * m_s[new, cfrow, :] + jnp.where(unit == k + 1, 1.0, 0.0)
        c_y = splat(cf_y[0:1, :])
        m_y[new, sums, :] = w0_y
        m_y[new, cfrow, :] = cf_y
        m_y[new, w2rows, :] = w2_part
        others = [(q_s, m_s, new), (q_s, m_s, old1), (q_s, m_s, old2), (q_y, m_y, old1), (q_y, m_y, old2)]
        accs = [
            c_y * m[slot, sums, :] + fold(w2_part * m[slot, w2rows, :]) * (1.0 / LANES) for _, m, slot in others
        ]
        acc_gp = c_y * m_g[sums, :] + fold(w2_part * m_g[w2rows, :]) * (1.0 / LANES)
        acc_yy = c_y * w0_y + fold(w2_part * w2_part) * (1.0 / LANES)
        for part in row_parts:
            d_part = d_y[new, :, part]
            for idx, (q, _, slot) in enumerate(others):
                accs[idx] = accs[idx] + fold(d_part * q[slot, :, part])
            q_old = q_g[:, part]
            acc_gp = acc_gp + fold(d_part * q_old)
            q_new = reg * q_s[new, :, part] + gram_times(part)
            q_y[new, :, part] = q_new
            q_g[:, part] = q_old + q_new
            acc_yy = acc_yy + fold(d_part * q_new)
        order = accs[:3] + [acc_yy] + accs[3:] + [acc_gp, acc_gs]
        rows = [jnp.sum(acc, axis=0, keepdims=True) for acc in order]
        totals = jnp.sum(jnp.concatenate(rows, axis=0), axis=1, keepdims=True)
        packed = jnp.sum(jnp.where(eye[:NUM_DOTS], totals, 0.0), axis=0, keepdims=True)
        dot_src[...] = packed
        dot_buf[me] = packed
        send_all(dot_src, dot_buf, 2)
        m_g[...] = m_g[...] + m_y[new]
        for part in tiles:
            d_g[:, part] = d_g[:, part] + d_y[new, :, part]

    def two_loop(carry):
        rho1, rho2, psg0, psg1, pyg0, pyg1, pys1, yy11, yy12, yy22 = carry
        wait_all(dot_buf, 2)
        total = jnp.sum(dot_buf[...], axis=0)
        ys0, ys1, ys2, yy0, yy1, yy2, ygp, gs0 = (
            jnp.broadcast_to(total[:, idx : idx + 1], (SUBL, LANES)) for idx in range(NUM_DOTS)
        )
        sg0, sg1, sg2 = gs0 + ys0, psg0 + ys1, psg1 + ys2
        yg0, yg1, yg2 = ygp + yy0, pyg0 + yy1, pyg1 + yy2
        rho0 = 1.0 / ys0
        gamma = ys0 / yy0
        a0 = rho0 * sg0
        a1 = rho1 * (sg1 - a0 * ys1)
        a2 = rho2 * (sg2 - a0 * ys2 - a1 * pys1)
        yq2 = yg2 - a0 * yy2 - a1 * yy12 - a2 * yy22
        yq1 = yg1 - a0 * yy1 - a1 * yy11 - a2 * yy12
        yq0 = yg0 - a0 * yy0 - a1 * yy1 - a2 * yy2
        c2 = a2 - rho2 * (gamma * yq2)
        c1 = a1 - rho1 * (gamma * yq1 + c2 * pys1)
        c0 = a0 - rho0 * (gamma * yq0 + c2 * ys2 + c1 * ys1)
        sgam = step * gamma
        for idx, val in enumerate((-sgam, -step * c0, -step * c1, -step * c2, sgam * a0, sgam * a1, sgam * a2)):
            coef[idx] = val
        return rho0, rho1, sg0, sg1, yg0, yg1, ys1, yy0, yy1, yy11

    def load_coef():
        return [coef[idx] for idx in range(1 + 2 * HIST)]

    w2_row = jnp.broadcast_to(wout_ref[...], (hid_rows, LANES))
    w2_col = jnp.sum(jnp.where(eye, w2_row, 0.0), axis=1, keepdims=True)
    w2[...] = jnp.broadcast_to(w2_col, (hid_rows, LANES))
    w_load.wait()
    w0_w0 = jnp.zeros((SUBL, LANES), F32)
    for start in range(0, dim, LANES):
        part = pl.ds(start, LANES)
        w_part = w0[:, part]
        w0_w0 = w0_w0 + fold(w_part * w_part)
        store_split(split_w, part, w_part)
    peaks = []
    for idx, part in enumerate(row_parts):
        x_loads[idx].wait()
        x_part = x_v[part, :]
        prod = lax.dot_general(split_w[...], x_part, (((1,), (1,)), ((), ())), preferred_element_type=F32)
        pre_part = merge3(prod, hid_rows) * in_scale
        pre[:, part] = pre_part
        pre0[:, part] = pre_part
        peaks.append(jnp.max(jnp.abs(x_part).reshape(ROW_CHUNK // 16, 16, dim), axis=0))
    pl.semaphore_wait(barrier, n - 1)
    send_logits(z_buf.at[0], 0)
    x_scale, x_inverse = power_of_two(jnp.max(functools.reduce(jnp.maximum, peaks).astype(F32)))
    for part in row_parts:
        xs[part, :] = x_v[part, :] * jnp.full((ROW_CHUNK, dim), x_inverse, F32).astype(BF16)
    for row, row_part in enumerate(row_parts):
        for col, col_part in enumerate(row_parts[: row + 1]):
            block = lax.dot_general(
                xs[row_part, :], xs[col_part, :], (((1,), (1,)), ((), ())), preferred_element_type=F32
            ) * (in_scale * in_scale)
            for idx, term in enumerate(split3(block)):
                gram[idx, row_part, col_part] = term
            if col < row:
                for idx, term in enumerate(split3(block.T)):
                    gram[idx, col_part, row_part] = term
    for ref in (q_s, q_y, d_s, d_y, m_s, m_y, coef):
        ref[...] = jnp.zeros_like(ref)
    cv[...] = jnp.where(unit == 0, 1.0, 0.0)
    coef[0] = jnp.full((SUBL, LANES), -step, F32)
    residual(z_buf.at[0], 0)
    acc_w0 = reg * w0_w0
    for idx, part in enumerate(tiles):
        d_new = fac[:, part] * resid[idx : idx + 1, :]
        d_old[:, part] = d_new
        d_g[:, part] = d_new
        store_split(split_d, part, d_new)
        acc_w0 = acc_w0 + fold(d_new * pre0[:, part])
    m_g[sums, :] = acc_w0
    m_g[cfrow, :] = reg * cv[...] + jnp.where(unit == 1, 1.0, 0.0)
    m_g[w2rows, :] = w2_grad()
    for part in row_parts:
        q_g[:, part] = reg * pre0[:, part] + gram_times(part)
    store_loss(0)

    def head(k):
        new, old1, old2 = lax.rem(k, HIST), lax.rem(k + 2, HIST), lax.rem(k + 1, HIST)
        prev = (old1, old2, new)
        cfs = load_coef()
        move(cfs, prev)
        send_logits(z_buf.at[1], 1)
        acc_gs = move_rest(cfs, prev)
        keep_g_part(k - 1)
        residual(z_buf.at[1], 1)
        new_grad(k, (new, old1, old2), acc_gs)

    def body(k, carry):
        head(k)
        store_loss(k)
        return two_loop(carry)

    zero = jnp.zeros((SUBL, LANES), F32)
    carry = lax.fori_loop(1, NUM_ITERS - 1, body, (zero,) * 10)

    last = NUM_ITERS - 1
    head(last)
    store_loss(last)
    keep_g_part(last)
    two_loop(carry)
    slots = (last % HIST, (last + 2) % HIST, (last + 1) % HIST)
    cfs = load_coef()
    w2_new = w2[...] + combine(cfs, slots, m_g, m_s, m_y, w2rows, lanes)
    out_w2[...] = jnp.sum(jnp.where(eye, w2_new, 0.0), axis=0, keepdims=True)
    cv_new = cv[...] + combine(cfs, slots, m_g, m_s, m_y, cfrow, lanes)
    for idx in range(1 + NUM_ITERS):
        weights[idx] = splat(cv_new[idx : idx + 1, :])


def write_out(w0, g_parts, weights, w2_ref, loss_ref, out_w, out_w2, out_loss, w_v, sems, w_sems):
    rows, dim = out_w.shape
    copies = [
        pltpu.make_async_copy(src, dst, sems.at[idx]) for idx, (src, dst) in enumerate(((w2_ref, out_w2), (loss_ref, out_loss)))
    ]
    for copy in copies:
        copy.start()
    factors = [weights[idx][None] for idx in range(1 + NUM_ITERS)]

    def weighted(factor, val):
        return (val.reshape(rows // SUBL, SUBL, LANES) * factor).reshape(rows, LANES)

    for idx, start in enumerate(range(0, dim, COL_CHUNK)):
        for tile in range(start, start + COL_CHUNK, LANES):
            part = pl.ds(tile, LANES)
            total = weighted(factors[0], w0[:, part])
            for term in range(NUM_ITERS):
                total = total + weighted(factors[1 + term], g_parts[term, :, part])
            w_v[:, part] = total
        part = pl.ds(start, COL_CHUNK)
        copy = pltpu.make_async_copy(w_v.at[:, part], out_w.at[:, part], w_sems.at[idx])
        copy.start()
        copies.append(copy)
    for copy in copies:
        copy.wait()


def solution(mesh):
    n = mesh.shape["feat"]

    def local_solve(x_loc, t_loc, win_loc, wout_loc, reg_loc, step_loc):
        num_rows, dim = x_loc.shape
        hid_rows = win_loc.shape[0]
        flat = pltpu.VMEM((hid_rows, num_rows + LANES), F32)
        past = pltpu.VMEM((HIST, hid_rows, num_rows + LANES), F32)
        meta = 2 * SUBL + hid_rows
        in_scale = 1.0 / math.sqrt(dim)
        out_scale = 1.0 / math.sqrt(hid_rows * n)
        row_tiles = num_rows // LANES
        vmem = pl.BlockSpec(memory_space=pltpu.VMEM)
        smem = pl.BlockSpec(memory_space=pltpu.SMEM)
        anym = pl.BlockSpec(memory_space=pl.ANY)
        solved = pl.pallas_call(
            functools.partial(kernel, "feat", n, in_scale, out_scale),
            out_shape=(
                pltpu.VMEM((hid_rows, dim + LANES), F32),
                pltpu.VMEM((NUM_ITERS, hid_rows, dim + LANES), F32),
                pltpu.VMEM((1 + NUM_ITERS, SUBL, LANES), F32),
                pltpu.VMEM((1, hid_rows), F32),
                pltpu.SMEM((NUM_ITERS,), F32),
            ),
            in_specs=[anym] * 6,
            out_specs=(vmem, vmem, vmem, vmem, smem),
            scratch_shapes=[
                pltpu.VMEM((row_tiles, LANES), F32),
                pltpu.VMEM((1, hid_rows), F32),
                pltpu.SMEM((1,), F32),
                pltpu.SMEM((1,), F32),
                pltpu.VMEM((num_rows, dim), BF16),
                pltpu.VMEM((num_rows, dim), BF16),
                pltpu.VMEM((3, num_rows, num_rows), BF16),
                *([flat] * 5),
                past, past, flat, past, past, flat,
                pltpu.VMEM((HIST, meta, LANES), F32),
                pltpu.VMEM((HIST, meta, LANES), F32),
                pltpu.VMEM((meta, LANES), F32),
                pltpu.VMEM((hid_rows, LANES), F32),
                pltpu.VMEM((SUBL, LANES), F32),
                pltpu.VMEM((3 * hid_rows, num_rows), BF16),
                pltpu.VMEM((3 * hid_rows, dim), BF16),
                pltpu.VMEM((row_tiles, LANES), F32),
                pltpu.VMEM((row_tiles, LANES), F32),
                pltpu.VMEM((1 + 2 * HIST, SUBL, LANES), F32),
                pltpu.VMEM((row_tiles, LANES), F32),
                pltpu.VMEM((2, n, row_tiles, LANES), F32),
                pltpu.VMEM((1, LANES), F32),
                pltpu.VMEM((n, 1, LANES), F32),
                pltpu.SemaphoreType.DMA((1 + num_rows // ROW_CHUNK,)),
                pltpu.SemaphoreType.DMA((4,)),
                pltpu.SemaphoreType.DMA((3,)),
                pltpu.SemaphoreType.DMA((3,)),
            ],
            compiler_params=pltpu.CompilerParams(
                collective_id=0, has_side_effects=True, vmem_limit_bytes=46 * 1024 * 1024
            ),
        )(
            *(
                pltpu.with_memory_space_constraint(arg, pltpu.HBM)
                for arg in (x_loc, t_loc.reshape(row_tiles, LANES), win_loc, wout_loc.reshape(1, hid_rows))
            ),
            reg_loc, step_loc,
        )
        new_w, new_w2, losses = pl.pallas_call(
            write_out,
            out_shape=tuple(jax.ShapeDtypeStruct(shape, F32) for shape in ((hid_rows, dim), (1, hid_rows), (NUM_ITERS,))),
            in_specs=[vmem, vmem, vmem, vmem, smem],
            out_specs=(anym, anym, anym),
            scratch_shapes=[
                pltpu.VMEM((hid_rows, dim + LANES), F32),
                pltpu.SemaphoreType.DMA((2,)),
                pltpu.SemaphoreType.DMA((dim // COL_CHUNK,)),
            ],
            compiler_params=pltpu.CompilerParams(vmem_limit_bytes=4 * 1024 * 1024),
        )(*solved)
        return new_w, new_w2.reshape(hid_rows), losses

    specs_in = (P("prob", None), P("prob"), P(("prob", "feat"), None), P(("prob", "feat")), P("prob"), P("prob"))
    specs_out = (P(("prob", "feat"), None), P(("prob", "feat")), P("prob"))
    return jax.shard_map(local_solve, mesh=mesh, in_specs=specs_in, out_specs=specs_out, check_vma=False)
```

```python
import functools
import math

import jax
import jax.numpy as jnp
from jax import lax
from jax.experimental import pallas as pl
from jax.experimental.pallas import tpu as pltpu
from jax.sharding import PartitionSpec as P

NUM_ITERS = 6
HIST = 3
LANES = 128
SUBL = 8
ROW_CHUNK = 512
COL_CHUNK = 512
NUM_DOTS = 8
MESH = pl.DeviceIdType.MESH
F32 = jnp.float32
BF16 = jnp.bfloat16


def split3(val):
    high = val.astype(BF16)
    rest = val - high.astype(F32)
    mid = rest.astype(BF16)
    low = (rest - mid.astype(F32)).astype(BF16)
    return high, mid, low


def fold(val):
    rows, cols = val.shape
    part = jnp.sum(val.reshape(rows // SUBL, SUBL, cols), axis=0)
    total = part[:, :LANES]
    for start in range(LANES, cols, LANES):
        total = total + part[:, start : start + LANES]
    return total


def merge3(prod, rows):
    return (prod[2 * rows :] + prod[rows : 2 * rows]) + prod[:rows]


def power_of_two(peak):
    scale = jnp.float32(1.0)
    inverse = jnp.float32(1.0)
    for up in (True, False):
        for bits in (64, 32, 16, 8, 4, 2):
            big, small = 2.0**bits, 2.0**-bits
            grow, shrink = (small, big) if up else (big, small)
            hit = (peak >= big) if up else (peak <= small)
            peak = jnp.where(hit, peak * grow, peak)
            inverse = jnp.where(hit, inverse * grow, inverse)
            scale = jnp.where(hit, scale * shrink, scale)
    return scale, inverse


def kernel(
    axis, n, in_scale, out_scale,
    x_hbm, t_hbm, win_hbm, wout_hbm, reg_hbm, step_hbm,
    w0, g_parts, weights, out_w2, out_loss,
    t_ref, wout_ref, reg_ref, step_ref,
    x_v, xs, gram, pre, pre0, hid, fac, d_old,
    q_s, q_y, q_g, d_s, d_y, d_g, m_s, m_y, m_g, w2, cv,
    split_d, split_w, resid, k_part, coef,
    z_src, z_buf, half_src, half_buf, dot_src, dot_buf,
    load_sem, small_sem, send_sem, recv_sem,
):
    num_rows, dim = x_v.shape
    hid_rows = w0.shape[0]
    row_tiles = num_rows // LANES
    half_tiles = row_tiles // 2
    half_rows = num_rows // 2
    me = lax.axis_index(axis)
    own = lax.rem(me, 2)
    partner = me + 1 - 2 * own
    offsets = sorted(range(1, n), key=lambda off: -min(off, n - off))
    peers = [lax.rem(me + off, n) for off in offsets]

    w_load = pltpu.make_async_copy(win_hbm, w0.at[:, pl.ds(0, dim)], load_sem.at[0])
    w_load.start()
    x_loads = []
    row_parts = [pl.ds(start, ROW_CHUNK) for start in range(0, num_rows, ROW_CHUNK)]
    for idx, part in enumerate(row_parts):
        load = pltpu.make_async_copy(x_hbm.at[part], x_v.at[part], load_sem.at[1 + idx])
        load.start()
        x_loads.append(load)
    smalls = []
    for idx, (src, dst) in enumerate(((t_hbm, t_ref), (wout_hbm, wout_ref), (reg_hbm, reg_ref), (step_hbm, step_ref))):
        load = pltpu.make_async_copy(src, dst, small_sem.at[idx])
        load.start()
        smalls.append(load)

    barrier = pltpu.get_barrier_semaphore()
    for peer in peers:
        pl.semaphore_signal(barrier, inc=1, device_id={axis: peer}, device_id_type=MESH)

    for load in smalls:
        load.wait()
    reg = reg_ref[0]
    step = step_ref[0]
    eye = lax.broadcasted_iota(jnp.int32, (hid_rows, LANES), 1) == lax.broadcasted_iota(jnp.int32, (hid_rows, LANES), 0)
    unit = lax.broadcasted_iota(jnp.int32, (SUBL, LANES), 0)
    col_parts = [pl.ds(start, COL_CHUNK) for start in range(0, dim, COL_CHUNK)]
    tiles = [pl.ds(start, LANES) for start in range(0, num_rows, LANES)]
    sums, cfrow, w2rows = pl.ds(0, SUBL), pl.ds(SUBL, SUBL), pl.ds(2 * SUBL, hid_rows)
    top = pl.ds(SUBL, 1)

    def send_all(src, dst, sem):
        for peer in peers:
            pltpu.make_async_remote_copy(
                src_ref=src, dst_ref=dst.at[me], send_sem=send_sem.at[sem], recv_sem=recv_sem.at[sem],
                device_id={axis: peer}, device_id_type=MESH,
            ).start()

    def send_halves(buf, sem):
        for peer in peers:
            pltpu.make_async_remote_copy(
                src_ref=z_src.at[lax.rem(peer, 2)], dst_ref=buf.at[me], send_sem=send_sem.at[sem],
                recv_sem=recv_sem.at[sem], device_id={axis: peer}, device_id_type=MESH,
            ).start()

    def wait_all(dst, sem):
        others = dst.at[pl.ds(0, n - 1)]
        pltpu.make_async_copy(others, others, recv_sem.at[sem]).wait()
        pltpu.make_async_copy(others, others, send_sem.at[sem]).wait()

    def splat(row):
        return jnp.broadcast_to(row, (SUBL, LANES))

    def store_split(ref, part, val):
        for idx, term in enumerate(split3(val)):
            ref[idx * hid_rows : (idx + 1) * hid_rows, part] = term

    def send_logits(buf, sem):
        rows = []
        for part in tiles:
            act = jnp.tanh(pre[:, part])
            hid[:, part] = act
            rows.append(jnp.sum(fold(act * w2[...]), axis=0, keepdims=True))
        z_src[0] = jnp.concatenate(rows[:half_tiles], axis=0)
        z_src[1] = jnp.concatenate(rows[half_tiles:], axis=0)
        buf[me] = z_src[own]
        send_halves(buf, sem)
        w2s = w2[...] * out_scale
        for part in tiles:
            act = hid[:, part]
            fac[:, part] = w2s * (1.0 - act * act)

    def gram_times(buf, sem, on_tile, after_tiles, finish):
        wait_all(buf, sem)
        logits = jnp.sum(buf[...], axis=0) * out_scale
        half_src[...] = logits
        half_buf[own] = logits
        swap = pltpu.make_async_remote_copy(
            src_ref=half_src, dst_ref=half_buf.at[own], send_sem=send_sem.at[3], recv_sem=recv_sem.at[3],
            device_id={axis: partner}, device_id_type=MESH,
        )
        swap.start()
        for slot, half in enumerate((own, 1 - own)):
            if slot:
                swap.wait()
                logits = half_buf[half]
            res = (jax.nn.sigmoid(logits) - t_ref[half]) * (1.0 / num_rows)
            resid[half] = res
            parts = []
            for idx in range(half_tiles):
                part = pl.ds(pl.multiple_of(half * half_rows + idx * LANES, LANES), LANES)
                parts.append(part)
                diff = on_tile(part, fac[:, part] * res[idx : idx + 1, :])
                for row, term in enumerate(split3(diff)):
                    split_d[slot, row * hid_rows : (row + 1) * hid_rows, idx * LANES : (idx + 1) * LANES] = term
            after_tiles(parts)
            rows = pl.ds(pl.multiple_of(half * half_rows, half_rows), half_rows)
            for part in row_parts:
                high = jnp.dot(split_d[slot], gram[0, rows, part], preferred_element_type=F32)
                mid = jnp.dot(split_d[slot, : 2 * hid_rows], gram[1, rows, part], preferred_element_type=F32)
                low = jnp.dot(split_d[slot, :hid_rows], gram[2, rows, part], preferred_element_type=F32)
                small = (high[2 * hid_rows :] + mid[hid_rows:]) + low
                total = ((high[hid_rows : 2 * hid_rows] + mid[:hid_rows]) + small) + high[:hid_rows]
                if slot:
                    finish(part, ((total + k_part[:, part]) * x_scale) * x_scale)
                else:
                    k_part[:, part] = total

    def w2_grad():
        total = hid[:, tiles[0]] * resid[0, 0:1, :]
        for idx in range(1, row_tiles):
            half, row = divmod(idx, half_tiles)
            total = total + hid[:, tiles[idx]] * resid[half, row : row + 1, :]
        g_out = jnp.sum(total, axis=1, keepdims=True) * out_scale
        return jnp.broadcast_to(g_out, (hid_rows, LANES)) + reg * w2[...]

    def keep_g_part(idx):
        for part in col_parts:
            prods = []
            for slot, half in enumerate((own, 1 - own)):
                rows = pl.ds(pl.multiple_of(half * half_rows, half_rows), half_rows)
                prods.append(jnp.dot(split_d[slot], xs[rows, part], preferred_element_type=F32))
            g_parts[idx, :, part] = merge3(prods[0] + prods[1], hid_rows) * in_scale * x_scale

    def store_loss(idx):
        logits = half_buf[...]
        soft = jnp.maximum(logits, 0.0) + jnp.log1p(jnp.exp(-jnp.abs(logits)))
        out_loss[idx] = jnp.sum(soft - t_ref[...] * logits) * (1.0 / num_rows)

    def combine(cfs, slots, vec_g, vec_s, vec_y, rows, part):
        def scaled(cf, val):
            count = val.shape[0]
            return (val.reshape(count // SUBL, SUBL, LANES) * cf[None]).reshape(count, LANES)

        total = scaled(cfs[0], vec_g[rows, part])
        for idx, slot in enumerate(slots):
            total = total + scaled(cfs[1 + idx], vec_s[slot, rows, part])
            total = total + scaled(cfs[1 + HIST + idx], vec_y[slot, rows, part])
        return total

    every, lanes = pl.ds(0, hid_rows), pl.ds(0, LANES)

    def move(cfs, slots):
        new = slots[-1]
        s_part = combine(cfs, slots, m_g, m_s, m_y, w2rows, lanes)
        m_s[new, w2rows, :] = s_part
        w2[...] = w2[...] + s_part
        for part in tiles:
            q_part = combine(cfs, slots, q_g, q_s, q_y, every, part)
            q_s[new, :, part] = q_part
            pre[:, part] = pre[:, part] + q_part

    def move_rest(cfs, slots):
        new = slots[-1]
        s_part = combine(cfs, slots, m_g, m_s, m_y, pl.ds(0, 2 * SUBL), lanes)
        m_s[new, pl.ds(0, 2 * SUBL), :] = s_part
        cv[...] = cv[...] + s_part[SUBL:]
        acc = splat(m_g[top, :]) * s_part[:SUBL] + fold(m_g[w2rows, :] * m_s[new, w2rows, :]) * (1.0 / LANES)
        for part in tiles:
            d_part = combine(cfs, slots, d_g, d_s, d_y, every, part)
            d_s[new, :, part] = d_part
            acc = acc + fold(d_g[:, part] * q_s[new, :, part])
        return acc

    def new_grad(k, slots, acc_gs):
        new, old1, old2 = slots
        others = [(q_s, m_s, new), (q_s, m_s, old1), (q_s, m_s, old2), (q_y, m_y, old1), (q_y, m_y, old2)]
        zero = jnp.zeros((SUBL, LANES), F32)
        accs = [zero] * len(others)
        rest = {"w0": zero, "gp": zero, "yy": zero}

        def on_tile(part, d_new):
            diff = d_new - d_old[:, part]
            d_old[:, part] = d_new
            d_y[new, :, part] = reg * d_s[new, :, part] + diff
            rest["w0"] = rest["w0"] + fold(diff * pre0[:, part])
            return diff

        def after_tiles(parts):
            for part in parts:
                d_part = d_y[new, :, part]
                for idx, (q, _, slot) in enumerate(others):
                    accs[idx] = accs[idx] + fold(d_part * q[slot, :, part])
                rest["gp"] = rest["gp"] + fold(d_part * q_g[:, part])

        def finish(part, val):
            q_new = reg * q_s[new, :, part] + val
            q_y[new, :, part] = q_new
            q_g[:, part] = q_g[:, part] + q_new
            rest["yy"] = rest["yy"] + fold(d_y[new, :, part] * q_new)

        gram_times(z_buf.at[1], 1, on_tile, after_tiles, finish)
        w2_part = w2_grad() - m_g[w2rows, :]
        w0_y = reg * m_s[new, sums, :] + rest["w0"]
        cf_y = reg * m_s[new, cfrow, :] + jnp.where(unit == k + 1, 1.0, 0.0)
        c_y = splat(cf_y[0:1, :])
        m_y[new, sums, :] = w0_y
        m_y[new, cfrow, :] = cf_y
        m_y[new, w2rows, :] = w2_part
        for idx, (_, m, slot) in enumerate(others):
            accs[idx] = accs[idx] + c_y * m[slot, sums, :] + fold(w2_part * m[slot, w2rows, :]) * (1.0 / LANES)
        acc_gp = rest["gp"] + c_y * m_g[sums, :] + fold(w2_part * m_g[w2rows, :]) * (1.0 / LANES)
        acc_yy = rest["yy"] + c_y * w0_y + fold(w2_part * w2_part) * (1.0 / LANES)
        order = accs[:3] + [acc_yy] + accs[3:] + [acc_gp, acc_gs]
        rows = [jnp.sum(acc, axis=0, keepdims=True) for acc in order]
        totals = jnp.sum(jnp.concatenate(rows, axis=0), axis=1, keepdims=True)
        packed = jnp.sum(jnp.where(eye[:NUM_DOTS], totals, 0.0), axis=0, keepdims=True)
        dot_src[...] = packed
        dot_buf[me] = packed
        send_all(dot_src, dot_buf, 2)
        m_g[...] = m_g[...] + m_y[new]
        for part in tiles:
            d_g[:, part] = d_g[:, part] + d_y[new, :, part]

    def two_loop(carry):
        rho1, rho2, psg0, psg1, pyg0, pyg1, pys1, yy11, yy12, yy22 = carry
        wait_all(dot_buf, 2)
        total = jnp.sum(dot_buf[...], axis=0)
        ys0, ys1, ys2, yy0, yy1, yy2, ygp, gs0 = (
            jnp.broadcast_to(total[:, idx : idx + 1], (SUBL, LANES)) for idx in range(NUM_DOTS)
        )
        sg0, sg1, sg2 = gs0 + ys0, psg0 + ys1, psg1 + ys2
        yg0, yg1, yg2 = ygp + yy0, pyg0 + yy1, pyg1 + yy2
        rho0 = 1.0 / ys0
        gamma = ys0 / yy0
        a0 = rho0 * sg0
        a1 = rho1 * (sg1 - a0 * ys1)
        a2 = rho2 * (sg2 - a0 * ys2 - a1 * pys1)
        yq2 = yg2 - a0 * yy2 - a1 * yy12 - a2 * yy22
        yq1 = yg1 - a0 * yy1 - a1 * yy11 - a2 * yy12
        yq0 = yg0 - a0 * yy0 - a1 * yy1 - a2 * yy2
        c2 = a2 - rho2 * (gamma * yq2)
        c1 = a1 - rho1 * (gamma * yq1 + c2 * pys1)
        c0 = a0 - rho0 * (gamma * yq0 + c2 * ys2 + c1 * ys1)
        sgam = step * gamma
        for idx, val in enumerate((-sgam, -step * c0, -step * c1, -step * c2, sgam * a0, sgam * a1, sgam * a2)):
            coef[idx] = val
        return rho0, rho1, sg0, sg1, yg0, yg1, ys1, yy0, yy1, yy11

    def load_coef():
        return [coef[idx] for idx in range(1 + 2 * HIST)]

    w2_row = jnp.broadcast_to(wout_ref[...], (hid_rows, LANES))
    w2_col = jnp.sum(jnp.where(eye, w2_row, 0.0), axis=1, keepdims=True)
    w2[...] = jnp.broadcast_to(w2_col, (hid_rows, LANES))
    w_load.wait()
    w0_w0 = jnp.zeros((SUBL, LANES), F32)
    for start in range(0, dim, LANES):
        part = pl.ds(start, LANES)
        w_part = w0[:, part]
        w0_w0 = w0_w0 + fold(w_part * w_part)
        store_split(split_w, part, w_part)
    peaks = []
    for idx, part in enumerate(row_parts):
        x_loads[idx].wait()
        x_part = x_v[part, :]
        prod = lax.dot_general(split_w[...], x_part, (((1,), (1,)), ((), ())), preferred_element_type=F32)
        pre_part = merge3(prod, hid_rows) * in_scale
        pre[:, part] = pre_part
        pre0[:, part] = pre_part
        peaks.append(jnp.max(jnp.abs(x_part).reshape(ROW_CHUNK // 16, 16, dim), axis=0))
    pl.semaphore_wait(barrier, n - 1)
    send_logits(z_buf.at[0], 0)
    x_scale, x_inverse = power_of_two(jnp.max(functools.reduce(jnp.maximum, peaks).astype(F32)))
    for part in row_parts:
        xs[part, :] = x_v[part, :] * jnp.full((ROW_CHUNK, dim), x_inverse, F32).astype(BF16)
    for row, row_part in enumerate(row_parts):
        for col, col_part in enumerate(row_parts[: row + 1]):
            block = lax.dot_general(
                xs[row_part, :], xs[col_part, :], (((1,), (1,)), ((), ())), preferred_element_type=F32
            ) * (in_scale * in_scale)
            for idx, term in enumerate(split3(block)):
                gram[idx, row_part, col_part] = term
            if col < row:
                for idx, term in enumerate(split3(block.T)):
                    gram[idx, col_part, row_part] = term
    for ref in (q_s, q_y, d_s, d_y, m_s, m_y, coef):
        ref[...] = jnp.zeros_like(ref)
    cv[...] = jnp.where(unit == 0, 1.0, 0.0)
    coef[0] = jnp.full((SUBL, LANES), -step, F32)
    first = {"w0": reg * w0_w0}

    def first_tile(part, d_new):
        d_old[:, part] = d_new
        d_g[:, part] = d_new
        first["w0"] = first["w0"] + fold(d_new * pre0[:, part])
        return d_new

    def first_q(part, val):
        q_g[:, part] = reg * pre0[:, part] + val

    gram_times(z_buf.at[0], 0, first_tile, lambda parts: None, first_q)
    m_g[sums, :] = first["w0"]
    m_g[cfrow, :] = reg * cv[...] + jnp.where(unit == 1, 1.0, 0.0)
    m_g[w2rows, :] = w2_grad()
    store_loss(0)

    def head(k):
        new, old1, old2 = lax.rem(k, HIST), lax.rem(k + 2, HIST), lax.rem(k + 1, HIST)
        prev = (old1, old2, new)
        cfs = load_coef()
        move(cfs, prev)
        send_logits(z_buf.at[1], 1)
        acc_gs = move_rest(cfs, prev)
        keep_g_part(k - 1)
        new_grad(k, (new, old1, old2), acc_gs)

    def body(k, carry):
        head(k)
        store_loss(k)
        return two_loop(carry)

    zero = jnp.zeros((SUBL, LANES), F32)
    carry = lax.fori_loop(1, NUM_ITERS - 1, body, (zero,) * 10)

    last = NUM_ITERS - 1
    head(last)
    store_loss(last)
    keep_g_part(last)
    two_loop(carry)
    slots = (last % HIST, (last + 2) % HIST, (last + 1) % HIST)
    cfs = load_coef()
    w2_new = w2[...] + combine(cfs, slots, m_g, m_s, m_y, w2rows, lanes)
    out_w2[...] = jnp.sum(jnp.where(eye, w2_new, 0.0), axis=0, keepdims=True)
    cv_new = cv[...] + combine(cfs, slots, m_g, m_s, m_y, cfrow, lanes)
    for idx in range(1 + NUM_ITERS):
        weights[idx] = splat(cv_new[idx : idx + 1, :])


def write_out(w0, g_parts, weights, w2_ref, loss_ref, out_w, out_w2, out_loss, w_v, sems, w_sems):
    rows, dim = out_w.shape
    copies = [
        pltpu.make_async_copy(src, dst, sems.at[idx]) for idx, (src, dst) in enumerate(((w2_ref, out_w2), (loss_ref, out_loss)))
    ]
    for copy in copies:
        copy.start()
    factors = [weights[idx][None] for idx in range(1 + NUM_ITERS)]

    def weighted(factor, val):
        return (val.reshape(rows // SUBL, SUBL, LANES) * factor).reshape(rows, LANES)

    for idx, start in enumerate(range(0, dim, COL_CHUNK)):
        for tile in range(start, start + COL_CHUNK, LANES):
            part = pl.ds(tile, LANES)
            total = weighted(factors[0], w0[:, part])
            for term in range(NUM_ITERS):
                total = total + weighted(factors[1 + term], g_parts[term, :, part])
            w_v[:, part] = total
        part = pl.ds(start, COL_CHUNK)
        copy = pltpu.make_async_copy(w_v.at[:, part], out_w.at[:, part], w_sems.at[idx])
        copy.start()
        copies.append(copy)
    for copy in copies:
        copy.wait()


def solution(mesh):
    n = mesh.shape["feat"]

    def local_solve(x_loc, t_loc, win_loc, wout_loc, reg_loc, step_loc):
        num_rows, dim = x_loc.shape
        hid_rows = win_loc.shape[0]
        flat = pltpu.VMEM((hid_rows, num_rows + LANES), F32)
        past = pltpu.VMEM((HIST, hid_rows, num_rows + LANES), F32)
        row_tiles = num_rows // LANES
        halves = pltpu.VMEM((2, row_tiles // 2, LANES), F32)
        meta = 2 * SUBL + hid_rows
        in_scale = 1.0 / math.sqrt(dim)
        out_scale = 1.0 / math.sqrt(hid_rows * n)
        vmem = pl.BlockSpec(memory_space=pltpu.VMEM)
        smem = pl.BlockSpec(memory_space=pltpu.SMEM)
        anym = pl.BlockSpec(memory_space=pl.ANY)
        solved = pl.pallas_call(
            functools.partial(kernel, "feat", n, in_scale, out_scale),
            out_shape=(
                pltpu.VMEM((hid_rows, dim + LANES), F32),
                pltpu.VMEM((NUM_ITERS, hid_rows, dim + LANES), F32),
                pltpu.VMEM((1 + NUM_ITERS, SUBL, LANES), F32),
                pltpu.VMEM((1, hid_rows), F32),
                pltpu.SMEM((NUM_ITERS,), F32),
            ),
            in_specs=[anym] * 6,
            out_specs=(vmem, vmem, vmem, vmem, smem),
            scratch_shapes=[
                halves,
                pltpu.VMEM((1, hid_rows), F32),
                pltpu.SMEM((1,), F32),
                pltpu.SMEM((1,), F32),
                pltpu.VMEM((num_rows, dim), BF16),
                pltpu.VMEM((num_rows, dim), BF16),
                pltpu.VMEM((3, num_rows, num_rows), BF16),
                *([flat] * 5),
                past, past, flat, past, past, flat,
                pltpu.VMEM((HIST, meta, LANES), F32),
                pltpu.VMEM((HIST, meta, LANES), F32),
                pltpu.VMEM((meta, LANES), F32),
                pltpu.VMEM((hid_rows, LANES), F32),
                pltpu.VMEM((SUBL, LANES), F32),
                pltpu.VMEM((2, 3 * hid_rows, num_rows // 2), BF16),
                pltpu.VMEM((3 * hid_rows, dim), BF16),
                halves,
                flat,
                pltpu.VMEM((1 + 2 * HIST, SUBL, LANES), F32),
                halves,
                pltpu.VMEM((2, n, row_tiles // 2, LANES), F32),
                pltpu.VMEM((row_tiles // 2, LANES), F32),
                halves,
                pltpu.VMEM((1, LANES), F32),
                pltpu.VMEM((n, 1, LANES), F32),
                pltpu.SemaphoreType.DMA((1 + num_rows // ROW_CHUNK,)),
                pltpu.SemaphoreType.DMA((4,)),
                pltpu.SemaphoreType.DMA((4,)),
                pltpu.SemaphoreType.DMA((4,)),
            ],
            compiler_params=pltpu.CompilerParams(
                collective_id=0, has_side_effects=True, vmem_limit_bytes=46 * 1024 * 1024
            ),
        )(
            *(
                pltpu.with_memory_space_constraint(arg, pltpu.HBM)
                for arg in (x_loc, t_loc.reshape(2, row_tiles // 2, LANES), win_loc, wout_loc.reshape(1, hid_rows))
            ),
            reg_loc, step_loc,
        )
        new_w, new_w2, losses = pl.pallas_call(
            write_out,
            out_shape=tuple(jax.ShapeDtypeStruct(shape, F32) for shape in ((hid_rows, dim), (1, hid_rows), (NUM_ITERS,))),
            in_specs=[vmem, vmem, vmem, vmem, smem],
            out_specs=(anym, anym, anym),
            scratch_shapes=[
                pltpu.VMEM((hid_rows, dim + LANES), F32),
                pltpu.SemaphoreType.DMA((2,)),
                pltpu.SemaphoreType.DMA((dim // COL_CHUNK,)),
            ],
            compiler_params=pltpu.CompilerParams(vmem_limit_bytes=4 * 1024 * 1024),
        )(*solved)
        return new_w, new_w2.reshape(hid_rows), losses

    specs_in = (P("prob", None), P("prob"), P(("prob", "feat"), None), P(("prob", "feat")), P("prob"), P("prob"))
    specs_out = (P(("prob", "feat"), None), P(("prob", "feat")), P("prob"))
    return jax.shard_map(local_solve, mesh=mesh, in_specs=specs_in, out_specs=specs_out, check_vma=False)
```

```python
import functools
import math

import jax
import jax.numpy as jnp
from jax import lax
from jax.experimental import pallas as pl
from jax.experimental.pallas import tpu as pltpu
from jax.sharding import PartitionSpec as P

NUM_ITERS = 6
HIST = 3
LANES = 128
SUBL = 8
ROW_CHUNK = 512
COL_CHUNK = 512
NUM_DOTS = 8
MESH = pl.DeviceIdType.MESH
F32 = jnp.float32
BF16 = jnp.bfloat16


def split3(val):
    high = val.astype(BF16)
    rest = val - high.astype(F32)
    mid = rest.astype(BF16)
    low = (rest - mid.astype(F32)).astype(BF16)
    return high, mid, low


def fold(val):
    rows, cols = val.shape
    part = jnp.sum(val.reshape(rows // SUBL, SUBL, cols), axis=0)
    total = part[:, :LANES]
    for start in range(LANES, cols, LANES):
        total = total + part[:, start : start + LANES]
    return total


def merge3(prod, rows):
    return (prod[2 * rows :] + prod[rows : 2 * rows]) + prod[:rows]


def power_of_two(peak):
    scale = jnp.float32(1.0)
    inverse = jnp.float32(1.0)
    for up in (True, False):
        for bits in (64, 32, 16, 8, 4, 2):
            big, small = 2.0**bits, 2.0**-bits
            grow, shrink = (small, big) if up else (big, small)
            hit = (peak >= big) if up else (peak <= small)
            peak = jnp.where(hit, peak * grow, peak)
            inverse = jnp.where(hit, inverse * grow, inverse)
            scale = jnp.where(hit, scale * shrink, scale)
    return scale, inverse


def kernel(
    axis, n, in_scale, out_scale,
    x_hbm, t_hbm, win_hbm, wout_hbm, reg_hbm, step_hbm,
    w0, g_parts, weights, out_w2, out_loss,
    t_ref, wout_ref, reg_ref, step_ref,
    x_v, xs, gram, pre, pre0, hid, fac, d_old,
    q_s, q_y, q_g, d_s, d_y, d_g, m_s, m_y, m_g, w2, cv,
    split_d, split_w, resid, logits_v, coef,
    z_src, z_buf, dot_src, dot_buf,
    load_sem, small_sem, send_sem, recv_sem,
):
    num_rows, dim = x_v.shape
    hid_rows = w0.shape[0]
    row_tiles = num_rows // LANES
    me = lax.axis_index(axis)
    offsets = sorted(range(1, n), key=lambda off: -min(off, n - off))
    peers = [lax.rem(me + off, n) for off in offsets]

    w_load = pltpu.make_async_copy(win_hbm, w0.at[:, pl.ds(0, dim)], load_sem.at[0])
    w_load.start()
    x_loads = []
    row_parts = [pl.ds(start, ROW_CHUNK) for start in range(0, num_rows, ROW_CHUNK)]
    for idx, part in enumerate(row_parts):
        load = pltpu.make_async_copy(x_hbm.at[part], x_v.at[part], load_sem.at[1 + idx])
        load.start()
        x_loads.append(load)
    smalls = []
    for idx, (src, dst) in enumerate(((t_hbm, t_ref), (wout_hbm, wout_ref), (reg_hbm, reg_ref), (step_hbm, step_ref))):
        load = pltpu.make_async_copy(src, dst, small_sem.at[idx])
        load.start()
        smalls.append(load)

    barrier = pltpu.get_barrier_semaphore()
    for peer in peers:
        pl.semaphore_signal(barrier, inc=1, device_id={axis: peer}, device_id_type=MESH)

    for load in smalls:
        load.wait()
    reg = reg_ref[0]
    step = step_ref[0]
    eye = lax.broadcasted_iota(jnp.int32, (hid_rows, LANES), 1) == lax.broadcasted_iota(jnp.int32, (hid_rows, LANES), 0)
    unit = lax.broadcasted_iota(jnp.int32, (SUBL, LANES), 0)
    col_parts = [pl.ds(start, COL_CHUNK) for start in range(0, dim, COL_CHUNK)]
    tiles = [pl.ds(start, LANES) for start in range(0, num_rows, LANES)]
    sums, cfrow, w2rows = pl.ds(0, SUBL), pl.ds(SUBL, SUBL), pl.ds(2 * SUBL, hid_rows)
    top = pl.ds(SUBL, 1)

    far = sum(1 for off in offsets if min(off, n - off) > n // 4)

    def send_all(src, dst, sem, targets=peers):
        for peer in targets:
            pltpu.make_async_remote_copy(
                src_ref=src, dst_ref=dst.at[me], send_sem=send_sem.at[sem], recv_sem=recv_sem.at[sem],
                device_id={axis: peer}, device_id_type=MESH,
            ).start()

    def wait_all(dst, sem):
        others = dst.at[pl.ds(0, n - 1)]
        pltpu.make_async_copy(others, others, recv_sem.at[sem]).wait()
        pltpu.make_async_copy(others, others, send_sem.at[sem]).wait()

    def splat(row):
        return jnp.broadcast_to(row, (SUBL, LANES))

    def store_split(ref, part, val):
        for idx, term in enumerate(split3(val)):
            ref[idx * hid_rows : (idx + 1) * hid_rows, part] = term

    def send_logits(buf, sem):
        rows = []
        for part in tiles:
            act = jnp.tanh(pre[:, part])
            hid[:, part] = act
            rows.append(jnp.sum(fold(act * w2[...]), axis=0, keepdims=True))
        z_mine = jnp.concatenate(rows, axis=0)
        z_src[...] = z_mine
        buf[me] = z_mine
        send_all(z_src, buf, sem, peers[:far])
        w2s = w2[...] * out_scale
        for part in tiles:
            act = hid[:, part]
            fac[:, part] = w2s * (1.0 - act * act)

    def residual(buf, sem):
        wait_all(buf, sem)
        logits = jnp.sum(buf[...], axis=0) * out_scale
        logits_v[...] = logits
        resid[...] = (jax.nn.sigmoid(logits) - t_ref[...]) * (1.0 / num_rows)

    def w2_grad():
        total = hid[:, tiles[0]] * resid[0:1, :]
        for idx in range(1, row_tiles):
            total = total + hid[:, tiles[idx]] * resid[idx : idx + 1, :]
        g_out = jnp.sum(total, axis=1, keepdims=True) * out_scale
        return jnp.broadcast_to(g_out, (hid_rows, LANES)) + reg * w2[...]

    def gram_times(part):
        high = jnp.dot(split_d[...], gram[0, :, part], preferred_element_type=F32)
        mid = jnp.dot(split_d[: 2 * hid_rows], gram[1, :, part], preferred_element_type=F32)
        low = jnp.dot(split_d[:hid_rows], gram[2, :, part], preferred_element_type=F32)
        small = (high[2 * hid_rows :] + mid[hid_rows:]) + low
        return (((high[hid_rows : 2 * hid_rows] + mid[:hid_rows]) + small + high[:hid_rows]) * x_scale) * x_scale

    def send_near(buf, sem):
        send_all(z_src, buf, sem, peers[far:])

    def keep_g_part(idx, parts=col_parts):
        for part in parts:
            prod = jnp.dot(split_d[...], xs[:, part], preferred_element_type=F32)
            g_parts[idx, :, part] = merge3(prod, hid_rows) * in_scale * x_scale

    def store_loss(idx):
        logits = logits_v[...]
        soft = jnp.maximum(logits, 0.0) + jnp.log1p(jnp.exp(-jnp.abs(logits)))
        out_loss[idx] = jnp.sum(soft - t_ref[...] * logits) * (1.0 / num_rows)

    def combine(cfs, slots, vec_g, vec_s, vec_y, rows, part):
        def scaled(cf, val):
            count = val.shape[0]
            return (val.reshape(count // SUBL, SUBL, LANES) * cf[None]).reshape(count, LANES)

        total = scaled(cfs[0], vec_g[rows, part])
        for idx, slot in enumerate(slots):
            total = total + scaled(cfs[1 + idx], vec_s[slot, rows, part])
            total = total + scaled(cfs[1 + HIST + idx], vec_y[slot, rows, part])
        return total

    every, lanes = pl.ds(0, hid_rows), pl.ds(0, LANES)

    def move(cfs, slots):
        new = slots[-1]
        s_part = combine(cfs, slots, m_g, m_s, m_y, w2rows, lanes)
        m_s[new, w2rows, :] = s_part
        w2[...] = w2[...] + s_part
        for part in tiles:
            q_part = combine(cfs, slots, q_g, q_s, q_y, every, part)
            q_s[new, :, part] = q_part
            pre[:, part] = pre[:, part] + q_part

    def move_rest(cfs, slots):
        new = slots[-1]
        s_part = combine(cfs, slots, m_g, m_s, m_y, pl.ds(0, 2 * SUBL), lanes)
        m_s[new, pl.ds(0, 2 * SUBL), :] = s_part
        cv[...] = cv[...] + s_part[SUBL:]
        acc = splat(m_g[top, :]) * s_part[:SUBL] + fold(m_g[w2rows, :] * m_s[new, w2rows, :]) * (1.0 / LANES)
        for part in tiles:
            d_part = combine(cfs, slots, d_g, d_s, d_y, every, part)
            d_s[new, :, part] = d_part
            acc = acc + fold(d_g[:, part] * q_s[new, :, part])
        return acc

    def new_grad(k, slots, acc_gs):
        new, old1, old2 = slots
        w2_part = w2_grad() - m_g[w2rows, :]
        acc_w0 = jnp.zeros((SUBL, LANES), F32)
        for idx, part in enumerate(tiles):
            d_new = fac[:, part] * resid[idx : idx + 1, :]
            diff = d_new - d_old[:, part]
            d_old[:, part] = d_new
            store_split(split_d, part, diff)
            d_y[new, :, part] = reg * d_s[new, :, part] + diff
            acc_w0 = acc_w0 + fold(diff * pre0[:, part])
        w0_y = reg * m_s[new, sums, :] + acc_w0
        cf_y = reg * m_s[new, cfrow, :] + jnp.where(unit == k + 1, 1.0, 0.0)
        c_y = splat(cf_y[0:1, :])
        m_y[new, sums, :] = w0_y
        m_y[new, cfrow, :] = cf_y
        m_y[new, w2rows, :] = w2_part
        others = [(q_s, m_s, new), (q_s, m_s, old1), (q_s, m_s, old2), (q_y, m_y, old1), (q_y, m_y, old2)]
        accs = [
            c_y * m[slot, sums, :] + fold(w2_part * m[slot, w2rows, :]) * (1.0 / LANES) for _, m, slot in others
        ]
        acc_gp = c_y * m_g[sums, :] + fold(w2_part * m_g[w2rows, :]) * (1.0 / LANES)
        acc_yy = c_y * w0_y + fold(w2_part * w2_part) * (1.0 / LANES)
        for part in row_parts:
            d_part = d_y[new, :, part]
            for idx, (q, _, slot) in enumerate(others):
                accs[idx] = accs[idx] + fold(d_part * q[slot, :, part])
            q_old = q_g[:, part]
            acc_gp = acc_gp + fold(d_part * q_old)
            q_new = reg * q_s[new, :, part] + gram_times(part)
            q_y[new, :, part] = q_new
            q_g[:, part] = q_old + q_new
            acc_yy = acc_yy + fold(d_part * q_new)
        order = accs[:3] + [acc_yy] + accs[3:] + [acc_gp, acc_gs]
        rows = [jnp.sum(acc, axis=0, keepdims=True) for acc in order]
        totals = jnp.sum(jnp.concatenate(rows, axis=0), axis=1, keepdims=True)
        packed = jnp.sum(jnp.where(eye[:NUM_DOTS], totals, 0.0), axis=0, keepdims=True)
        dot_src[...] = packed
        dot_buf[me] = packed
        send_all(dot_src, dot_buf, 2)
        m_g[...] = m_g[...] + m_y[new]
        for part in tiles:
            d_g[:, part] = d_g[:, part] + d_y[new, :, part]

    def two_loop(carry):
        rho1, rho2, psg0, psg1, pyg0, pyg1, pys1, yy11, yy12, yy22 = carry
        wait_all(dot_buf, 2)
        total = jnp.sum(dot_buf[...], axis=0)
        ys0, ys1, ys2, yy0, yy1, yy2, ygp, gs0 = (
            jnp.broadcast_to(total[:, idx : idx + 1], (SUBL, LANES)) for idx in range(NUM_DOTS)
        )
        sg0, sg1, sg2 = gs0 + ys0, psg0 + ys1, psg1 + ys2
        yg0, yg1, yg2 = ygp + yy0, pyg0 + yy1, pyg1 + yy2
        rho0 = 1.0 / ys0
        gamma = ys0 / yy0
        a0 = rho0 * sg0
        a1 = rho1 * (sg1 - a0 * ys1)
        a2 = rho2 * (sg2 - a0 * ys2 - a1 * pys1)
        yq2 = yg2 - a0 * yy2 - a1 * yy12 - a2 * yy22
        yq1 = yg1 - a0 * yy1 - a1 * yy11 - a2 * yy12
        yq0 = yg0 - a0 * yy0 - a1 * yy1 - a2 * yy2
        c2 = a2 - rho2 * (gamma * yq2)
        c1 = a1 - rho1 * (gamma * yq1 + c2 * pys1)
        c0 = a0 - rho0 * (gamma * yq0 + c2 * ys2 + c1 * ys1)
        sgam = step * gamma
        for idx, val in enumerate((-sgam, -step * c0, -step * c1, -step * c2, sgam * a0, sgam * a1, sgam * a2)):
            coef[idx] = val
        return rho0, rho1, sg0, sg1, yg0, yg1, ys1, yy0, yy1, yy11

    def load_coef():
        return [coef[idx] for idx in range(1 + 2 * HIST)]

    w2_row = jnp.broadcast_to(wout_ref[...], (hid_rows, LANES))
    w2_col = jnp.sum(jnp.where(eye, w2_row, 0.0), axis=1, keepdims=True)
    w2[...] = jnp.broadcast_to(w2_col, (hid_rows, LANES))
    w_load.wait()
    w0_w0 = jnp.zeros((SUBL, LANES), F32)
    for start in range(0, dim, LANES):
        part = pl.ds(start, LANES)
        w_part = w0[:, part]
        w0_w0 = w0_w0 + fold(w_part * w_part)
        store_split(split_w, part, w_part)
    peaks = []
    for idx, part in enumerate(row_parts):
        x_loads[idx].wait()
        x_part = x_v[part, :]
        prod = lax.dot_general(split_w[...], x_part, (((1,), (1,)), ((), ())), preferred_element_type=F32)
        pre_part = merge3(prod, hid_rows) * in_scale
        pre[:, part] = pre_part
        pre0[:, part] = pre_part
        peaks.append(jnp.max(jnp.abs(x_part).reshape(ROW_CHUNK // 16, 16, dim), axis=0))
    pl.semaphore_wait(barrier, n - 1)
    send_logits(z_buf.at[0], 0)
    x_scale, x_inverse = power_of_two(jnp.max(functools.reduce(jnp.maximum, peaks).astype(F32)))
    for part in row_parts:
        xs[part, :] = x_v[part, :] * jnp.full((ROW_CHUNK, dim), x_inverse, F32).astype(BF16)
    send_near(z_buf.at[0], 0)
    for row, row_part in enumerate(row_parts):
        for col, col_part in enumerate(row_parts[: row + 1]):
            block = lax.dot_general(
                xs[row_part, :], xs[col_part, :], (((1,), (1,)), ((), ())), preferred_element_type=F32
            ) * (in_scale * in_scale)
            for idx, term in enumerate(split3(block)):
                gram[idx, row_part, col_part] = term
            if col < row:
                for idx, term in enumerate(split3(block.T)):
                    gram[idx, col_part, row_part] = term
    for ref in (q_s, q_y, d_s, d_y, m_s, m_y, coef):
        ref[...] = jnp.zeros_like(ref)
    cv[...] = jnp.where(unit == 0, 1.0, 0.0)
    coef[0] = jnp.full((SUBL, LANES), -step, F32)
    residual(z_buf.at[0], 0)
    acc_w0 = reg * w0_w0
    for idx, part in enumerate(tiles):
        d_new = fac[:, part] * resid[idx : idx + 1, :]
        d_old[:, part] = d_new
        d_g[:, part] = d_new
        store_split(split_d, part, d_new)
        acc_w0 = acc_w0 + fold(d_new * pre0[:, part])
    m_g[sums, :] = acc_w0
    m_g[cfrow, :] = reg * cv[...] + jnp.where(unit == 1, 1.0, 0.0)
    m_g[w2rows, :] = w2_grad()
    for part in row_parts:
        q_g[:, part] = reg * pre0[:, part] + gram_times(part)
    store_loss(0)

    def head(k):
        new, old1, old2 = lax.rem(k, HIST), lax.rem(k + 2, HIST), lax.rem(k + 1, HIST)
        prev = (old1, old2, new)
        cfs = load_coef()
        move(cfs, prev)
        send_logits(z_buf.at[1], 1)
        acc_gs = move_rest(cfs, prev)
        keep_g_part(k - 1, col_parts[:1])
        send_near(z_buf.at[1], 1)
        keep_g_part(k - 1, col_parts[1:])
        residual(z_buf.at[1], 1)
        new_grad(k, (new, old1, old2), acc_gs)

    def body(k, carry):
        head(k)
        store_loss(k)
        return two_loop(carry)

    zero = jnp.zeros((SUBL, LANES), F32)
    carry = lax.fori_loop(1, NUM_ITERS - 1, body, (zero,) * 10)

    last = NUM_ITERS - 1
    head(last)
    store_loss(last)
    keep_g_part(last)
    two_loop(carry)
    slots = (last % HIST, (last + 2) % HIST, (last + 1) % HIST)
    cfs = load_coef()
    w2_new = w2[...] + combine(cfs, slots, m_g, m_s, m_y, w2rows, lanes)
    out_w2[...] = jnp.sum(jnp.where(eye, w2_new, 0.0), axis=0, keepdims=True)
    cv_new = cv[...] + combine(cfs, slots, m_g, m_s, m_y, cfrow, lanes)
    for idx in range(1 + NUM_ITERS):
        weights[idx] = splat(cv_new[idx : idx + 1, :])


def write_out(w0, g_parts, weights, w2_ref, loss_ref, out_w, out_w2, out_loss, w_v, sems, w_sems):
    rows, dim = out_w.shape
    copies = [
        pltpu.make_async_copy(src, dst, sems.at[idx]) for idx, (src, dst) in enumerate(((w2_ref, out_w2), (loss_ref, out_loss)))
    ]
    for copy in copies:
        copy.start()
    factors = [weights[idx][None] for idx in range(1 + NUM_ITERS)]

    def weighted(factor, val):
        return (val.reshape(rows // SUBL, SUBL, LANES) * factor).reshape(rows, LANES)

    for idx, start in enumerate(range(0, dim, COL_CHUNK)):
        for tile in range(start, start + COL_CHUNK, LANES):
            part = pl.ds(tile, LANES)
            total = weighted(factors[0], w0[:, part])
            for term in range(NUM_ITERS):
                total = total + weighted(factors[1 + term], g_parts[term, :, part])
            w_v[:, part] = total
        part = pl.ds(start, COL_CHUNK)
        copy = pltpu.make_async_copy(w_v.at[:, part], out_w.at[:, part], w_sems.at[idx])
        copy.start()
        copies.append(copy)
    for copy in copies:
        copy.wait()


def solution(mesh):
    n = mesh.shape["feat"]

    def local_solve(x_loc, t_loc, win_loc, wout_loc, reg_loc, step_loc):
        num_rows, dim = x_loc.shape
        hid_rows = win_loc.shape[0]
        flat = pltpu.VMEM((hid_rows, num_rows + LANES), F32)
        past = pltpu.VMEM((HIST, hid_rows, num_rows + LANES), F32)
        meta = 2 * SUBL + hid_rows
        in_scale = 1.0 / math.sqrt(dim)
        out_scale = 1.0 / math.sqrt(hid_rows * n)
        row_tiles = num_rows // LANES
        vmem = pl.BlockSpec(memory_space=pltpu.VMEM)
        smem = pl.BlockSpec(memory_space=pltpu.SMEM)
        anym = pl.BlockSpec(memory_space=pl.ANY)
        solved = pl.pallas_call(
            functools.partial(kernel, "feat", n, in_scale, out_scale),
            out_shape=(
                pltpu.VMEM((hid_rows, dim + LANES), F32),
                pltpu.VMEM((NUM_ITERS, hid_rows, dim + LANES), F32),
                pltpu.VMEM((1 + NUM_ITERS, SUBL, LANES), F32),
                pltpu.VMEM((1, hid_rows), F32),
                pltpu.SMEM((NUM_ITERS,), F32),
            ),
            in_specs=[anym] * 6,
            out_specs=(vmem, vmem, vmem, vmem, smem),
            scratch_shapes=[
                pltpu.VMEM((row_tiles, LANES), F32),
                pltpu.VMEM((1, hid_rows), F32),
                pltpu.SMEM((1,), F32),
                pltpu.SMEM((1,), F32),
                pltpu.VMEM((num_rows, dim), BF16),
                pltpu.VMEM((num_rows, dim), BF16),
                pltpu.VMEM((3, num_rows, num_rows), BF16),
                *([flat] * 5),
                past, past, flat, past, past, flat,
                pltpu.VMEM((HIST, meta, LANES), F32),
                pltpu.VMEM((HIST, meta, LANES), F32),
                pltpu.VMEM((meta, LANES), F32),
                pltpu.VMEM((hid_rows, LANES), F32),
                pltpu.VMEM((SUBL, LANES), F32),
                pltpu.VMEM((3 * hid_rows, num_rows), BF16),
                pltpu.VMEM((3 * hid_rows, dim), BF16),
                pltpu.VMEM((row_tiles, LANES), F32),
                pltpu.VMEM((row_tiles, LANES), F32),
                pltpu.VMEM((1 + 2 * HIST, SUBL, LANES), F32),
                pltpu.VMEM((row_tiles, LANES), F32),
                pltpu.VMEM((2, n, row_tiles, LANES), F32),
                pltpu.VMEM((1, LANES), F32),
                pltpu.VMEM((n, 1, LANES), F32),
                pltpu.SemaphoreType.DMA((1 + num_rows // ROW_CHUNK,)),
                pltpu.SemaphoreType.DMA((4,)),
                pltpu.SemaphoreType.DMA((3,)),
                pltpu.SemaphoreType.DMA((3,)),
            ],
            compiler_params=pltpu.CompilerParams(
                collective_id=0, has_side_effects=True, vmem_limit_bytes=46 * 1024 * 1024
            ),
        )(
            *(
                pltpu.with_memory_space_constraint(arg, pltpu.HBM)
                for arg in (x_loc, t_loc.reshape(row_tiles, LANES), win_loc, wout_loc.reshape(1, hid_rows))
            ),
            reg_loc, step_loc,
        )
        new_w, new_w2, losses = pl.pallas_call(
            write_out,
            out_shape=tuple(jax.ShapeDtypeStruct(shape, F32) for shape in ((hid_rows, dim), (1, hid_rows), (NUM_ITERS,))),
            in_specs=[vmem, vmem, vmem, vmem, smem],
            out_specs=(anym, anym, anym),
            scratch_shapes=[
                pltpu.VMEM((hid_rows, dim + LANES), F32),
                pltpu.SemaphoreType.DMA((2,)),
                pltpu.SemaphoreType.DMA((dim // COL_CHUNK,)),
            ],
            compiler_params=pltpu.CompilerParams(vmem_limit_bytes=4 * 1024 * 1024),
        )(*solved)
        return new_w, new_w2.reshape(hid_rows), losses

    specs_in = (P("prob", None), P("prob"), P(("prob", "feat"), None), P(("prob", "feat")), P("prob"), P("prob"))
    specs_out = (P(("prob", "feat"), None), P(("prob", "feat")), P("prob"))
    return jax.shard_map(local_solve, mesh=mesh, in_specs=specs_in, out_specs=specs_out, check_vma=False)
```

```python
import functools
import math

import jax
import jax.numpy as jnp
from jax import lax
from jax.experimental import pallas as pl
from jax.experimental.pallas import tpu as pltpu
from jax.sharding import PartitionSpec as P

NUM_ITERS = 6
HIST = 3
LANES = 128
SUBL = 8
ROW_CHUNK = 512
COL_CHUNK = 512
NUM_DOTS = 8
MESH = pl.DeviceIdType.MESH
F32 = jnp.float32
BF16 = jnp.bfloat16


def split3(val):
    high = val.astype(BF16)
    rest = val - high.astype(F32)
    mid = rest.astype(BF16)
    low = (rest - mid.astype(F32)).astype(BF16)
    return high, mid, low


def fold(val):
    rows, cols = val.shape
    part = jnp.sum(val.reshape(rows // SUBL, SUBL, cols), axis=0)
    total = part[:, :LANES]
    for start in range(LANES, cols, LANES):
        total = total + part[:, start : start + LANES]
    return total


def merge3(prod, rows):
    return (prod[2 * rows :] + prod[rows : 2 * rows]) + prod[:rows]


def power_of_two(peak):
    scale = jnp.float32(1.0)
    inverse = jnp.float32(1.0)
    for up in (True, False):
        for bits in (64, 32, 16, 8, 4, 2):
            big, small = 2.0**bits, 2.0**-bits
            grow, shrink = (small, big) if up else (big, small)
            hit = (peak >= big) if up else (peak <= small)
            peak = jnp.where(hit, peak * grow, peak)
            inverse = jnp.where(hit, inverse * grow, inverse)
            scale = jnp.where(hit, scale * shrink, scale)
    return scale, inverse


def kernel(
    axis, n, in_scale, out_scale,
    x_hbm, t_hbm, win_hbm, wout_hbm, reg_hbm, step_hbm,
    w0, g_parts, weights, out_w2, out_loss,
    t_ref, wout_ref, reg_ref, step_ref,
    x_v, xs, gram, pre, pre0, hid, fac, d_old,
    q_s, q_y, q_g, d_s, d_y, d_g, m_s, m_y, m_g, w2, cv,
    split_d, split_w, resid, k_part, coef,
    z_src, z_buf, logits_v, dot_src, dot_buf,
    load_sem, small_sem, send_sem, recv_sem,
):
    num_rows, dim = x_v.shape
    hid_rows = w0.shape[0]
    row_tiles = num_rows // LANES
    half_tiles = row_tiles // 2
    half_rows = num_rows // 2
    me = lax.axis_index(axis)
    offsets = sorted(range(1, n), key=lambda off: -min(off, n - off))
    peers = [lax.rem(me + off, n) for off in offsets]

    w_load = pltpu.make_async_copy(win_hbm, w0.at[:, pl.ds(0, dim)], load_sem.at[0])
    w_load.start()
    x_loads = []
    row_parts = [pl.ds(start, ROW_CHUNK) for start in range(0, num_rows, ROW_CHUNK)]
    for idx, part in enumerate(row_parts):
        load = pltpu.make_async_copy(x_hbm.at[part], x_v.at[part], load_sem.at[1 + idx])
        load.start()
        x_loads.append(load)
    smalls = []
    for idx, (src, dst) in enumerate(((t_hbm, t_ref), (wout_hbm, wout_ref), (reg_hbm, reg_ref), (step_hbm, step_ref))):
        load = pltpu.make_async_copy(src, dst, small_sem.at[idx])
        load.start()
        smalls.append(load)

    barrier = pltpu.get_barrier_semaphore()
    for peer in peers:
        pl.semaphore_signal(barrier, inc=1, device_id={axis: peer}, device_id_type=MESH)

    for load in smalls:
        load.wait()
    reg = reg_ref[0]
    step = step_ref[0]
    eye = lax.broadcasted_iota(jnp.int32, (hid_rows, LANES), 1) == lax.broadcasted_iota(jnp.int32, (hid_rows, LANES), 0)
    unit = lax.broadcasted_iota(jnp.int32, (SUBL, LANES), 0)
    col_parts = [pl.ds(start, COL_CHUNK) for start in range(0, dim, COL_CHUNK)]
    tiles = [pl.ds(start, LANES) for start in range(0, num_rows, LANES)]
    sums, cfrow, w2rows = pl.ds(0, SUBL), pl.ds(SUBL, SUBL), pl.ds(2 * SUBL, hid_rows)
    top = pl.ds(SUBL, 1)

    far = sum(1 for off in offsets if min(off, n - off) > n // 4)

    def send_all(src, dst, sem, targets=peers):
        for peer in targets:
            pltpu.make_async_remote_copy(
                src_ref=src, dst_ref=dst.at[me], send_sem=send_sem.at[sem], recv_sem=recv_sem.at[sem],
                device_id={axis: peer}, device_id_type=MESH,
            ).start()

    def wait_all(dst, sem):
        others = dst.at[pl.ds(0, n - 1)]
        pltpu.make_async_copy(others, others, recv_sem.at[sem]).wait()
        pltpu.make_async_copy(others, others, send_sem.at[sem]).wait()

    def splat(row):
        return jnp.broadcast_to(row, (SUBL, LANES))

    def store_split(ref, part, val):
        for idx, term in enumerate(split3(val)):
            ref[idx * hid_rows : (idx + 1) * hid_rows, part] = term

    def send_logits(buf, sem, update=None):
        for half in range(2):
            rows = []
            for part in tiles[half * half_tiles : (half + 1) * half_tiles]:
                if update is not None:
                    update(part)
                act = jnp.tanh(pre[:, part])
                hid[:, part] = act
                rows.append(jnp.sum(fold(act * w2[...]), axis=0, keepdims=True))
            z_mine = jnp.concatenate(rows, axis=0)
            z_src[half] = z_mine
            buf[half, me] = z_mine
            send_all(z_src.at[half], buf.at[half], sem + half, peers[:far])
        for half in range(2):
            send_all(z_src.at[half], buf.at[half], sem + half, peers[far:])
        w2s = w2[...] * out_scale
        for part in tiles:
            act = hid[:, part]
            fac[:, part] = w2s * (1.0 - act * act)

    def gram_times(buf, sem, on_tile, after_tiles, finish):
        for half in range(2):
            wait_all(buf.at[half], sem + half)
            logits = jnp.sum(buf[half], axis=0) * out_scale
            logits_v[half] = logits
            res = (jax.nn.sigmoid(logits) - t_ref[half]) * (1.0 / num_rows)
            resid[half] = res
            parts = tiles[half * half_tiles : (half + 1) * half_tiles]
            for idx, part in enumerate(parts):
                store_split(split_d, part, on_tile(part, fac[:, part] * res[idx : idx + 1, :]))
            after_tiles(parts)
            rows = pl.ds(half * half_rows, half_rows)
            for part in row_parts:
                high = jnp.dot(split_d[:, rows], gram[0, rows, part], preferred_element_type=F32)
                mid = jnp.dot(split_d[: 2 * hid_rows, rows], gram[1, rows, part], preferred_element_type=F32)
                low = jnp.dot(split_d[:hid_rows, rows], gram[2, rows, part], preferred_element_type=F32)
                small = (high[2 * hid_rows :] + mid[hid_rows:]) + low
                total = ((high[hid_rows : 2 * hid_rows] + mid[:hid_rows]) + small) + high[:hid_rows]
                if half:
                    finish(part, ((total + k_part[:, part]) * x_scale) * x_scale)
                else:
                    k_part[:, part] = total

    def w2_grad():
        total = hid[:, tiles[0]] * resid[0, 0:1, :]
        for idx in range(1, row_tiles):
            half, row = divmod(idx, half_tiles)
            total = total + hid[:, tiles[idx]] * resid[half, row : row + 1, :]
        g_out = jnp.sum(total, axis=1, keepdims=True) * out_scale
        return jnp.broadcast_to(g_out, (hid_rows, LANES)) + reg * w2[...]

    def keep_g_part(idx):
        for part in col_parts:
            prod = jnp.dot(split_d[...], xs[:, part], preferred_element_type=F32)
            g_parts[idx, :, part] = merge3(prod, hid_rows) * in_scale * x_scale

    def store_loss(idx):
        logits = logits_v[...]
        soft = jnp.maximum(logits, 0.0) + jnp.log1p(jnp.exp(-jnp.abs(logits)))
        out_loss[idx] = jnp.sum(soft - t_ref[...] * logits) * (1.0 / num_rows)

    def combine(cfs, slots, vec_g, vec_s, vec_y, rows, part):
        def scaled(cf, val):
            count = val.shape[0]
            return (val.reshape(count // SUBL, SUBL, LANES) * cf[None]).reshape(count, LANES)

        total = scaled(cfs[0], vec_g[rows, part])
        for idx, slot in enumerate(slots):
            total = total + scaled(cfs[1 + idx], vec_s[slot, rows, part])
            total = total + scaled(cfs[1 + HIST + idx], vec_y[slot, rows, part])
        return total

    every, lanes = pl.ds(0, hid_rows), pl.ds(0, LANES)

    def move(cfs, slots):
        new = slots[-1]
        s_part = combine(cfs, slots, m_g, m_s, m_y, w2rows, lanes)
        m_s[new, w2rows, :] = s_part
        w2[...] = w2[...] + s_part

        def update(part):
            q_part = combine(cfs, slots, q_g, q_s, q_y, every, part)
            q_s[new, :, part] = q_part
            pre[:, part] = pre[:, part] + q_part

        return update

    def move_rest(cfs, slots):
        new = slots[-1]
        s_part = combine(cfs, slots, m_g, m_s, m_y, pl.ds(0, 2 * SUBL), lanes)
        m_s[new, pl.ds(0, 2 * SUBL), :] = s_part
        cv[...] = cv[...] + s_part[SUBL:]
        acc = splat(m_g[top, :]) * s_part[:SUBL] + fold(m_g[w2rows, :] * m_s[new, w2rows, :]) * (1.0 / LANES)
        for part in tiles:
            d_part = combine(cfs, slots, d_g, d_s, d_y, every, part)
            d_s[new, :, part] = d_part
            acc = acc + fold(d_g[:, part] * q_s[new, :, part])
        return acc

    def new_grad(k, slots, acc_gs):
        new, old1, old2 = slots
        others = [(q_s, m_s, new), (q_s, m_s, old1), (q_s, m_s, old2), (q_y, m_y, old1), (q_y, m_y, old2)]
        zero = jnp.zeros((SUBL, LANES), F32)
        accs = [zero] * len(others)
        rest = {"w0": zero, "gp": zero, "yy": zero}

        def on_tile(part, d_new):
            diff = d_new - d_old[:, part]
            d_old[:, part] = d_new
            d_y[new, :, part] = reg * d_s[new, :, part] + diff
            rest["w0"] = rest["w0"] + fold(diff * pre0[:, part])
            return diff

        def after_tiles(parts):
            for part in parts:
                d_part = d_y[new, :, part]
                for idx, (q, _, slot) in enumerate(others):
                    accs[idx] = accs[idx] + fold(d_part * q[slot, :, part])
                rest["gp"] = rest["gp"] + fold(d_part * q_g[:, part])

        def finish(part, val):
            q_new = reg * q_s[new, :, part] + val
            q_y[new, :, part] = q_new
            q_g[:, part] = q_g[:, part] + q_new
            rest["yy"] = rest["yy"] + fold(d_y[new, :, part] * q_new)

        gram_times(z_buf.at[1], 2, on_tile, after_tiles, finish)
        w2_part = w2_grad() - m_g[w2rows, :]
        w0_y = reg * m_s[new, sums, :] + rest["w0"]
        cf_y = reg * m_s[new, cfrow, :] + jnp.where(unit == k + 1, 1.0, 0.0)
        c_y = splat(cf_y[0:1, :])
        m_y[new, sums, :] = w0_y
        m_y[new, cfrow, :] = cf_y
        m_y[new, w2rows, :] = w2_part
        for idx, (_, m, slot) in enumerate(others):
            accs[idx] = accs[idx] + c_y * m[slot, sums, :] + fold(w2_part * m[slot, w2rows, :]) * (1.0 / LANES)
        acc_gp = rest["gp"] + c_y * m_g[sums, :] + fold(w2_part * m_g[w2rows, :]) * (1.0 / LANES)
        acc_yy = rest["yy"] + c_y * w0_y + fold(w2_part * w2_part) * (1.0 / LANES)
        order = accs[:3] + [acc_yy] + accs[3:] + [acc_gp, acc_gs]
        rows = [jnp.sum(acc, axis=0, keepdims=True) for acc in order]
        totals = jnp.sum(jnp.concatenate(rows, axis=0), axis=1, keepdims=True)
        packed = jnp.sum(jnp.where(eye[:NUM_DOTS], totals, 0.0), axis=0, keepdims=True)
        dot_src[...] = packed
        dot_buf[me] = packed
        send_all(dot_src, dot_buf, 4)
        m_g[...] = m_g[...] + m_y[new]
        for part in tiles:
            d_g[:, part] = d_g[:, part] + d_y[new, :, part]

    def two_loop(carry):
        rho1, rho2, psg0, psg1, pyg0, pyg1, pys1, yy11, yy12, yy22 = carry
        wait_all(dot_buf, 4)
        total = jnp.sum(dot_buf[...], axis=0)
        ys0, ys1, ys2, yy0, yy1, yy2, ygp, gs0 = (
            jnp.broadcast_to(total[:, idx : idx + 1], (SUBL, LANES)) for idx in range(NUM_DOTS)
        )
        sg0, sg1, sg2 = gs0 + ys0, psg0 + ys1, psg1 + ys2
        yg0, yg1, yg2 = ygp + yy0, pyg0 + yy1, pyg1 + yy2
        rho0 = 1.0 / ys0
        gamma = ys0 / yy0
        a0 = rho0 * sg0
        a1 = rho1 * (sg1 - a0 * ys1)
        a2 = rho2 * (sg2 - a0 * ys2 - a1 * pys1)
        yq2 = yg2 - a0 * yy2 - a1 * yy12 - a2 * yy22
        yq1 = yg1 - a0 * yy1 - a1 * yy11 - a2 * yy12
        yq0 = yg0 - a0 * yy0 - a1 * yy1 - a2 * yy2
        c2 = a2 - rho2 * (gamma * yq2)
        c1 = a1 - rho1 * (gamma * yq1 + c2 * pys1)
        c0 = a0 - rho0 * (gamma * yq0 + c2 * ys2 + c1 * ys1)
        sgam = step * gamma
        for idx, val in enumerate((-sgam, -step * c0, -step * c1, -step * c2, sgam * a0, sgam * a1, sgam * a2)):
            coef[idx] = val
        return rho0, rho1, sg0, sg1, yg0, yg1, ys1, yy0, yy1, yy11

    def load_coef():
        return [coef[idx] for idx in range(1 + 2 * HIST)]

    w2_row = jnp.broadcast_to(wout_ref[...], (hid_rows, LANES))
    w2_col = jnp.sum(jnp.where(eye, w2_row, 0.0), axis=1, keepdims=True)
    w2[...] = jnp.broadcast_to(w2_col, (hid_rows, LANES))
    w_load.wait()
    w0_w0 = jnp.zeros((SUBL, LANES), F32)
    for start in range(0, dim, LANES):
        part = pl.ds(start, LANES)
        w_part = w0[:, part]
        w0_w0 = w0_w0 + fold(w_part * w_part)
        store_split(split_w, part, w_part)
    peaks = []
    for idx, part in enumerate(row_parts):
        x_loads[idx].wait()
        x_part = x_v[part, :]
        prod = lax.dot_general(split_w[...], x_part, (((1,), (1,)), ((), ())), preferred_element_type=F32)
        pre_part = merge3(prod, hid_rows) * in_scale
        pre[:, part] = pre_part
        pre0[:, part] = pre_part
        peaks.append(jnp.max(jnp.abs(x_part).reshape(ROW_CHUNK // 16, 16, dim), axis=0))
    pl.semaphore_wait(barrier, n - 1)
    send_logits(z_buf.at[0], 0)
    x_scale, x_inverse = power_of_two(jnp.max(functools.reduce(jnp.maximum, peaks).astype(F32)))
    for part in row_parts:
        xs[part, :] = x_v[part, :] * jnp.full((ROW_CHUNK, dim), x_inverse, F32).astype(BF16)
    for row, row_part in enumerate(row_parts):
        for col, col_part in enumerate(row_parts[: row + 1]):
            block = lax.dot_general(
                xs[row_part, :], xs[col_part, :], (((1,), (1,)), ((), ())), preferred_element_type=F32
            ) * (in_scale * in_scale)
            for idx, term in enumerate(split3(block)):
                gram[idx, row_part, col_part] = term
            if col < row:
                for idx, term in enumerate(split3(block.T)):
                    gram[idx, col_part, row_part] = term
    for ref in (q_s, q_y, d_s, d_y, m_s, m_y, coef):
        ref[...] = jnp.zeros_like(ref)
    cv[...] = jnp.where(unit == 0, 1.0, 0.0)
    coef[0] = jnp.full((SUBL, LANES), -step, F32)
    first = {"w0": reg * w0_w0}

    def first_tile(part, d_new):
        d_old[:, part] = d_new
        d_g[:, part] = d_new
        first["w0"] = first["w0"] + fold(d_new * pre0[:, part])
        return d_new

    def first_q(part, val):
        q_g[:, part] = reg * pre0[:, part] + val

    gram_times(z_buf.at[0], 0, first_tile, lambda parts: None, first_q)
    m_g[sums, :] = first["w0"]
    m_g[cfrow, :] = reg * cv[...] + jnp.where(unit == 1, 1.0, 0.0)
    m_g[w2rows, :] = w2_grad()
    store_loss(0)

    def head(k):
        new, old1, old2 = lax.rem(k, HIST), lax.rem(k + 2, HIST), lax.rem(k + 1, HIST)
        prev = (old1, old2, new)
        cfs = load_coef()
        send_logits(z_buf.at[1], 2, move(cfs, prev))
        acc_gs = move_rest(cfs, prev)
        keep_g_part(k - 1)
        new_grad(k, (new, old1, old2), acc_gs)

    def body(k, carry):
        head(k)
        store_loss(k)
        return two_loop(carry)

    zero = jnp.zeros((SUBL, LANES), F32)
    carry = lax.fori_loop(1, NUM_ITERS - 1, body, (zero,) * 10)

    last = NUM_ITERS - 1
    head(last)
    store_loss(last)
    keep_g_part(last)
    two_loop(carry)
    slots = (last % HIST, (last + 2) % HIST, (last + 1) % HIST)
    cfs = load_coef()
    w2_new = w2[...] + combine(cfs, slots, m_g, m_s, m_y, w2rows, lanes)
    out_w2[...] = jnp.sum(jnp.where(eye, w2_new, 0.0), axis=0, keepdims=True)
    cv_new = cv[...] + combine(cfs, slots, m_g, m_s, m_y, cfrow, lanes)
    for idx in range(1 + NUM_ITERS):
        weights[idx] = splat(cv_new[idx : idx + 1, :])


def write_out(w0, g_parts, weights, w2_ref, loss_ref, out_w, out_w2, out_loss, w_v, sems, w_sems):
    rows, dim = out_w.shape
    copies = [
        pltpu.make_async_copy(src, dst, sems.at[idx]) for idx, (src, dst) in enumerate(((w2_ref, out_w2), (loss_ref, out_loss)))
    ]
    for copy in copies:
        copy.start()
    factors = [weights[idx][None] for idx in range(1 + NUM_ITERS)]

    def weighted(factor, val):
        return (val.reshape(rows // SUBL, SUBL, LANES) * factor).reshape(rows, LANES)

    for idx, start in enumerate(range(0, dim, COL_CHUNK)):
        for tile in range(start, start + COL_CHUNK, LANES):
            part = pl.ds(tile, LANES)
            total = weighted(factors[0], w0[:, part])
            for term in range(NUM_ITERS):
                total = total + weighted(factors[1 + term], g_parts[term, :, part])
            w_v[:, part] = total
        part = pl.ds(start, COL_CHUNK)
        copy = pltpu.make_async_copy(w_v.at[:, part], out_w.at[:, part], w_sems.at[idx])
        copy.start()
        copies.append(copy)
    for copy in copies:
        copy.wait()


def solution(mesh):
    n = mesh.shape["feat"]

    def local_solve(x_loc, t_loc, win_loc, wout_loc, reg_loc, step_loc):
        num_rows, dim = x_loc.shape
        hid_rows = win_loc.shape[0]
        flat = pltpu.VMEM((hid_rows, num_rows + LANES), F32)
        past = pltpu.VMEM((HIST, hid_rows, num_rows + LANES), F32)
        row_tiles = num_rows // LANES
        halves = pltpu.VMEM((2, row_tiles // 2, LANES), F32)
        meta = 2 * SUBL + hid_rows
        in_scale = 1.0 / math.sqrt(dim)
        out_scale = 1.0 / math.sqrt(hid_rows * n)
        vmem = pl.BlockSpec(memory_space=pltpu.VMEM)
        smem = pl.BlockSpec(memory_space=pltpu.SMEM)
        anym = pl.BlockSpec(memory_space=pl.ANY)
        solved = pl.pallas_call(
            functools.partial(kernel, "feat", n, in_scale, out_scale),
            out_shape=(
                pltpu.VMEM((hid_rows, dim + LANES), F32),
                pltpu.VMEM((NUM_ITERS, hid_rows, dim + LANES), F32),
                pltpu.VMEM((1 + NUM_ITERS, SUBL, LANES), F32),
                pltpu.VMEM((1, hid_rows), F32),
                pltpu.SMEM((NUM_ITERS,), F32),
            ),
            in_specs=[anym] * 6,
            out_specs=(vmem, vmem, vmem, vmem, smem),
            scratch_shapes=[
                halves,
                pltpu.VMEM((1, hid_rows), F32),
                pltpu.SMEM((1,), F32),
                pltpu.SMEM((1,), F32),
                pltpu.VMEM((num_rows, dim), BF16),
                pltpu.VMEM((num_rows, dim), BF16),
                pltpu.VMEM((3, num_rows, num_rows), BF16),
                *([flat] * 5),
                past, past, flat, past, past, flat,
                pltpu.VMEM((HIST, meta, LANES), F32),
                pltpu.VMEM((HIST, meta, LANES), F32),
                pltpu.VMEM((meta, LANES), F32),
                pltpu.VMEM((hid_rows, LANES), F32),
                pltpu.VMEM((SUBL, LANES), F32),
                pltpu.VMEM((3 * hid_rows, num_rows), BF16),
                pltpu.VMEM((3 * hid_rows, dim), BF16),
                halves,
                flat,
                pltpu.VMEM((1 + 2 * HIST, SUBL, LANES), F32),
                halves,
                pltpu.VMEM((2, 2, n, row_tiles // 2, LANES), F32),
                halves,
                pltpu.VMEM((1, LANES), F32),
                pltpu.VMEM((n, 1, LANES), F32),
                pltpu.SemaphoreType.DMA((1 + num_rows // ROW_CHUNK,)),
                pltpu.SemaphoreType.DMA((4,)),
                pltpu.SemaphoreType.DMA((5,)),
                pltpu.SemaphoreType.DMA((5,)),
            ],
            compiler_params=pltpu.CompilerParams(
                collective_id=0, has_side_effects=True, vmem_limit_bytes=46 * 1024 * 1024
            ),
        )(
            *(
                pltpu.with_memory_space_constraint(arg, pltpu.HBM)
                for arg in (x_loc, t_loc.reshape(2, row_tiles // 2, LANES), win_loc, wout_loc.reshape(1, hid_rows))
            ),
            reg_loc, step_loc,
        )
        new_w, new_w2, losses = pl.pallas_call(
            write_out,
            out_shape=tuple(jax.ShapeDtypeStruct(shape, F32) for shape in ((hid_rows, dim), (1, hid_rows), (NUM_ITERS,))),
            in_specs=[vmem, vmem, vmem, vmem, smem],
            out_specs=(anym, anym, anym),
            scratch_shapes=[
                pltpu.VMEM((hid_rows, dim + LANES), F32),
                pltpu.SemaphoreType.DMA((2,)),
                pltpu.SemaphoreType.DMA((dim // COL_CHUNK,)),
            ],
            compiler_params=pltpu.CompilerParams(vmem_limit_bytes=4 * 1024 * 1024),
        )(*solved)
        return new_w, new_w2.reshape(hid_rows), losses

    specs_in = (P("prob", None), P("prob"), P(("prob", "feat"), None), P(("prob", "feat")), P("prob"), P("prob"))
    specs_out = (P(("prob", "feat"), None), P(("prob", "feat")), P("prob"))
    return jax.shard_map(local_solve, mesh=mesh, in_specs=specs_in, out_specs=specs_out, check_vma=False)
```

```python
import functools
import math

import jax
import jax.numpy as jnp
from jax import lax
from jax.experimental import pallas as pl
from jax.experimental.pallas import tpu as pltpu
from jax.sharding import PartitionSpec as P

NUM_ITERS = 6
HIST = 3
LANES = 128
SUBL = 8
ROW_CHUNK = 512
COL_CHUNK = 512
G_TRIPS = 3
NUM_DOTS = 8
MESH = pl.DeviceIdType.MESH
F32 = jnp.float32
BF16 = jnp.bfloat16


def split3(val):
    high = val.astype(BF16)
    rest = val - high.astype(F32)
    mid = rest.astype(BF16)
    low = (rest - mid.astype(F32)).astype(BF16)
    return high, mid, low


def fold(val):
    rows, cols = val.shape
    part = jnp.sum(val.reshape(rows // SUBL, SUBL, cols), axis=0)
    total = part[:, :LANES]
    for start in range(LANES, cols, LANES):
        total = total + part[:, start : start + LANES]
    return total


def merge3(prod, rows):
    return (prod[2 * rows :] + prod[rows : 2 * rows]) + prod[:rows]


def power_of_two(peak):
    scale = jnp.float32(1.0)
    inverse = jnp.float32(1.0)
    for up in (True, False):
        for bits in (64, 32, 16, 8, 4, 2):
            big, small = 2.0**bits, 2.0**-bits
            grow, shrink = (small, big) if up else (big, small)
            hit = (peak >= big) if up else (peak <= small)
            peak = jnp.where(hit, peak * grow, peak)
            inverse = jnp.where(hit, inverse * grow, inverse)
            scale = jnp.where(hit, scale * shrink, scale)
    return scale, inverse


def kernel(
    axis, n, in_scale, out_scale,
    x_hbm, t_hbm, win_hbm, wout_hbm, reg_hbm, step_hbm,
    w0, g_parts, weights, out_w2, out_loss,
    t_ref, wout_ref, reg_ref, step_ref,
    x_v, xs, gram, pre, pre0, hid, fac, d_old,
    q_s, q_y, q_g, d_s, d_y, d_g, m_s, m_y, m_g, w2, cv,
    split_d, split_w, resid, logits_v, coef,
    z_src, z_buf, dot_src, dot_buf,
    load_sem, small_sem, send_sem, recv_sem,
):
    num_rows, dim = x_v.shape
    hid_rows = w0.shape[0]
    row_tiles = num_rows // LANES
    me = lax.axis_index(axis)
    offsets = sorted(range(1, n), key=lambda off: -min(off, n - off))
    peers = [lax.rem(me + off, n) for off in offsets]

    w_load = pltpu.make_async_copy(win_hbm, w0.at[:, pl.ds(0, dim)], load_sem.at[0])
    w_load.start()
    x_loads = []
    row_parts = [pl.ds(start, ROW_CHUNK) for start in range(0, num_rows, ROW_CHUNK)]
    for idx, part in enumerate(row_parts):
        load = pltpu.make_async_copy(x_hbm.at[part], x_v.at[part], load_sem.at[1 + idx])
        load.start()
        x_loads.append(load)
    smalls = []
    for idx, (src, dst) in enumerate(((t_hbm, t_ref), (wout_hbm, wout_ref), (reg_hbm, reg_ref), (step_hbm, step_ref))):
        load = pltpu.make_async_copy(src, dst, small_sem.at[idx])
        load.start()
        smalls.append(load)

    barrier = pltpu.get_barrier_semaphore()
    for peer in peers:
        pl.semaphore_signal(barrier, inc=1, device_id={axis: peer}, device_id_type=MESH)

    for load in smalls:
        load.wait()
    reg = reg_ref[0]
    step = step_ref[0]
    eye = lax.broadcasted_iota(jnp.int32, (hid_rows, LANES), 1) == lax.broadcasted_iota(jnp.int32, (hid_rows, LANES), 0)
    unit = lax.broadcasted_iota(jnp.int32, (SUBL, LANES), 0)
    col_parts = [pl.ds(start, COL_CHUNK) for start in range(0, dim, COL_CHUNK)]
    tiles = [pl.ds(start, LANES) for start in range(0, num_rows, LANES)]
    sums, cfrow, w2rows = pl.ds(0, SUBL), pl.ds(SUBL, SUBL), pl.ds(2 * SUBL, hid_rows)
    top = pl.ds(SUBL, 1)

    def send_all(src, dst, sem):
        for peer in peers:
            pltpu.make_async_remote_copy(
                src_ref=src, dst_ref=dst.at[me], send_sem=send_sem.at[sem], recv_sem=recv_sem.at[sem],
                device_id={axis: peer}, device_id_type=MESH,
            ).start()

    def wait_all(dst, sem):
        others = dst.at[pl.ds(0, n - 1)]
        pltpu.make_async_copy(others, others, recv_sem.at[sem]).wait()
        pltpu.make_async_copy(others, others, send_sem.at[sem]).wait()

    def splat(row):
        return jnp.broadcast_to(row, (SUBL, LANES))

    def store_split(ref, part, val):
        for idx, term in enumerate(split3(val)):
            ref[idx * hid_rows : (idx + 1) * hid_rows, part] = term

    def send_logits(buf, sem):
        rows = []
        for part in tiles:
            act = jnp.tanh(pre[:, part])
            hid[:, part] = act
            rows.append(jnp.sum(fold(act * w2[...]), axis=0, keepdims=True))
        z_mine = jnp.concatenate(rows, axis=0)
        z_src[...] = z_mine
        buf[me] = z_mine
        send_all(z_src, buf, sem)
        w2s = w2[...] * out_scale
        for part in tiles:
            act = hid[:, part]
            fac[:, part] = w2s * (1.0 - act * act)

    def residual(buf, sem):
        wait_all(buf, sem)
        logits = jnp.sum(buf[...], axis=0) * out_scale
        logits_v[...] = logits
        resid[...] = (jax.nn.sigmoid(logits) - t_ref[...]) * (1.0 / num_rows)

    def w2_grad():
        total = hid[:, tiles[0]] * resid[0:1, :]
        for idx in range(1, row_tiles):
            total = total + hid[:, tiles[idx]] * resid[idx : idx + 1, :]
        g_out = jnp.sum(total, axis=1, keepdims=True) * out_scale
        return jnp.broadcast_to(g_out, (hid_rows, LANES)) + reg * w2[...]

    def gram_times(part):
        high = jnp.dot(split_d[...], gram[0, :, part], preferred_element_type=F32)
        mid = jnp.dot(split_d[: 2 * hid_rows], gram[1, :, part], preferred_element_type=F32)
        low = jnp.dot(split_d[:hid_rows], gram[2, :, part], preferred_element_type=F32)
        small = (high[2 * hid_rows :] + mid[hid_rows:]) + low
        return (((high[hid_rows : 2 * hid_rows] + mid[:hid_rows]) + small + high[:hid_rows]) * x_scale) * x_scale

    def keep_g_part(idx):
        width = dim // G_TRIPS

        @pl.loop(0, G_TRIPS)
        def _(trip):
            part = pl.ds(pl.multiple_of(trip * width, width), width)
            prod = jnp.dot(split_d[...], xs[:, part], preferred_element_type=F32)
            g_parts[idx, :, part] = merge3(prod, hid_rows) * in_scale * x_scale

    def store_loss(idx):
        logits = logits_v[...]
        soft = jnp.maximum(logits, 0.0) + jnp.log1p(jnp.exp(-jnp.abs(logits)))
        out_loss[idx] = jnp.sum(soft - t_ref[...] * logits) * (1.0 / num_rows)

    def combine(cfs, slots, vec_g, vec_s, vec_y, rows, part):
        def scaled(cf, val):
            count = val.shape[0]
            return (val.reshape(count // SUBL, SUBL, LANES) * cf[None]).reshape(count, LANES)

        total = scaled(cfs[0], vec_g[rows, part])
        for idx, slot in enumerate(slots):
            total = total + scaled(cfs[1 + idx], vec_s[slot, rows, part])
            total = total + scaled(cfs[1 + HIST + idx], vec_y[slot, rows, part])
        return total

    every, lanes = pl.ds(0, hid_rows), pl.ds(0, LANES)

    def move(cfs, slots):
        new = slots[-1]
        s_part = combine(cfs, slots, m_g, m_s, m_y, w2rows, lanes)
        m_s[new, w2rows, :] = s_part
        w2[...] = w2[...] + s_part
        for part in tiles:
            q_part = combine(cfs, slots, q_g, q_s, q_y, every, part)
            q_s[new, :, part] = q_part
            pre[:, part] = pre[:, part] + q_part

    def move_rest(cfs, slots):
        new = slots[-1]
        s_part = combine(cfs, slots, m_g, m_s, m_y, pl.ds(0, 2 * SUBL), lanes)
        m_s[new, pl.ds(0, 2 * SUBL), :] = s_part
        cv[...] = cv[...] + s_part[SUBL:]
        acc = splat(m_g[top, :]) * s_part[:SUBL] + fold(m_g[w2rows, :] * m_s[new, w2rows, :]) * (1.0 / LANES)
        for part in tiles:
            d_part = combine(cfs, slots, d_g, d_s, d_y, every, part)
            d_s[new, :, part] = d_part
            acc = acc + fold(d_g[:, part] * q_s[new, :, part])
        return acc

    def new_grad(k, slots, acc_gs):
        new, old1, old2 = slots
        w2_part = w2_grad() - m_g[w2rows, :]
        acc_w0 = jnp.zeros((SUBL, LANES), F32)
        for idx, part in enumerate(tiles):
            d_new = fac[:, part] * resid[idx : idx + 1, :]
            diff = d_new - d_old[:, part]
            d_old[:, part] = d_new
            store_split(split_d, part, diff)
            d_y[new, :, part] = reg * d_s[new, :, part] + diff
            acc_w0 = acc_w0 + fold(diff * pre0[:, part])
        w0_y = reg * m_s[new, sums, :] + acc_w0
        cf_y = reg * m_s[new, cfrow, :] + jnp.where(unit == k + 1, 1.0, 0.0)
        c_y = splat(cf_y[0:1, :])
        m_y[new, sums, :] = w0_y
        m_y[new, cfrow, :] = cf_y
        m_y[new, w2rows, :] = w2_part
        others = [(q_s, m_s, new), (q_s, m_s, old1), (q_s, m_s, old2), (q_y, m_y, old1), (q_y, m_y, old2)]
        accs = [
            c_y * m[slot, sums, :] + fold(w2_part * m[slot, w2rows, :]) * (1.0 / LANES) for _, m, slot in others
        ]
        acc_gp = c_y * m_g[sums, :] + fold(w2_part * m_g[w2rows, :]) * (1.0 / LANES)
        acc_yy = c_y * w0_y + fold(w2_part * w2_part) * (1.0 / LANES)
        for part in row_parts:
            d_part = d_y[new, :, part]
            for idx, (q, _, slot) in enumerate(others):
                accs[idx] = accs[idx] + fold(d_part * q[slot, :, part])
            q_old = q_g[:, part]
            acc_gp = acc_gp + fold(d_part * q_old)
            q_new = reg * q_s[new, :, part] + gram_times(part)
            q_y[new, :, part] = q_new
            q_g[:, part] = q_old + q_new
            acc_yy = acc_yy + fold(d_part * q_new)
        order = accs[:3] + [acc_yy] + accs[3:] + [acc_gp, acc_gs]
        rows = [jnp.sum(acc, axis=0, keepdims=True) for acc in order]
        totals = jnp.sum(jnp.concatenate(rows, axis=0), axis=1, keepdims=True)
        packed = jnp.sum(jnp.where(eye[:NUM_DOTS], totals, 0.0), axis=0, keepdims=True)
        dot_src[...] = packed
        dot_buf[me] = packed
        send_all(dot_src, dot_buf, 2)
        m_g[...] = m_g[...] + m_y[new]
        for part in tiles:
            d_g[:, part] = d_g[:, part] + d_y[new, :, part]

    def two_loop(carry):
        rho1, rho2, psg0, psg1, pyg0, pyg1, pys1, yy11, yy12, yy22 = carry
        wait_all(dot_buf, 2)
        total = jnp.sum(dot_buf[...], axis=0)
        ys0, ys1, ys2, yy0, yy1, yy2, ygp, gs0 = (
            jnp.broadcast_to(total[:, idx : idx + 1], (SUBL, LANES)) for idx in range(NUM_DOTS)
        )
        sg0, sg1, sg2 = gs0 + ys0, psg0 + ys1, psg1 + ys2
        yg0, yg1, yg2 = ygp + yy0, pyg0 + yy1, pyg1 + yy2
        rho0 = 1.0 / ys0
        gamma = ys0 / yy0
        a0 = rho0 * sg0
        a1 = rho1 * (sg1 - a0 * ys1)
        a2 = rho2 * (sg2 - a0 * ys2 - a1 * pys1)
        yq2 = yg2 - a0 * yy2 - a1 * yy12 - a2 * yy22
        yq1 = yg1 - a0 * yy1 - a1 * yy11 - a2 * yy12
        yq0 = yg0 - a0 * yy0 - a1 * yy1 - a2 * yy2
        c2 = a2 - rho2 * (gamma * yq2)
        c1 = a1 - rho1 * (gamma * yq1 + c2 * pys1)
        c0 = a0 - rho0 * (gamma * yq0 + c2 * ys2 + c1 * ys1)
        sgam = step * gamma
        for idx, val in enumerate((-sgam, -step * c0, -step * c1, -step * c2, sgam * a0, sgam * a1, sgam * a2)):
            coef[idx] = val
        return rho0, rho1, sg0, sg1, yg0, yg1, ys1, yy0, yy1, yy11

    def load_coef():
        return [coef[idx] for idx in range(1 + 2 * HIST)]

    w2_row = jnp.broadcast_to(wout_ref[...], (hid_rows, LANES))
    w2_col = jnp.sum(jnp.where(eye, w2_row, 0.0), axis=1, keepdims=True)
    w2[...] = jnp.broadcast_to(w2_col, (hid_rows, LANES))
    w_load.wait()
    w0_w0 = jnp.zeros((SUBL, LANES), F32)
    for start in range(0, dim, LANES):
        part = pl.ds(start, LANES)
        w_part = w0[:, part]
        w0_w0 = w0_w0 + fold(w_part * w_part)
        store_split(split_w, part, w_part)
    peaks = []
    for idx, part in enumerate(row_parts):
        x_loads[idx].wait()
        x_part = x_v[part, :]
        prod = lax.dot_general(split_w[...], x_part, (((1,), (1,)), ((), ())), preferred_element_type=F32)
        pre_part = merge3(prod, hid_rows) * in_scale
        pre[:, part] = pre_part
        pre0[:, part] = pre_part
        peaks.append(jnp.max(jnp.abs(x_part).reshape(ROW_CHUNK // 16, 16, dim), axis=0))
    pl.semaphore_wait(barrier, n - 1)
    send_logits(z_buf.at[0], 0)
    x_scale, x_inverse = power_of_two(jnp.max(functools.reduce(jnp.maximum, peaks).astype(F32)))
    for part in row_parts:
        xs[part, :] = x_v[part, :] * jnp.full((ROW_CHUNK, dim), x_inverse, F32).astype(BF16)
    for row, row_part in enumerate(row_parts):
        for col, col_part in enumerate(row_parts[: row + 1]):
            block = lax.dot_general(
                xs[row_part, :], xs[col_part, :], (((1,), (1,)), ((), ())), preferred_element_type=F32
            ) * (in_scale * in_scale)
            for idx, term in enumerate(split3(block)):
                gram[idx, row_part, col_part] = term
            if col < row:
                for idx, term in enumerate(split3(block.T)):
                    gram[idx, col_part, row_part] = term
    for ref in (q_s, q_y, d_s, d_y, m_s, m_y, coef):
        ref[...] = jnp.zeros_like(ref)
    cv[...] = jnp.where(unit == 0, 1.0, 0.0)
    coef[0] = jnp.full((SUBL, LANES), -step, F32)
    residual(z_buf.at[0], 0)
    acc_w0 = reg * w0_w0
    for idx, part in enumerate(tiles):
        d_new = fac[:, part] * resid[idx : idx + 1, :]
        d_old[:, part] = d_new
        d_g[:, part] = d_new
        store_split(split_d, part, d_new)
        acc_w0 = acc_w0 + fold(d_new * pre0[:, part])
    m_g[sums, :] = acc_w0
    m_g[cfrow, :] = reg * cv[...] + jnp.where(unit == 1, 1.0, 0.0)
    m_g[w2rows, :] = w2_grad()
    for part in row_parts:
        q_g[:, part] = reg * pre0[:, part] + gram_times(part)
    store_loss(0)

    def head(k):
        new, old1, old2 = lax.rem(k, HIST), lax.rem(k + 2, HIST), lax.rem(k + 1, HIST)
        prev = (old1, old2, new)
        cfs = load_coef()
        move(cfs, prev)
        send_logits(z_buf.at[1], 1)
        acc_gs = move_rest(cfs, prev)
        keep_g_part(k - 1)
        residual(z_buf.at[1], 1)
        new_grad(k, (new, old1, old2), acc_gs)

    last = NUM_ITERS - 1

    def body(k, carry):
        head(k)
        store_loss(k)

        @pl.when(k == last)
        def _():
            keep_g_part(last)

        return two_loop(carry)

    zero = jnp.zeros((SUBL, LANES), F32)
    lax.fori_loop(1, NUM_ITERS, body, (zero,) * 10)

    slots = (last % HIST, (last + 2) % HIST, (last + 1) % HIST)
    cfs = load_coef()
    w2_new = w2[...] + combine(cfs, slots, m_g, m_s, m_y, w2rows, lanes)
    out_w2[...] = jnp.sum(jnp.where(eye, w2_new, 0.0), axis=0, keepdims=True)
    cv_new = cv[...] + combine(cfs, slots, m_g, m_s, m_y, cfrow, lanes)
    for idx in range(1 + NUM_ITERS):
        weights[idx] = splat(cv_new[idx : idx + 1, :])


def write_out(w0, g_parts, weights, w2_ref, loss_ref, out_w, out_w2, out_loss, w_v, sems, w_sems):
    rows, dim = out_w.shape
    copies = [
        pltpu.make_async_copy(src, dst, sems.at[idx]) for idx, (src, dst) in enumerate(((w2_ref, out_w2), (loss_ref, out_loss)))
    ]
    for copy in copies:
        copy.start()
    factors = [weights[idx][None] for idx in range(1 + NUM_ITERS)]

    def weighted(factor, val):
        return (val.reshape(rows // SUBL, SUBL, LANES) * factor).reshape(rows, LANES)

    for idx, start in enumerate(range(0, dim, COL_CHUNK)):
        for tile in range(start, start + COL_CHUNK, LANES):
            part = pl.ds(tile, LANES)
            total = weighted(factors[0], w0[:, part])
            for term in range(NUM_ITERS):
                total = total + weighted(factors[1 + term], g_parts[term, :, part])
            w_v[:, part] = total
        part = pl.ds(start, COL_CHUNK)
        copy = pltpu.make_async_copy(w_v.at[:, part], out_w.at[:, part], w_sems.at[idx])
        copy.start()
        copies.append(copy)
    for copy in copies:
        copy.wait()


def solution(mesh):
    n = mesh.shape["feat"]

    def local_solve(x_loc, t_loc, win_loc, wout_loc, reg_loc, step_loc):
        num_rows, dim = x_loc.shape
        hid_rows = win_loc.shape[0]
        flat = pltpu.VMEM((hid_rows, num_rows + LANES), F32)
        past = pltpu.VMEM((HIST, hid_rows, num_rows + LANES), F32)
        meta = 2 * SUBL + hid_rows
        in_scale = 1.0 / math.sqrt(dim)
        out_scale = 1.0 / math.sqrt(hid_rows * n)
        row_tiles = num_rows // LANES
        vmem = pl.BlockSpec(memory_space=pltpu.VMEM)
        smem = pl.BlockSpec(memory_space=pltpu.SMEM)
        anym = pl.BlockSpec(memory_space=pl.ANY)
        solved = pl.pallas_call(
            functools.partial(kernel, "feat", n, in_scale, out_scale),
            out_shape=(
                pltpu.VMEM((hid_rows, dim + LANES), F32),
                pltpu.VMEM((NUM_ITERS, hid_rows, dim + LANES), F32),
                pltpu.VMEM((1 + NUM_ITERS, SUBL, LANES), F32),
                pltpu.VMEM((1, hid_rows), F32),
                pltpu.SMEM((NUM_ITERS,), F32),
            ),
            in_specs=[anym] * 6,
            out_specs=(vmem, vmem, vmem, vmem, smem),
            scratch_shapes=[
                pltpu.VMEM((row_tiles, LANES), F32),
                pltpu.VMEM((1, hid_rows), F32),
                pltpu.SMEM((1,), F32),
                pltpu.SMEM((1,), F32),
                pltpu.VMEM((num_rows, dim), BF16),
                pltpu.VMEM((num_rows, dim), BF16),
                pltpu.VMEM((3, num_rows, num_rows), BF16),
                *([flat] * 5),
                past, past, flat, past, past, flat,
                pltpu.VMEM((HIST, meta, LANES), F32),
                pltpu.VMEM((HIST, meta, LANES), F32),
                pltpu.VMEM((meta, LANES), F32),
                pltpu.VMEM((hid_rows, LANES), F32),
                pltpu.VMEM((SUBL, LANES), F32),
                pltpu.VMEM((3 * hid_rows, num_rows), BF16),
                pltpu.VMEM((3 * hid_rows, dim), BF16),
                pltpu.VMEM((row_tiles, LANES), F32),
                pltpu.VMEM((row_tiles, LANES), F32),
                pltpu.VMEM((1 + 2 * HIST, SUBL, LANES), F32),
                pltpu.VMEM((row_tiles, LANES), F32),
                pltpu.VMEM((2, n, row_tiles, LANES), F32),
                pltpu.VMEM((1, LANES), F32),
                pltpu.VMEM((n, 1, LANES), F32),
                pltpu.SemaphoreType.DMA((1 + num_rows // ROW_CHUNK,)),
                pltpu.SemaphoreType.DMA((4,)),
                pltpu.SemaphoreType.DMA((3,)),
                pltpu.SemaphoreType.DMA((3,)),
            ],
            compiler_params=pltpu.CompilerParams(
                collective_id=0, has_side_effects=True, vmem_limit_bytes=46 * 1024 * 1024
            ),
        )(
            *(
                pltpu.with_memory_space_constraint(arg, pltpu.HBM)
                for arg in (x_loc, t_loc.reshape(row_tiles, LANES), win_loc, wout_loc.reshape(1, hid_rows))
            ),
            reg_loc, step_loc,
        )
        new_w, new_w2, losses = pl.pallas_call(
            write_out,
            out_shape=tuple(jax.ShapeDtypeStruct(shape, F32) for shape in ((hid_rows, dim), (1, hid_rows), (NUM_ITERS,))),
            in_specs=[vmem, vmem, vmem, vmem, smem],
            out_specs=(anym, anym, anym),
            scratch_shapes=[
                pltpu.VMEM((hid_rows, dim + LANES), F32),
                pltpu.SemaphoreType.DMA((2,)),
                pltpu.SemaphoreType.DMA((dim // COL_CHUNK,)),
            ],
            compiler_params=pltpu.CompilerParams(vmem_limit_bytes=4 * 1024 * 1024),
        )(*solved)
        return new_w, new_w2.reshape(hid_rows), losses

    specs_in = (P("prob", None), P("prob"), P(("prob", "feat"), None), P(("prob", "feat")), P("prob"), P("prob"))
    specs_out = (P(("prob", "feat"), None), P(("prob", "feat")), P("prob"))
    return jax.shard_map(local_solve, mesh=mesh, in_specs=specs_in, out_specs=specs_out, check_vma=False)
```

```python
import functools
import math

import jax
import jax.numpy as jnp
from jax import lax
from jax.experimental import pallas as pl
from jax.experimental.pallas import tpu as pltpu
from jax.sharding import PartitionSpec as P

NUM_ITERS = 6
HIST = 3
LANES = 128
SUBL = 8
ROW_CHUNK = 512
COL_CHUNK = 512
G_TRIPS = 3
NUM_DOTS = 8
MESH = pl.DeviceIdType.MESH
F32 = jnp.float32
BF16 = jnp.bfloat16


def split3(val):
    high = val.astype(BF16)
    rest = val - high.astype(F32)
    mid = rest.astype(BF16)
    low = (rest - mid.astype(F32)).astype(BF16)
    return high, mid, low


def fold(val):
    rows, cols = val.shape
    part = jnp.sum(val.reshape(rows // SUBL, SUBL, cols), axis=0)
    total = part[:, :LANES]
    for start in range(LANES, cols, LANES):
        total = total + part[:, start : start + LANES]
    return total


def merge3(prod, rows):
    return (prod[2 * rows :] + prod[rows : 2 * rows]) + prod[:rows]


def power_of_two(peak):
    scale = jnp.float32(1.0)
    inverse = jnp.float32(1.0)
    for up in (True, False):
        for bits in (64, 32, 16, 8, 4, 2):
            big, small = 2.0**bits, 2.0**-bits
            grow, shrink = (small, big) if up else (big, small)
            hit = (peak >= big) if up else (peak <= small)
            peak = jnp.where(hit, peak * grow, peak)
            inverse = jnp.where(hit, inverse * grow, inverse)
            scale = jnp.where(hit, scale * shrink, scale)
    return scale, inverse


def kernel(
    axis, n, in_scale, out_scale,
    x_hbm, t_hbm, win_hbm, wout_hbm, reg_hbm, step_hbm,
    w0, g_parts, weights, out_w2, out_loss,
    t_ref, wout_ref, reg_ref, step_ref,
    x_v, xs, gram, pre, pre0, hid, fac, d_old,
    q_s, q_y, q_g, d_s, d_y, d_g, m_s, m_y, m_g, w2, cv,
    split_d, split_w, resid, logits_v, coef,
    z_src, z_buf, dot_src, dot_buf,
    load_sem, small_sem, send_sem, recv_sem,
):
    num_rows, dim = x_v.shape
    hid_rows = w0.shape[0]
    row_tiles = num_rows // LANES
    me = lax.axis_index(axis)
    offsets = sorted(range(1, n), key=lambda off: -min(off, n - off))
    peers = [lax.rem(me + off, n) for off in offsets]

    w_load = pltpu.make_async_copy(win_hbm, w0.at[:, pl.ds(0, dim)], load_sem.at[0])
    w_load.start()
    row_parts = [pl.ds(start, ROW_CHUNK) for start in range(0, num_rows, ROW_CHUNK)]
    dim_halves = [pl.ds(0, dim // 2), pl.ds(dim // 2, dim // 2)]
    x_loads = []
    for part in row_parts:
        for half in dim_halves:
            sem = load_sem.at[1 + len(x_loads)]
            x_loads.append(pltpu.make_async_copy(x_hbm.at[part, half], x_v.at[part, half], sem))
    for load in x_loads[:2]:
        load.start()
    smalls = []
    for idx, (src, dst) in enumerate(((t_hbm, t_ref), (wout_hbm, wout_ref), (reg_hbm, reg_ref), (step_hbm, step_ref))):
        load = pltpu.make_async_copy(src, dst, small_sem.at[idx])
        load.start()
        smalls.append(load)

    barrier = pltpu.get_barrier_semaphore()
    for peer in peers:
        pl.semaphore_signal(barrier, inc=1, device_id={axis: peer}, device_id_type=MESH)

    w_load.wait()
    for load in x_loads[2:]:
        load.start()
    for load in smalls:
        load.wait()
    reg = reg_ref[0]
    step = step_ref[0]
    eye = lax.broadcasted_iota(jnp.int32, (hid_rows, LANES), 1) == lax.broadcasted_iota(jnp.int32, (hid_rows, LANES), 0)
    unit = lax.broadcasted_iota(jnp.int32, (SUBL, LANES), 0)
    col_parts = [pl.ds(start, COL_CHUNK) for start in range(0, dim, COL_CHUNK)]
    tiles = [pl.ds(start, LANES) for start in range(0, num_rows, LANES)]
    sums, cfrow, w2rows = pl.ds(0, SUBL), pl.ds(SUBL, SUBL), pl.ds(2 * SUBL, hid_rows)
    top = pl.ds(SUBL, 1)

    def send_all(src, dst, sem):
        for peer in peers:
            pltpu.make_async_remote_copy(
                src_ref=src, dst_ref=dst.at[me], send_sem=send_sem.at[sem], recv_sem=recv_sem.at[sem],
                device_id={axis: peer}, device_id_type=MESH,
            ).start()

    def wait_all(dst, sem):
        others = dst.at[pl.ds(0, n - 1)]
        pltpu.make_async_copy(others, others, recv_sem.at[sem]).wait()
        pltpu.make_async_copy(others, others, send_sem.at[sem]).wait()

    def splat(row):
        return jnp.broadcast_to(row, (SUBL, LANES))

    def store_split(ref, part, val):
        for idx, term in enumerate(split3(val)):
            ref[idx * hid_rows : (idx + 1) * hid_rows, part] = term

    def set_factor():
        w2s = w2[...] * out_scale
        for part in tiles:
            act = hid[:, part]
            fac[:, part] = w2s * (1.0 - act * act)

    def send_logits(buf, sem, lazy=False):
        rows = []
        for part in tiles:
            act = jnp.tanh(pre[:, part])
            hid[:, part] = act
            rows.append(jnp.sum(fold(act * w2[...]), axis=0, keepdims=True))
        z_mine = jnp.concatenate(rows, axis=0)
        z_src[...] = z_mine
        buf[me] = z_mine
        send_all(z_src, buf, sem)
        if not lazy:
            set_factor()

    def residual(buf, sem):
        wait_all(buf, sem)
        logits = jnp.sum(buf[...], axis=0) * out_scale
        logits_v[...] = logits
        resid[...] = (jax.nn.sigmoid(logits) - t_ref[...]) * (1.0 / num_rows)

    def w2_grad():
        total = hid[:, tiles[0]] * resid[0:1, :]
        for idx in range(1, row_tiles):
            total = total + hid[:, tiles[idx]] * resid[idx : idx + 1, :]
        g_out = jnp.sum(total, axis=1, keepdims=True) * out_scale
        return jnp.broadcast_to(g_out, (hid_rows, LANES)) + reg * w2[...]

    def gram_times(part):
        high = jnp.dot(split_d[...], gram[0, :, part], preferred_element_type=F32)
        mid = jnp.dot(split_d[: 2 * hid_rows], gram[1, :, part], preferred_element_type=F32)
        low = jnp.dot(split_d[:hid_rows], gram[2, :, part], preferred_element_type=F32)
        small = (high[2 * hid_rows :] + mid[hid_rows:]) + low
        return (((high[hid_rows : 2 * hid_rows] + mid[:hid_rows]) + small + high[:hid_rows]) * x_scale) * x_scale

    def keep_g_part(idx):
        width = dim // G_TRIPS

        @pl.loop(0, G_TRIPS)
        def _(trip):
            part = pl.ds(pl.multiple_of(trip * width, width), width)
            prod = jnp.dot(split_d[...], xs[:, part], preferred_element_type=F32)
            g_parts[idx, :, part] = merge3(prod, hid_rows) * in_scale * x_scale

    def store_loss(idx):
        logits = logits_v[...]
        soft = jnp.maximum(logits, 0.0) + jnp.log1p(jnp.exp(-jnp.abs(logits)))
        out_loss[idx] = jnp.sum(soft - t_ref[...] * logits) * (1.0 / num_rows)

    def combine(cfs, slots, vec_g, vec_s, vec_y, rows, part):
        def scaled(cf, val):
            count = val.shape[0]
            return (val.reshape(count // SUBL, SUBL, LANES) * cf[None]).reshape(count, LANES)

        total = scaled(cfs[0], vec_g[rows, part])
        for idx, slot in enumerate(slots):
            total = total + scaled(cfs[1 + idx], vec_s[slot, rows, part])
            total = total + scaled(cfs[1 + HIST + idx], vec_y[slot, rows, part])
        return total

    every, lanes = pl.ds(0, hid_rows), pl.ds(0, LANES)

    def move(cfs, slots):
        new = slots[-1]
        s_part = combine(cfs, slots, m_g, m_s, m_y, w2rows, lanes)
        m_s[new, w2rows, :] = s_part
        w2[...] = w2[...] + s_part
        for part in tiles:
            q_part = combine(cfs, slots, q_g, q_s, q_y, every, part)
            q_s[new, :, part] = q_part
            pre[:, part] = pre[:, part] + q_part

    def move_rest(cfs, slots):
        new = slots[-1]
        s_part = combine(cfs, slots, m_g, m_s, m_y, pl.ds(0, 2 * SUBL), lanes)
        m_s[new, pl.ds(0, 2 * SUBL), :] = s_part
        cv[...] = cv[...] + s_part[SUBL:]
        acc = splat(m_g[top, :]) * s_part[:SUBL] + fold(m_g[w2rows, :] * m_s[new, w2rows, :]) * (1.0 / LANES)
        for part in tiles:
            d_part = combine(cfs, slots, d_g, d_s, d_y, every, part)
            d_s[new, :, part] = d_part
            acc = acc + fold(d_g[:, part] * q_s[new, :, part])
        return acc

    def new_grad(k, slots, acc_gs):
        new, old1, old2 = slots
        w2_part = w2_grad() - m_g[w2rows, :]
        acc_w0 = jnp.zeros((SUBL, LANES), F32)
        for idx, part in enumerate(tiles):
            d_new = fac[:, part] * resid[idx : idx + 1, :]
            diff = d_new - d_old[:, part]
            d_old[:, part] = d_new
            store_split(split_d, part, diff)
            d_y[new, :, part] = reg * d_s[new, :, part] + diff
            acc_w0 = acc_w0 + fold(diff * pre0[:, part])
        w0_y = reg * m_s[new, sums, :] + acc_w0
        cf_y = reg * m_s[new, cfrow, :] + jnp.where(unit == k + 1, 1.0, 0.0)
        c_y = splat(cf_y[0:1, :])
        m_y[new, sums, :] = w0_y
        m_y[new, cfrow, :] = cf_y
        m_y[new, w2rows, :] = w2_part
        others = [(q_s, m_s, new), (q_s, m_s, old1), (q_s, m_s, old2), (q_y, m_y, old1), (q_y, m_y, old2)]
        accs = [
            c_y * m[slot, sums, :] + fold(w2_part * m[slot, w2rows, :]) * (1.0 / LANES) for _, m, slot in others
        ]
        acc_gp = c_y * m_g[sums, :] + fold(w2_part * m_g[w2rows, :]) * (1.0 / LANES)
        acc_yy = c_y * w0_y + fold(w2_part * w2_part) * (1.0 / LANES)
        for part in row_parts:
            d_part = d_y[new, :, part]
            for idx, (q, _, slot) in enumerate(others):
                accs[idx] = accs[idx] + fold(d_part * q[slot, :, part])
            q_old = q_g[:, part]
            acc_gp = acc_gp + fold(d_part * q_old)
            q_new = reg * q_s[new, :, part] + gram_times(part)
            q_y[new, :, part] = q_new
            q_g[:, part] = q_old + q_new
            acc_yy = acc_yy + fold(d_part * q_new)
        order = accs[:3] + [acc_yy] + accs[3:] + [acc_gp, acc_gs]
        rows = [jnp.sum(acc, axis=0, keepdims=True) for acc in order]
        totals = jnp.sum(jnp.concatenate(rows, axis=0), axis=1, keepdims=True)
        packed = jnp.sum(jnp.where(eye[:NUM_DOTS], totals, 0.0), axis=0, keepdims=True)
        dot_src[...] = packed
        dot_buf[me] = packed
        send_all(dot_src, dot_buf, 2)
        m_g[...] = m_g[...] + m_y[new]
        for part in tiles:
            d_g[:, part] = d_g[:, part] + d_y[new, :, part]

    def two_loop(carry):
        rho1, rho2, psg0, psg1, pyg0, pyg1, pys1, yy11, yy12, yy22 = carry
        wait_all(dot_buf, 2)
        total = jnp.sum(dot_buf[...], axis=0)
        ys0, ys1, ys2, yy0, yy1, yy2, ygp, gs0 = (
            jnp.broadcast_to(total[:, idx : idx + 1], (SUBL, LANES)) for idx in range(NUM_DOTS)
        )
        sg0, sg1, sg2 = gs0 + ys0, psg0 + ys1, psg1 + ys2
        yg0, yg1, yg2 = ygp + yy0, pyg0 + yy1, pyg1 + yy2
        rho0 = 1.0 / ys0
        gamma = ys0 / yy0
        a0 = rho0 * sg0
        a1 = rho1 * (sg1 - a0 * ys1)
        a2 = rho2 * (sg2 - a0 * ys2 - a1 * pys1)
        yq2 = yg2 - a0 * yy2 - a1 * yy12 - a2 * yy22
        yq1 = yg1 - a0 * yy1 - a1 * yy11 - a2 * yy12
        yq0 = yg0 - a0 * yy0 - a1 * yy1 - a2 * yy2
        c2 = a2 - rho2 * (gamma * yq2)
        c1 = a1 - rho1 * (gamma * yq1 + c2 * pys1)
        c0 = a0 - rho0 * (gamma * yq0 + c2 * ys2 + c1 * ys1)
        sgam = step * gamma
        for idx, val in enumerate((-sgam, -step * c0, -step * c1, -step * c2, sgam * a0, sgam * a1, sgam * a2)):
            coef[idx] = val
        return rho0, rho1, sg0, sg1, yg0, yg1, ys1, yy0, yy1, yy11

    def load_coef():
        return [coef[idx] for idx in range(1 + 2 * HIST)]

    w2_row = jnp.broadcast_to(wout_ref[...], (hid_rows, LANES))
    w2_col = jnp.sum(jnp.where(eye, w2_row, 0.0), axis=1, keepdims=True)
    w2[...] = jnp.broadcast_to(w2_col, (hid_rows, LANES))
    w0_w0 = jnp.zeros((SUBL, LANES), F32)
    for start in range(0, dim, LANES):
        part = pl.ds(start, LANES)
        w_part = w0[:, part]
        w0_w0 = w0_w0 + fold(w_part * w_part)
        store_split(split_w, part, w_part)
    peaks = []
    for idx, part in enumerate(row_parts):
        total = None
        for half, load in zip(dim_halves, x_loads[2 * idx : 2 * idx + 2]):
            load.wait()
            prod = lax.dot_general(
                split_w[:, half], x_v[part, half], (((1,), (1,)), ((), ())), preferred_element_type=F32
            )
            total = merge3(prod, hid_rows) if total is None else total + merge3(prod, hid_rows)
        pre_part = total * in_scale
        pre[:, part] = pre_part
        pre0[:, part] = pre_part
        peaks.append(jnp.max(jnp.abs(x_v[part, :]).reshape(ROW_CHUNK // 16, 16, dim), axis=0))
    x_scale, x_inverse = power_of_two(jnp.max(functools.reduce(jnp.maximum, peaks).astype(F32)))
    pl.semaphore_wait(barrier, n - 1)
    send_logits(z_buf.at[0], 0, lazy=True)
    for row, row_part in enumerate(row_parts):
        xs[row_part, :] = x_v[row_part, :] * jnp.full((ROW_CHUNK, dim), x_inverse, F32).astype(BF16)
        for col, col_part in enumerate(row_parts[: row + 1]):
            block = lax.dot_general(
                xs[row_part, :], xs[col_part, :], (((1,), (1,)), ((), ())), preferred_element_type=F32
            ) * (in_scale * in_scale)
            for idx, term in enumerate(split3(block)):
                gram[idx, row_part, col_part] = term
            if col < row:
                for idx, term in enumerate(split3(block.T)):
                    gram[idx, col_part, row_part] = term
    set_factor()
    for ref in (q_s, q_y, d_s, d_y, m_s, m_y, coef):
        ref[...] = jnp.zeros_like(ref)
    cv[...] = jnp.where(unit == 0, 1.0, 0.0)
    coef[0] = jnp.full((SUBL, LANES), -step, F32)
    residual(z_buf.at[0], 0)
    acc_w0 = reg * w0_w0
    for idx, part in enumerate(tiles):
        d_new = fac[:, part] * resid[idx : idx + 1, :]
        d_old[:, part] = d_new
        d_g[:, part] = d_new
        store_split(split_d, part, d_new)
        acc_w0 = acc_w0 + fold(d_new * pre0[:, part])
    m_g[sums, :] = acc_w0
    m_g[cfrow, :] = reg * cv[...] + jnp.where(unit == 1, 1.0, 0.0)
    m_g[w2rows, :] = w2_grad()
    for part in row_parts:
        q_g[:, part] = reg * pre0[:, part] + gram_times(part)
    store_loss(0)

    def head(k):
        new, old1, old2 = lax.rem(k, HIST), lax.rem(k + 2, HIST), lax.rem(k + 1, HIST)
        prev = (old1, old2, new)
        cfs = load_coef()
        move(cfs, prev)
        send_logits(z_buf.at[1], 1)
        acc_gs = move_rest(cfs, prev)
        keep_g_part(k - 1)
        residual(z_buf.at[1], 1)
        new_grad(k, (new, old1, old2), acc_gs)

    last = NUM_ITERS - 1

    def body(k, carry):
        head(k)
        store_loss(k)

        @pl.when(k == last)
        def _():
            keep_g_part(last)

        return two_loop(carry)

    zero = jnp.zeros((SUBL, LANES), F32)
    lax.fori_loop(1, NUM_ITERS, body, (zero,) * 10)

    slots = (last % HIST, (last + 2) % HIST, (last + 1) % HIST)
    cfs = load_coef()
    w2_new = w2[...] + combine(cfs, slots, m_g, m_s, m_y, w2rows, lanes)
    out_w2[...] = jnp.sum(jnp.where(eye, w2_new, 0.0), axis=0, keepdims=True)
    cv_new = cv[...] + combine(cfs, slots, m_g, m_s, m_y, cfrow, lanes)
    for idx in range(1 + NUM_ITERS):
        weights[idx] = splat(cv_new[idx : idx + 1, :])


def write_out(w0, g_parts, weights, w2_ref, loss_ref, out_w, out_w2, out_loss, w_v, sems, w_sems):
    rows, dim = out_w.shape
    copies = [
        pltpu.make_async_copy(src, dst, sems.at[idx]) for idx, (src, dst) in enumerate(((w2_ref, out_w2), (loss_ref, out_loss)))
    ]
    for copy in copies:
        copy.start()
    factors = [weights[idx][None] for idx in range(1 + NUM_ITERS)]

    def weighted(factor, val):
        return (val.reshape(rows // SUBL, SUBL, LANES) * factor).reshape(rows, LANES)

    for idx, start in enumerate(range(0, dim, COL_CHUNK)):
        for tile in range(start, start + COL_CHUNK, LANES):
            part = pl.ds(tile, LANES)
            total = weighted(factors[0], w0[:, part])
            for term in range(NUM_ITERS):
                total = total + weighted(factors[1 + term], g_parts[term, :, part])
            w_v[:, part] = total
        part = pl.ds(start, COL_CHUNK)
        copy = pltpu.make_async_copy(w_v.at[:, part], out_w.at[:, part], w_sems.at[idx])
        copy.start()
        copies.append(copy)
    for copy in copies:
        copy.wait()


def solution(mesh):
    n = mesh.shape["feat"]

    def local_solve(x_loc, t_loc, win_loc, wout_loc, reg_loc, step_loc):
        num_rows, dim = x_loc.shape
        hid_rows = win_loc.shape[0]
        flat = pltpu.VMEM((hid_rows, num_rows + LANES), F32)
        past = pltpu.VMEM((HIST, hid_rows, num_rows + LANES), F32)
        meta = 2 * SUBL + hid_rows
        in_scale = 1.0 / math.sqrt(dim)
        out_scale = 1.0 / math.sqrt(hid_rows * n)
        row_tiles = num_rows // LANES
        vmem = pl.BlockSpec(memory_space=pltpu.VMEM)
        smem = pl.BlockSpec(memory_space=pltpu.SMEM)
        anym = pl.BlockSpec(memory_space=pl.ANY)
        solved = pl.pallas_call(
            functools.partial(kernel, "feat", n, in_scale, out_scale),
            out_shape=(
                pltpu.VMEM((hid_rows, dim + LANES), F32),
                pltpu.VMEM((NUM_ITERS, hid_rows, dim + LANES), F32),
                pltpu.VMEM((1 + NUM_ITERS, SUBL, LANES), F32),
                pltpu.VMEM((1, hid_rows), F32),
                pltpu.SMEM((NUM_ITERS,), F32),
            ),
            in_specs=[anym] * 6,
            out_specs=(vmem, vmem, vmem, vmem, smem),
            scratch_shapes=[
                pltpu.VMEM((row_tiles, LANES), F32),
                pltpu.VMEM((1, hid_rows), F32),
                pltpu.SMEM((1,), F32),
                pltpu.SMEM((1,), F32),
                pltpu.VMEM((num_rows, dim), BF16),
                pltpu.VMEM((num_rows, dim), BF16),
                pltpu.VMEM((3, num_rows, num_rows), BF16),
                *([flat] * 5),
                past, past, flat, past, past, flat,
                pltpu.VMEM((HIST, meta, LANES), F32),
                pltpu.VMEM((HIST, meta, LANES), F32),
                pltpu.VMEM((meta, LANES), F32),
                pltpu.VMEM((hid_rows, LANES), F32),
                pltpu.VMEM((SUBL, LANES), F32),
                pltpu.VMEM((3 * hid_rows, num_rows), BF16),
                pltpu.VMEM((3 * hid_rows, dim), BF16),
                pltpu.VMEM((row_tiles, LANES), F32),
                pltpu.VMEM((row_tiles, LANES), F32),
                pltpu.VMEM((1 + 2 * HIST, SUBL, LANES), F32),
                pltpu.VMEM((row_tiles, LANES), F32),
                pltpu.VMEM((2, n, row_tiles, LANES), F32),
                pltpu.VMEM((1, LANES), F32),
                pltpu.VMEM((n, 1, LANES), F32),
                pltpu.SemaphoreType.DMA((1 + 2 * (num_rows // ROW_CHUNK),)),
                pltpu.SemaphoreType.DMA((4,)),
                pltpu.SemaphoreType.DMA((3,)),
                pltpu.SemaphoreType.DMA((3,)),
            ],
            compiler_params=pltpu.CompilerParams(
                collective_id=0, has_side_effects=True, vmem_limit_bytes=46 * 1024 * 1024
            ),
        )(
            *(
                pltpu.with_memory_space_constraint(arg, pltpu.HBM)
                for arg in (x_loc, t_loc.reshape(row_tiles, LANES), win_loc, wout_loc.reshape(1, hid_rows))
            ),
            reg_loc, step_loc,
        )
        new_w, new_w2, losses = pl.pallas_call(
            write_out,
            out_shape=tuple(jax.ShapeDtypeStruct(shape, F32) for shape in ((hid_rows, dim), (1, hid_rows), (NUM_ITERS,))),
            in_specs=[vmem, vmem, vmem, vmem, smem],
            out_specs=(anym, anym, anym),
            scratch_shapes=[
                pltpu.VMEM((hid_rows, dim + LANES), F32),
                pltpu.SemaphoreType.DMA((2,)),
                pltpu.SemaphoreType.DMA((dim // COL_CHUNK,)),
            ],
            compiler_params=pltpu.CompilerParams(vmem_limit_bytes=4 * 1024 * 1024),
        )(*solved)
        return new_w, new_w2.reshape(hid_rows), losses

    specs_in = (P("prob", None), P("prob"), P(("prob", "feat"), None), P(("prob", "feat")), P("prob"), P("prob"))
    specs_out = (P(("prob", "feat"), None), P(("prob", "feat")), P("prob"))
    return jax.shard_map(local_solve, mesh=mesh, in_specs=specs_in, out_specs=specs_out, check_vma=False)
```

```python
import functools
import math

import jax
import jax.numpy as jnp
from jax import lax
from jax.experimental import pallas as pl
from jax.experimental.pallas import tpu as pltpu
from jax.sharding import PartitionSpec as P

NUM_ITERS = 6
HIST = 3
LANES = 128
SUBL = 8
ROW_CHUNK = 512
COL_CHUNK = 512
NUM_DOTS = 8
MESH = pl.DeviceIdType.MESH
F32 = jnp.float32
BF16 = jnp.bfloat16


def split3(val):
    high = val.astype(BF16)
    rest = val - high.astype(F32)
    mid = rest.astype(BF16)
    low = (rest - mid.astype(F32)).astype(BF16)
    return high, mid, low


def fold(val):
    rows, cols = val.shape
    part = jnp.sum(val.reshape(rows // SUBL, SUBL, cols), axis=0)
    total = part[:, :LANES]
    for start in range(LANES, cols, LANES):
        total = total + part[:, start : start + LANES]
    return total


def merge3(prod, rows):
    return (prod[2 * rows :] + prod[rows : 2 * rows]) + prod[:rows]


def power_of_two(peak):
    scale = jnp.float32(1.0)
    inverse = jnp.float32(1.0)
    for up in (True, False):
        for bits in (64, 32, 16, 8, 4, 2):
            big, small = 2.0**bits, 2.0**-bits
            grow, shrink = (small, big) if up else (big, small)
            hit = (peak >= big) if up else (peak <= small)
            peak = jnp.where(hit, peak * grow, peak)
            inverse = jnp.where(hit, inverse * grow, inverse)
            scale = jnp.where(hit, scale * shrink, scale)
    return scale, inverse


def kernel(
    axis, n, in_scale, out_scale,
    x_hbm, t_hbm, win_hbm, wout_hbm, reg_hbm, step_hbm,
    w0, g_parts, weights, out_w2, out_loss,
    t_ref, wout_ref, reg_ref, step_ref,
    x_v, xs, gram, pre, pre0, hid, fac, d_old,
    q_s, q_y, q_g, d_s, d_y, d_g, m_s, m_y, m_g, w2, cv,
    split_d, split_w, resid, logits_v, coef,
    z_src, z_buf, dot_src, dot_buf,
    load_sem, small_sem, send_sem, recv_sem,
):
    num_rows, dim = x_v.shape
    hid_rows = w0.shape[0]
    row_tiles = num_rows // LANES
    me = lax.axis_index(axis)
    offsets = sorted(range(1, n), key=lambda off: -min(off, n - off))
    peers = [lax.rem(me + off, n) for off in offsets]

    w_load = pltpu.make_async_copy(win_hbm, w0.at[:, pl.ds(0, dim)], load_sem.at[0])
    w_load.start()
    row_parts = [pl.ds(start, ROW_CHUNK) for start in range(0, num_rows, ROW_CHUNK)]
    dim_halves = [pl.ds(0, dim // 2), pl.ds(dim // 2, dim // 2)]
    x_loads = []
    for part in row_parts:
        for half in dim_halves:
            sem = load_sem.at[1 + len(x_loads)]
            x_loads.append(pltpu.make_async_copy(x_hbm.at[part, half], x_v.at[part, half], sem))
    for load in x_loads[:2]:
        load.start()
    smalls = []
    for idx, (src, dst) in enumerate(((t_hbm, t_ref), (wout_hbm, wout_ref), (reg_hbm, reg_ref), (step_hbm, step_ref))):
        load = pltpu.make_async_copy(src, dst, small_sem.at[idx])
        load.start()
        smalls.append(load)

    barrier = pltpu.get_barrier_semaphore()
    for peer in peers:
        pl.semaphore_signal(barrier, inc=1, device_id={axis: peer}, device_id_type=MESH)

    w_load.wait()
    for load in x_loads[2:]:
        load.start()
    for load in smalls:
        load.wait()
    reg = reg_ref[0]
    step = step_ref[0]
    eye = lax.broadcasted_iota(jnp.int32, (hid_rows, LANES), 1) == lax.broadcasted_iota(jnp.int32, (hid_rows, LANES), 0)
    unit = lax.broadcasted_iota(jnp.int32, (SUBL, LANES), 0)
    col_parts = [pl.ds(start, COL_CHUNK) for start in range(0, dim, COL_CHUNK)]
    tiles = [pl.ds(start, LANES) for start in range(0, num_rows, LANES)]
    sums, cfrow, w2rows = pl.ds(0, SUBL), pl.ds(SUBL, SUBL), pl.ds(2 * SUBL, hid_rows)
    top = pl.ds(SUBL, 1)

    def send_all(src, dst, sem):
        for peer in peers:
            pltpu.make_async_remote_copy(
                src_ref=src, dst_ref=dst.at[me], send_sem=send_sem.at[sem], recv_sem=recv_sem.at[sem],
                device_id={axis: peer}, device_id_type=MESH,
            ).start()

    def wait_all(dst, sem):
        others = dst.at[pl.ds(0, n - 1)]
        pltpu.make_async_copy(others, others, recv_sem.at[sem]).wait()
        pltpu.make_async_copy(others, others, send_sem.at[sem]).wait()

    def splat(row):
        return jnp.broadcast_to(row, (SUBL, LANES))

    def store_split(ref, part, val):
        for idx, term in enumerate(split3(val)):
            ref[idx * hid_rows : (idx + 1) * hid_rows, part] = term

    def set_factor():
        w2s = w2[...] * out_scale
        for part in tiles:
            act = hid[:, part]
            fac[:, part] = w2s * (1.0 - act * act)

    def send_logits(buf, sem, lazy=False):
        rows = []
        for part in tiles:
            act = jnp.tanh(pre[:, part])
            hid[:, part] = act
            rows.append(jnp.sum(fold(act * w2[...]), axis=0, keepdims=True))
        z_mine = jnp.concatenate(rows, axis=0)
        z_src[...] = z_mine
        buf[me] = z_mine
        send_all(z_src, buf, sem)
        if not lazy:
            set_factor()

    def residual(buf, sem):
        wait_all(buf, sem)
        logits = jnp.sum(buf[...], axis=0) * out_scale
        logits_v[...] = logits
        resid[...] = (jax.nn.sigmoid(logits) - t_ref[...]) * (1.0 / num_rows)

    def w2_grad():
        total = hid[:, tiles[0]] * resid[0:1, :]
        for idx in range(1, row_tiles):
            total = total + hid[:, tiles[idx]] * resid[idx : idx + 1, :]
        g_out = jnp.sum(total, axis=1, keepdims=True) * out_scale
        return jnp.broadcast_to(g_out, (hid_rows, LANES)) + reg * w2[...]

    def gram_times(part):
        high = jnp.dot(split_d[...], gram[0, :, part], preferred_element_type=F32)
        mid = jnp.dot(split_d[: 2 * hid_rows], gram[1, :, part], preferred_element_type=F32)
        low = jnp.dot(split_d[:hid_rows], gram[2, :, part], preferred_element_type=F32)
        small = (high[2 * hid_rows :] + mid[hid_rows:]) + low
        return (((high[hid_rows : 2 * hid_rows] + mid[:hid_rows]) + small + high[:hid_rows]) * x_scale) * x_scale

    def keep_g_part(idx):
        for part in col_parts:
            prod = jnp.dot(split_d[...], xs[:, part], preferred_element_type=F32)
            g_parts[idx, :, part] = merge3(prod, hid_rows) * in_scale * x_scale

    def store_loss(idx):
        logits = logits_v[...]
        soft = jnp.maximum(logits, 0.0) + jnp.log1p(jnp.exp(-jnp.abs(logits)))
        out_loss[idx] = jnp.sum(soft - t_ref[...] * logits) * (1.0 / num_rows)

    def combine(cfs, slots, vec_g, vec_s, vec_y, rows, part):
        def scaled(cf, val):
            count = val.shape[0]
            return (val.reshape(count // SUBL, SUBL, LANES) * cf[None]).reshape(count, LANES)

        total = scaled(cfs[0], vec_g[rows, part])
        for idx, slot in enumerate(slots):
            total = total + scaled(cfs[1 + idx], vec_s[slot, rows, part])
            total = total + scaled(cfs[1 + HIST + idx], vec_y[slot, rows, part])
        return total

    every, lanes = pl.ds(0, hid_rows), pl.ds(0, LANES)

    def move(cfs, slots):
        new = slots[-1]
        s_part = combine(cfs, slots, m_g, m_s, m_y, w2rows, lanes)
        m_s[new, w2rows, :] = s_part
        w2[...] = w2[...] + s_part
        for part in tiles:
            q_part = combine(cfs, slots, q_g, q_s, q_y, every, part)
            q_s[new, :, part] = q_part
            pre[:, part] = pre[:, part] + q_part

    def move_rest(cfs, slots):
        new = slots[-1]
        s_part = combine(cfs, slots, m_g, m_s, m_y, pl.ds(0, 2 * SUBL), lanes)
        m_s[new, pl.ds(0, 2 * SUBL), :] = s_part
        cv[...] = cv[...] + s_part[SUBL:]
        acc = splat(m_g[top, :]) * s_part[:SUBL] + fold(m_g[w2rows, :] * m_s[new, w2rows, :]) * (1.0 / LANES)
        for part in tiles:
            d_part = combine(cfs, slots, d_g, d_s, d_y, every, part)
            d_s[new, :, part] = d_part
            acc = acc + fold(d_g[:, part] * q_s[new, :, part])
        return acc

    def new_grad(k, slots, acc_gs):
        new, old1, old2 = slots
        w2_part = w2_grad() - m_g[w2rows, :]
        acc_w0 = jnp.zeros((SUBL, LANES), F32)
        for idx, part in enumerate(tiles):
            d_new = fac[:, part] * resid[idx : idx + 1, :]
            diff = d_new - d_old[:, part]
            d_old[:, part] = d_new
            store_split(split_d, part, diff)
            d_y[new, :, part] = reg * d_s[new, :, part] + diff
            acc_w0 = acc_w0 + fold(diff * pre0[:, part])
        w0_y = reg * m_s[new, sums, :] + acc_w0
        cf_y = reg * m_s[new, cfrow, :] + jnp.where(unit == k + 1, 1.0, 0.0)
        c_y = splat(cf_y[0:1, :])
        m_y[new, sums, :] = w0_y
        m_y[new, cfrow, :] = cf_y
        m_y[new, w2rows, :] = w2_part
        others = [(q_s, m_s, new), (q_s, m_s, old1), (q_s, m_s, old2), (q_y, m_y, old1), (q_y, m_y, old2)]
        accs = [
            c_y * m[slot, sums, :] + fold(w2_part * m[slot, w2rows, :]) * (1.0 / LANES) for _, m, slot in others
        ]
        acc_gp = c_y * m_g[sums, :] + fold(w2_part * m_g[w2rows, :]) * (1.0 / LANES)
        acc_yy = c_y * w0_y + fold(w2_part * w2_part) * (1.0 / LANES)
        for part in row_parts:
            d_part = d_y[new, :, part]
            for idx, (q, _, slot) in enumerate(others):
                accs[idx] = accs[idx] + fold(d_part * q[slot, :, part])
            q_old = q_g[:, part]
            acc_gp = acc_gp + fold(d_part * q_old)
            q_new = reg * q_s[new, :, part] + gram_times(part)
            q_y[new, :, part] = q_new
            q_g[:, part] = q_old + q_new
            acc_yy = acc_yy + fold(d_part * q_new)
        order = accs[:3] + [acc_yy] + accs[3:] + [acc_gp, acc_gs]
        rows = [jnp.sum(acc, axis=0, keepdims=True) for acc in order]
        totals = jnp.sum(jnp.concatenate(rows, axis=0), axis=1, keepdims=True)
        packed = jnp.sum(jnp.where(eye[:NUM_DOTS], totals, 0.0), axis=0, keepdims=True)
        dot_src[...] = packed
        dot_buf[me] = packed
        send_all(dot_src, dot_buf, 2)
        m_g[...] = m_g[...] + m_y[new]
        for part in tiles:
            d_g[:, part] = d_g[:, part] + d_y[new, :, part]

    def two_loop(carry):
        rho1, rho2, psg0, psg1, pyg0, pyg1, pys1, yy11, yy12, yy22 = carry
        wait_all(dot_buf, 2)
        total = jnp.sum(dot_buf[...], axis=0)
        ys0, ys1, ys2, yy0, yy1, yy2, ygp, gs0 = (
            jnp.broadcast_to(total[:, idx : idx + 1], (SUBL, LANES)) for idx in range(NUM_DOTS)
        )
        sg0, sg1, sg2 = gs0 + ys0, psg0 + ys1, psg1 + ys2
        yg0, yg1, yg2 = ygp + yy0, pyg0 + yy1, pyg1 + yy2
        rho0 = 1.0 / ys0
        gamma = ys0 / yy0
        a0 = rho0 * sg0
        a1 = rho1 * (sg1 - a0 * ys1)
        a2 = rho2 * (sg2 - a0 * ys2 - a1 * pys1)
        yq2 = yg2 - a0 * yy2 - a1 * yy12 - a2 * yy22
        yq1 = yg1 - a0 * yy1 - a1 * yy11 - a2 * yy12
        yq0 = yg0 - a0 * yy0 - a1 * yy1 - a2 * yy2
        c2 = a2 - rho2 * (gamma * yq2)
        c1 = a1 - rho1 * (gamma * yq1 + c2 * pys1)
        c0 = a0 - rho0 * (gamma * yq0 + c2 * ys2 + c1 * ys1)
        sgam = step * gamma
        for idx, val in enumerate((-sgam, -step * c0, -step * c1, -step * c2, sgam * a0, sgam * a1, sgam * a2)):
            coef[idx] = val
        return rho0, rho1, sg0, sg1, yg0, yg1, ys1, yy0, yy1, yy11

    def load_coef():
        return [coef[idx] for idx in range(1 + 2 * HIST)]

    w2_row = jnp.broadcast_to(wout_ref[...], (hid_rows, LANES))
    w2_col = jnp.sum(jnp.where(eye, w2_row, 0.0), axis=1, keepdims=True)
    w2[...] = jnp.broadcast_to(w2_col, (hid_rows, LANES))
    w0_w0 = jnp.zeros((SUBL, LANES), F32)
    for start in range(0, dim, LANES):
        part = pl.ds(start, LANES)
        w_part = w0[:, part]
        w0_w0 = w0_w0 + fold(w_part * w_part)
        store_split(split_w, part, w_part)
    peaks = []
    for idx, part in enumerate(row_parts):
        total = None
        for half, load in zip(dim_halves, x_loads[2 * idx : 2 * idx + 2]):
            load.wait()
            prod = lax.dot_general(
                split_w[:, half], x_v[part, half], (((1,), (1,)), ((), ())), preferred_element_type=F32
            )
            total = merge3(prod, hid_rows) if total is None else total + merge3(prod, hid_rows)
        pre_part = total * in_scale
        pre[:, part] = pre_part
        pre0[:, part] = pre_part
        peaks.append(jnp.max(jnp.abs(x_v[part, :]).reshape(ROW_CHUNK // 16, 16, dim), axis=0))
    x_scale, x_inverse = power_of_two(jnp.max(functools.reduce(jnp.maximum, peaks).astype(F32)))
    pl.semaphore_wait(barrier, n - 1)
    send_logits(z_buf.at[0], 0, lazy=True)
    for row, row_part in enumerate(row_parts):
        xs[row_part, :] = x_v[row_part, :] * jnp.full((ROW_CHUNK, dim), x_inverse, F32).astype(BF16)
        for col, col_part in enumerate(row_parts[: row + 1]):
            block = lax.dot_general(
                xs[row_part, :], xs[col_part, :], (((1,), (1,)), ((), ())), preferred_element_type=F32
            ) * (in_scale * in_scale)
            for idx, term in enumerate(split3(block)):
                gram[idx, row_part, col_part] = term
            if col < row:
                for idx, term in enumerate(split3(block.T)):
                    gram[idx, col_part, row_part] = term
    set_factor()
    for ref in (q_s, q_y, d_s, d_y, m_s, m_y, coef):
        ref[...] = jnp.zeros_like(ref)
    cv[...] = jnp.where(unit == 0, 1.0, 0.0)
    coef[0] = jnp.full((SUBL, LANES), -step, F32)
    residual(z_buf.at[0], 0)
    acc_w0 = reg * w0_w0
    for idx, part in enumerate(tiles):
        d_new = fac[:, part] * resid[idx : idx + 1, :]
        d_old[:, part] = d_new
        d_g[:, part] = d_new
        store_split(split_d, part, d_new)
        acc_w0 = acc_w0 + fold(d_new * pre0[:, part])
    m_g[sums, :] = acc_w0
    m_g[cfrow, :] = reg * cv[...] + jnp.where(unit == 1, 1.0, 0.0)
    m_g[w2rows, :] = w2_grad()
    for part in row_parts:
        q_g[:, part] = reg * pre0[:, part] + gram_times(part)
    store_loss(0)

    def head(k):
        new, old1, old2 = lax.rem(k, HIST), lax.rem(k + 2, HIST), lax.rem(k + 1, HIST)
        prev = (old1, old2, new)
        cfs = load_coef()
        move(cfs, prev)
        send_logits(z_buf.at[1], 1)
        acc_gs = move_rest(cfs, prev)
        keep_g_part(k - 1)
        residual(z_buf.at[1], 1)
        new_grad(k, (new, old1, old2), acc_gs)

    def body(k, carry):
        head(k)
        store_loss(k)
        return two_loop(carry)

    zero = jnp.zeros((SUBL, LANES), F32)
    carry = lax.fori_loop(1, NUM_ITERS - 1, body, (zero,) * 10)

    last = NUM_ITERS - 1
    head(last)
    store_loss(last)
    keep_g_part(last)
    two_loop(carry)
    slots = (last % HIST, (last + 2) % HIST, (last + 1) % HIST)
    cfs = load_coef()
    w2_new = w2[...] + combine(cfs, slots, m_g, m_s, m_y, w2rows, lanes)
    out_w2[...] = jnp.sum(jnp.where(eye, w2_new, 0.0), axis=0, keepdims=True)
    cv_new = cv[...] + combine(cfs, slots, m_g, m_s, m_y, cfrow, lanes)
    for idx in range(1 + NUM_ITERS):
        weights[idx] = splat(cv_new[idx : idx + 1, :])


def write_out(w0, g_parts, weights, w2_ref, loss_ref, out_w, out_w2, out_loss, w_v, sems, w_sems):
    rows, dim = out_w.shape
    copies = [
        pltpu.make_async_copy(src, dst, sems.at[idx]) for idx, (src, dst) in enumerate(((w2_ref, out_w2), (loss_ref, out_loss)))
    ]
    for copy in copies:
        copy.start()
    factors = [weights[idx][None] for idx in range(1 + NUM_ITERS)]

    def weighted(factor, val):
        return (val.reshape(rows // SUBL, SUBL, LANES) * factor).reshape(rows, LANES)

    for idx, start in enumerate(range(0, dim, COL_CHUNK)):
        for tile in range(start, start + COL_CHUNK, LANES):
            part = pl.ds(tile, LANES)
            total = weighted(factors[0], w0[:, part])
            for term in range(NUM_ITERS):
                total = total + weighted(factors[1 + term], g_parts[term, :, part])
            w_v[:, part] = total
        part = pl.ds(start, COL_CHUNK)
        copy = pltpu.make_async_copy(w_v.at[:, part], out_w.at[:, part], w_sems.at[idx])
        copy.start()
        copies.append(copy)
    for copy in copies:
        copy.wait()


def solution(mesh):
    n = mesh.shape["feat"]

    def local_solve(x_loc, t_loc, win_loc, wout_loc, reg_loc, step_loc):
        num_rows, dim = x_loc.shape
        hid_rows = win_loc.shape[0]
        flat = pltpu.VMEM((hid_rows, num_rows + LANES), F32)
        past = pltpu.VMEM((HIST, hid_rows, num_rows + LANES), F32)
        meta = 2 * SUBL + hid_rows
        in_scale = 1.0 / math.sqrt(dim)
        out_scale = 1.0 / math.sqrt(hid_rows * n)
        row_tiles = num_rows // LANES
        vmem = pl.BlockSpec(memory_space=pltpu.VMEM)
        smem = pl.BlockSpec(memory_space=pltpu.SMEM)
        anym = pl.BlockSpec(memory_space=pl.ANY)
        solved = pl.pallas_call(
            functools.partial(kernel, "feat", n, in_scale, out_scale),
            out_shape=(
                pltpu.VMEM((hid_rows, dim + LANES), F32),
                pltpu.VMEM((NUM_ITERS, hid_rows, dim + LANES), F32),
                pltpu.VMEM((1 + NUM_ITERS, SUBL, LANES), F32),
                pltpu.VMEM((1, hid_rows), F32),
                pltpu.SMEM((NUM_ITERS,), F32),
            ),
            in_specs=[anym] * 6,
            out_specs=(vmem, vmem, vmem, vmem, smem),
            scratch_shapes=[
                pltpu.VMEM((row_tiles, LANES), F32),
                pltpu.VMEM((1, hid_rows), F32),
                pltpu.SMEM((1,), F32),
                pltpu.SMEM((1,), F32),
                pltpu.VMEM((num_rows, dim), BF16),
                pltpu.VMEM((num_rows, dim), BF16),
                pltpu.VMEM((3, num_rows, num_rows), BF16),
                *([flat] * 5),
                past, past, flat, past, past, flat,
                pltpu.VMEM((HIST, meta, LANES), F32),
                pltpu.VMEM((HIST, meta, LANES), F32),
                pltpu.VMEM((meta, LANES), F32),
                pltpu.VMEM((hid_rows, LANES), F32),
                pltpu.VMEM((SUBL, LANES), F32),
                pltpu.VMEM((3 * hid_rows, num_rows), BF16),
                pltpu.VMEM((3 * hid_rows, dim), BF16),
                pltpu.VMEM((row_tiles, LANES), F32),
                pltpu.VMEM((row_tiles, LANES), F32),
                pltpu.VMEM((1 + 2 * HIST, SUBL, LANES), F32),
                pltpu.VMEM((row_tiles, LANES), F32),
                pltpu.VMEM((2, n, row_tiles, LANES), F32),
                pltpu.VMEM((1, LANES), F32),
                pltpu.VMEM((n, 1, LANES), F32),
                pltpu.SemaphoreType.DMA((1 + 2 * (num_rows // ROW_CHUNK),)),
                pltpu.SemaphoreType.DMA((4,)),
                pltpu.SemaphoreType.DMA((3,)),
                pltpu.SemaphoreType.DMA((3,)),
            ],
            compiler_params=pltpu.CompilerParams(
                collective_id=0, has_side_effects=True, vmem_limit_bytes=46 * 1024 * 1024
            ),
        )(
            *(
                pltpu.with_memory_space_constraint(arg, pltpu.HBM)
                for arg in (x_loc, t_loc.reshape(row_tiles, LANES), win_loc, wout_loc.reshape(1, hid_rows))
            ),
            reg_loc, step_loc,
        )
        new_w, new_w2, losses = pl.pallas_call(
            write_out,
            out_shape=tuple(jax.ShapeDtypeStruct(shape, F32) for shape in ((hid_rows, dim), (1, hid_rows), (NUM_ITERS,))),
            in_specs=[vmem, vmem, vmem, vmem, smem],
            out_specs=(anym, anym, anym),
            scratch_shapes=[
                pltpu.VMEM((hid_rows, dim + LANES), F32),
                pltpu.SemaphoreType.DMA((2,)),
                pltpu.SemaphoreType.DMA((dim // COL_CHUNK,)),
            ],
            compiler_params=pltpu.CompilerParams(vmem_limit_bytes=4 * 1024 * 1024),
        )(*solved)
        return new_w, new_w2.reshape(hid_rows), losses

    specs_in = (P("prob", None), P("prob"), P(("prob", "feat"), None), P(("prob", "feat")), P("prob"), P("prob"))
    specs_out = (P(("prob", "feat"), None), P(("prob", "feat")), P("prob"))
    return jax.shard_map(local_solve, mesh=mesh, in_specs=specs_in, out_specs=specs_out, check_vma=False)
```

```python
import functools
import math

import jax
import jax.numpy as jnp
from jax import lax
from jax.experimental import pallas as pl
from jax.experimental.pallas import tpu as pltpu
from jax.sharding import PartitionSpec as P

NUM_ITERS = 6
HIST = 3
LANES = 128
SUBL = 8
ROW_CHUNK = 512
COL_CHUNK = 512
NUM_DOTS = 8
MESH = pl.DeviceIdType.MESH
F32 = jnp.float32
BF16 = jnp.bfloat16


def split3(val):
    high = val.astype(BF16)
    rest = val - high.astype(F32)
    mid = rest.astype(BF16)
    low = (rest - mid.astype(F32)).astype(BF16)
    return high, mid, low


def fold(val):
    rows, cols = val.shape
    part = jnp.sum(val.reshape(rows // SUBL, SUBL, cols), axis=0)
    total = part[:, :LANES]
    for start in range(LANES, cols, LANES):
        total = total + part[:, start : start + LANES]
    return total


def merge3(prod, rows):
    return (prod[2 * rows :] + prod[rows : 2 * rows]) + prod[:rows]


def power_of_two(peak):
    scale = jnp.float32(1.0)
    inverse = jnp.float32(1.0)
    for up in (True, False):
        for bits in (64, 32, 16, 8, 4, 2):
            big, small = 2.0**bits, 2.0**-bits
            grow, shrink = (small, big) if up else (big, small)
            hit = (peak >= big) if up else (peak <= small)
            peak = jnp.where(hit, peak * grow, peak)
            inverse = jnp.where(hit, inverse * grow, inverse)
            scale = jnp.where(hit, scale * shrink, scale)
    return scale, inverse


def kernel(
    axis, n, in_scale, out_scale,
    x_hbm, t_hbm, win_hbm, wout_hbm, reg_hbm, step_hbm,
    w0, g_parts, weights, out_w2, out_loss,
    t_ref, wout_ref, reg_ref, step_ref,
    x_v, xs, gram, pre, pre0, hid, fac, d_old,
    q_s, q_y, q_g, d_s, d_y, d_g, m_s, m_y, m_g, w2, cv,
    split_d, split_w, resid, logits_v, coef,
    z_src, z_buf, dot_src, dot_buf,
    load_sem, small_sem, send_sem, recv_sem,
):
    num_rows, dim = x_v.shape
    hid_rows = w0.shape[0]
    row_tiles = num_rows // LANES
    me = lax.axis_index(axis)
    offsets = sorted(range(1, n), key=lambda off: -min(off, n - off))
    peers = [lax.rem(me + off, n) for off in offsets]

    w_load = pltpu.make_async_copy(win_hbm, w0.at[:, pl.ds(0, dim)], load_sem.at[0])
    w_load.start()
    row_parts = [pl.ds(start, ROW_CHUNK) for start in range(0, num_rows, ROW_CHUNK)]
    dim_halves = [pl.ds(0, dim // 2), pl.ds(dim // 2, dim // 2)]
    x_loads = []
    for part in row_parts:
        for half in dim_halves:
            sem = load_sem.at[1 + len(x_loads)]
            x_loads.append(pltpu.make_async_copy(x_hbm.at[part, half], x_v.at[part, half], sem))
    for load in x_loads[:2]:
        load.start()
    smalls = []
    for idx, (src, dst) in enumerate(((t_hbm, t_ref), (wout_hbm, wout_ref), (reg_hbm, reg_ref), (step_hbm, step_ref))):
        load = pltpu.make_async_copy(src, dst, small_sem.at[idx])
        load.start()
        smalls.append(load)

    barrier = pltpu.get_barrier_semaphore()
    for peer in peers:
        pl.semaphore_signal(barrier, inc=1, device_id={axis: peer}, device_id_type=MESH)

    w_load.wait()
    for load in x_loads[2:]:
        load.start()
    for load in smalls:
        load.wait()
    reg = reg_ref[0]
    step = step_ref[0]
    eye = lax.broadcasted_iota(jnp.int32, (hid_rows, LANES), 1) == lax.broadcasted_iota(jnp.int32, (hid_rows, LANES), 0)
    unit = lax.broadcasted_iota(jnp.int32, (SUBL, LANES), 0)
    col_parts = [pl.ds(start, COL_CHUNK) for start in range(0, dim, COL_CHUNK)]
    tiles = [pl.ds(start, LANES) for start in range(0, num_rows, LANES)]
    sums, cfrow, w2rows = pl.ds(0, SUBL), pl.ds(SUBL, SUBL), pl.ds(2 * SUBL, hid_rows)
    top = pl.ds(SUBL, 1)

    def send_all(src, dst, sem):
        for peer in peers:
            pltpu.make_async_remote_copy(
                src_ref=src, dst_ref=dst.at[me], send_sem=send_sem.at[sem], recv_sem=recv_sem.at[sem],
                device_id={axis: peer}, device_id_type=MESH,
            ).start()

    def wait_all(dst, sem):
        others = dst.at[pl.ds(0, n - 1)]
        pltpu.make_async_copy(others, others, recv_sem.at[sem]).wait()
        pltpu.make_async_copy(others, others, send_sem.at[sem]).wait()

    def splat(row):
        return jnp.broadcast_to(row, (SUBL, LANES))

    def store_split(ref, part, val):
        for idx, term in enumerate(split3(val)):
            ref[idx * hid_rows : (idx + 1) * hid_rows, part] = term

    def set_factor():
        w2s = w2[...] * out_scale
        for part in tiles:
            act = hid[:, part]
            fac[:, part] = w2s * (1.0 - act * act)

    def send_logits(buf, sem, lazy=False):
        rows = []
        for part in tiles:
            act = jnp.tanh(pre[:, part])
            hid[:, part] = act
            rows.append(jnp.sum(fold(act * w2[...]), axis=0, keepdims=True))
        z_mine = jnp.concatenate(rows, axis=0)
        z_src[...] = z_mine
        buf[me] = z_mine
        send_all(z_src, buf, sem)
        if not lazy:
            set_factor()

    def residual(buf, sem):
        wait_all(buf, sem)
        logits = jnp.sum(buf[...], axis=0) * out_scale
        logits_v[...] = logits
        resid[...] = (jax.nn.sigmoid(logits) - t_ref[...]) * (1.0 / num_rows)

    def w2_grad():
        total = hid[:, tiles[0]] * resid[0:1, :]
        for idx in range(1, row_tiles):
            total = total + hid[:, tiles[idx]] * resid[idx : idx + 1, :]
        g_out = jnp.sum(total, axis=1, keepdims=True) * out_scale
        return jnp.broadcast_to(g_out, (hid_rows, LANES)) + reg * w2[...]

    def gram_times(part):
        high = jnp.dot(split_d[...], gram[0, :, part], preferred_element_type=F32)
        mid = jnp.dot(split_d[: 2 * hid_rows], gram[1, :, part], preferred_element_type=F32)
        low = jnp.dot(split_d[:hid_rows], gram[2, :, part], preferred_element_type=F32)
        small = (high[2 * hid_rows :] + mid[hid_rows:]) + low
        return (((high[hid_rows : 2 * hid_rows] + mid[:hid_rows]) + small + high[:hid_rows]) * x_scale) * x_scale

    def keep_g_part(idx):
        for part in col_parts:
            prod = jnp.dot(split_d[...], xs[:, part], preferred_element_type=F32)
            g_parts[idx, :, part] = merge3(prod, hid_rows) * in_scale * x_scale

    def store_loss(idx):
        logits = logits_v[...]
        soft = jnp.maximum(logits, 0.0) + jnp.log1p(jnp.exp(-jnp.abs(logits)))
        out_loss[idx] = jnp.sum(soft - t_ref[...] * logits) * (1.0 / num_rows)

    def combine(cfs, slots, vec_g, vec_s, vec_y, rows, part):
        def scaled(cf, val):
            count = val.shape[0]
            return (val.reshape(count // SUBL, SUBL, LANES) * cf[None]).reshape(count, LANES)

        total = scaled(cfs[0], vec_g[rows, part])
        for idx, slot in enumerate(slots):
            total = total + scaled(cfs[1 + idx], vec_s[slot, rows, part])
            total = total + scaled(cfs[1 + HIST + idx], vec_y[slot, rows, part])
        return total

    every, lanes = pl.ds(0, hid_rows), pl.ds(0, LANES)

    def move(cfs, slots):
        new = slots[-1]
        s_part = combine(cfs, slots, m_g, m_s, m_y, w2rows, lanes)
        m_s[new, w2rows, :] = s_part
        w2[...] = w2[...] + s_part
        for part in tiles:
            q_part = combine(cfs, slots, q_g, q_s, q_y, every, part)
            q_s[new, :, part] = q_part
            pre[:, part] = pre[:, part] + q_part

    def move_rest(cfs, slots):
        new = slots[-1]
        s_part = combine(cfs, slots, m_g, m_s, m_y, pl.ds(0, 2 * SUBL), lanes)
        m_s[new, pl.ds(0, 2 * SUBL), :] = s_part
        cv[...] = cv[...] + s_part[SUBL:]
        acc = splat(m_g[top, :]) * s_part[:SUBL] + fold(m_g[w2rows, :] * m_s[new, w2rows, :]) * (1.0 / LANES)
        for part in tiles:
            d_part = combine(cfs, slots, d_g, d_s, d_y, every, part)
            d_s[new, :, part] = d_part
            acc = acc + fold(d_g[:, part] * q_s[new, :, part])
        return acc

    def new_grad(k, slots, acc_gs):
        new, old1, old2 = slots
        w2_part = w2_grad() - m_g[w2rows, :]
        acc_w0 = jnp.zeros((SUBL, LANES), F32)
        for idx, part in enumerate(tiles):
            d_new = fac[:, part] * resid[idx : idx + 1, :]
            diff = d_new - d_old[:, part]
            d_old[:, part] = d_new
            store_split(split_d, part, diff)
            d_y[new, :, part] = reg * d_s[new, :, part] + diff
            acc_w0 = acc_w0 + fold(diff * pre0[:, part])
        w0_y = reg * m_s[new, sums, :] + acc_w0
        cf_y = reg * m_s[new, cfrow, :] + jnp.where(unit == k + 1, 1.0, 0.0)
        c_y = splat(cf_y[0:1, :])
        m_y[new, sums, :] = w0_y
        m_y[new, cfrow, :] = cf_y
        m_y[new, w2rows, :] = w2_part
        others = [(q_s, m_s, new), (q_s, m_s, old1), (q_s, m_s, old2), (q_y, m_y, old1), (q_y, m_y, old2)]
        accs = [
            c_y * m[slot, sums, :] + fold(w2_part * m[slot, w2rows, :]) * (1.0 / LANES) for _, m, slot in others
        ]
        acc_gp = c_y * m_g[sums, :] + fold(w2_part * m_g[w2rows, :]) * (1.0 / LANES)
        acc_yy = c_y * w0_y + fold(w2_part * w2_part) * (1.0 / LANES)
        for part in row_parts:
            d_part = d_y[new, :, part]
            for idx, (q, _, slot) in enumerate(others):
                accs[idx] = accs[idx] + fold(d_part * q[slot, :, part])
            q_old = q_g[:, part]
            acc_gp = acc_gp + fold(d_part * q_old)
            q_new = reg * q_s[new, :, part] + gram_times(part)
            q_y[new, :, part] = q_new
            q_g[:, part] = q_old + q_new
            acc_yy = acc_yy + fold(d_part * q_new)
        order = accs[:3] + [acc_yy] + accs[3:] + [acc_gp, acc_gs]
        rows = [jnp.sum(acc, axis=0, keepdims=True) for acc in order]
        totals = jnp.sum(jnp.concatenate(rows, axis=0), axis=1, keepdims=True)
        packed = jnp.sum(jnp.where(eye[:NUM_DOTS], totals, 0.0), axis=0, keepdims=True)
        dot_src[...] = packed
        dot_buf[me] = packed
        send_all(dot_src, dot_buf, 2)
        m_g[...] = m_g[...] + m_y[new]
        for part in tiles:
            d_g[:, part] = d_g[:, part] + d_y[new, :, part]

    def two_loop(carry):
        rho1, rho2, psg0, psg1, pyg0, pyg1, pys1, yy11, yy12, yy22 = carry
        wait_all(dot_buf, 2)
        total = jnp.sum(dot_buf[...], axis=0)
        ys0, ys1, ys2, yy0, yy1, yy2, ygp, gs0 = (
            jnp.broadcast_to(total[:, idx : idx + 1], (SUBL, LANES)) for idx in range(NUM_DOTS)
        )
        sg0, sg1, sg2 = gs0 + ys0, psg0 + ys1, psg1 + ys2
        yg0, yg1, yg2 = ygp + yy0, pyg0 + yy1, pyg1 + yy2
        rho0 = 1.0 / ys0
        gamma = ys0 / yy0
        a0 = rho0 * sg0
        a1 = rho1 * (sg1 - a0 * ys1)
        a2 = rho2 * (sg2 - a0 * ys2 - a1 * pys1)
        yq2 = yg2 - a0 * yy2 - a1 * yy12 - a2 * yy22
        yq1 = yg1 - a0 * yy1 - a1 * yy11 - a2 * yy12
        yq0 = yg0 - a0 * yy0 - a1 * yy1 - a2 * yy2
        c2 = a2 - rho2 * (gamma * yq2)
        c1 = a1 - rho1 * (gamma * yq1 + c2 * pys1)
        c0 = a0 - rho0 * (gamma * yq0 + c2 * ys2 + c1 * ys1)
        sgam = step * gamma
        for idx, val in enumerate((-sgam, -step * c0, -step * c1, -step * c2, sgam * a0, sgam * a1, sgam * a2)):
            coef[idx] = val
        return rho0, rho1, sg0, sg1, yg0, yg1, ys1, yy0, yy1, yy11

    def load_coef():
        return [coef[idx] for idx in range(1 + 2 * HIST)]

    w2_row = jnp.broadcast_to(wout_ref[...], (hid_rows, LANES))
    w2_col = jnp.sum(jnp.where(eye, w2_row, 0.0), axis=1, keepdims=True)
    w2[...] = jnp.broadcast_to(w2_col, (hid_rows, LANES))
    w0_w0 = jnp.zeros((SUBL, LANES), F32)

    def split_half(first, acc):
        for start in range(first, first + dim // 2, LANES):
            part = pl.ds(start, LANES)
            w_part = w0[:, part]
            acc = acc + fold(w_part * w_part)
            store_split(split_w, part, w_part)
        return acc

    w0_w0 = split_half(0, w0_w0)
    peaks = []
    for idx, part in enumerate(row_parts):
        total = None
        for half, load in zip(dim_halves, x_loads[2 * idx : 2 * idx + 2]):
            if idx == 0 and total is not None:
                w0_w0 = split_half(dim // 2, w0_w0)
            load.wait()
            prod = lax.dot_general(
                split_w[:, half], x_v[part, half], (((1,), (1,)), ((), ())), preferred_element_type=F32
            )
            total = merge3(prod, hid_rows) if total is None else total + merge3(prod, hid_rows)
        pre_part = total * in_scale
        pre[:, part] = pre_part
        pre0[:, part] = pre_part
        peaks.append(jnp.max(jnp.abs(x_v[part, :]).reshape(ROW_CHUNK // 16, 16, dim), axis=0))
    x_scale, x_inverse = power_of_two(jnp.max(functools.reduce(jnp.maximum, peaks).astype(F32)))
    pl.semaphore_wait(barrier, n - 1)
    send_logits(z_buf.at[0], 0, lazy=True)
    for row, row_part in enumerate(row_parts):
        xs[row_part, :] = x_v[row_part, :] * jnp.full((ROW_CHUNK, dim), x_inverse, F32).astype(BF16)
        for col, col_part in enumerate(row_parts[: row + 1]):
            block = lax.dot_general(
                xs[row_part, :], xs[col_part, :], (((1,), (1,)), ((), ())), preferred_element_type=F32
            ) * (in_scale * in_scale)
            for idx, term in enumerate(split3(block)):
                gram[idx, row_part, col_part] = term
            if col < row:
                for idx, term in enumerate(split3(block.T)):
                    gram[idx, col_part, row_part] = term
    set_factor()
    for ref in (q_s, q_y, d_s, d_y, m_s, m_y, coef):
        ref[...] = jnp.zeros_like(ref)
    cv[...] = jnp.where(unit == 0, 1.0, 0.0)
    coef[0] = jnp.full((SUBL, LANES), -step, F32)
    residual(z_buf.at[0], 0)
    acc_w0 = reg * w0_w0
    for idx, part in enumerate(tiles):
        d_new = fac[:, part] * resid[idx : idx + 1, :]
        d_old[:, part] = d_new
        d_g[:, part] = d_new
        store_split(split_d, part, d_new)
        acc_w0 = acc_w0 + fold(d_new * pre0[:, part])
    m_g[sums, :] = acc_w0
    m_g[cfrow, :] = reg * cv[...] + jnp.where(unit == 1, 1.0, 0.0)
    m_g[w2rows, :] = w2_grad()
    for part in row_parts:
        q_g[:, part] = reg * pre0[:, part] + gram_times(part)
    store_loss(0)

    def head(k):
        new, old1, old2 = lax.rem(k, HIST), lax.rem(k + 2, HIST), lax.rem(k + 1, HIST)
        prev = (old1, old2, new)
        cfs = load_coef()
        move(cfs, prev)
        send_logits(z_buf.at[1], 1)
        acc_gs = move_rest(cfs, prev)
        keep_g_part(k - 1)
        residual(z_buf.at[1], 1)
        new_grad(k, (new, old1, old2), acc_gs)

    def body(k, carry):
        head(k)
        store_loss(k)
        return two_loop(carry)

    zero = jnp.zeros((SUBL, LANES), F32)
    carry = lax.fori_loop(1, NUM_ITERS - 1, body, (zero,) * 10)

    last = NUM_ITERS - 1
    head(last)
    store_loss(last)
    keep_g_part(last)
    two_loop(carry)
    slots = (last % HIST, (last + 2) % HIST, (last + 1) % HIST)
    cfs = load_coef()
    w2_new = w2[...] + combine(cfs, slots, m_g, m_s, m_y, w2rows, lanes)
    out_w2[...] = jnp.sum(jnp.where(eye, w2_new, 0.0), axis=0, keepdims=True)
    cv_new = cv[...] + combine(cfs, slots, m_g, m_s, m_y, cfrow, lanes)
    for idx in range(1 + NUM_ITERS):
        weights[idx] = splat(cv_new[idx : idx + 1, :])


def write_out(w0, g_parts, weights, w2_ref, loss_ref, out_w, out_w2, out_loss, w_v, sems, w_sems):
    rows, dim = out_w.shape
    copies = [
        pltpu.make_async_copy(src, dst, sems.at[idx]) for idx, (src, dst) in enumerate(((w2_ref, out_w2), (loss_ref, out_loss)))
    ]
    for copy in copies:
        copy.start()
    factors = [weights[idx][None] for idx in range(1 + NUM_ITERS)]

    def weighted(factor, val):
        return (val.reshape(rows // SUBL, SUBL, LANES) * factor).reshape(rows, LANES)

    for idx, start in enumerate(range(0, dim, COL_CHUNK)):
        for tile in range(start, start + COL_CHUNK, LANES):
            part = pl.ds(tile, LANES)
            total = weighted(factors[0], w0[:, part])
            for term in range(NUM_ITERS):
                total = total + weighted(factors[1 + term], g_parts[term, :, part])
            w_v[:, part] = total
        part = pl.ds(start, COL_CHUNK)
        copy = pltpu.make_async_copy(w_v.at[:, part], out_w.at[:, part], w_sems.at[idx])
        copy.start()
        copies.append(copy)
    for copy in copies:
        copy.wait()


def solution(mesh):
    n = mesh.shape["feat"]

    def local_solve(x_loc, t_loc, win_loc, wout_loc, reg_loc, step_loc):
        num_rows, dim = x_loc.shape
        hid_rows = win_loc.shape[0]
        flat = pltpu.VMEM((hid_rows, num_rows + LANES), F32)
        past = pltpu.VMEM((HIST, hid_rows, num_rows + LANES), F32)
        meta = 2 * SUBL + hid_rows
        in_scale = 1.0 / math.sqrt(dim)
        out_scale = 1.0 / math.sqrt(hid_rows * n)
        row_tiles = num_rows // LANES
        vmem = pl.BlockSpec(memory_space=pltpu.VMEM)
        smem = pl.BlockSpec(memory_space=pltpu.SMEM)
        anym = pl.BlockSpec(memory_space=pl.ANY)
        solved = pl.pallas_call(
            functools.partial(kernel, "feat", n, in_scale, out_scale),
            out_shape=(
                pltpu.VMEM((hid_rows, dim + LANES), F32),
                pltpu.VMEM((NUM_ITERS, hid_rows, dim + LANES), F32),
                pltpu.VMEM((1 + NUM_ITERS, SUBL, LANES), F32),
                pltpu.VMEM((1, hid_rows), F32),
                pltpu.SMEM((NUM_ITERS,), F32),
            ),
            in_specs=[anym] * 6,
            out_specs=(vmem, vmem, vmem, vmem, smem),
            scratch_shapes=[
                pltpu.VMEM((row_tiles, LANES), F32),
                pltpu.VMEM((1, hid_rows), F32),
                pltpu.SMEM((1,), F32),
                pltpu.SMEM((1,), F32),
                pltpu.VMEM((num_rows, dim), BF16),
                pltpu.VMEM((num_rows, dim), BF16),
                pltpu.VMEM((3, num_rows, num_rows), BF16),
                *([flat] * 5),
                past, past, flat, past, past, flat,
                pltpu.VMEM((HIST, meta, LANES), F32),
                pltpu.VMEM((HIST, meta, LANES), F32),
                pltpu.VMEM((meta, LANES), F32),
                pltpu.VMEM((hid_rows, LANES), F32),
                pltpu.VMEM((SUBL, LANES), F32),
                pltpu.VMEM((3 * hid_rows, num_rows), BF16),
                pltpu.VMEM((3 * hid_rows, dim), BF16),
                pltpu.VMEM((row_tiles, LANES), F32),
                pltpu.VMEM((row_tiles, LANES), F32),
                pltpu.VMEM((1 + 2 * HIST, SUBL, LANES), F32),
                pltpu.VMEM((row_tiles, LANES), F32),
                pltpu.VMEM((2, n, row_tiles, LANES), F32),
                pltpu.VMEM((1, LANES), F32),
                pltpu.VMEM((n, 1, LANES), F32),
                pltpu.SemaphoreType.DMA((1 + 2 * (num_rows // ROW_CHUNK),)),
                pltpu.SemaphoreType.DMA((4,)),
                pltpu.SemaphoreType.DMA((3,)),
                pltpu.SemaphoreType.DMA((3,)),
            ],
            compiler_params=pltpu.CompilerParams(
                collective_id=0, has_side_effects=True, vmem_limit_bytes=46 * 1024 * 1024
            ),
        )(
            *(
                pltpu.with_memory_space_constraint(arg, pltpu.HBM)
                for arg in (x_loc, t_loc.reshape(row_tiles, LANES), win_loc, wout_loc.reshape(1, hid_rows))
            ),
            reg_loc, step_loc,
        )
        new_w, new_w2, losses = pl.pallas_call(
            write_out,
            out_shape=tuple(jax.ShapeDtypeStruct(shape, F32) for shape in ((hid_rows, dim), (1, hid_rows), (NUM_ITERS,))),
            in_specs=[vmem, vmem, vmem, vmem, smem],
            out_specs=(anym, anym, anym),
            scratch_shapes=[
                pltpu.VMEM((hid_rows, dim + LANES), F32),
                pltpu.SemaphoreType.DMA((2,)),
                pltpu.SemaphoreType.DMA((dim // COL_CHUNK,)),
            ],
            compiler_params=pltpu.CompilerParams(vmem_limit_bytes=4 * 1024 * 1024),
        )(*solved)
        return new_w, new_w2.reshape(hid_rows), losses

    specs_in = (P("prob", None), P("prob"), P(("prob", "feat"), None), P(("prob", "feat")), P("prob"), P("prob"))
    specs_out = (P(("prob", "feat"), None), P(("prob", "feat")), P("prob"))
    return jax.shard_map(local_solve, mesh=mesh, in_specs=specs_in, out_specs=specs_out, check_vma=False)
```
